128 devices in a mesh: cell: 8 (over z, core), tm: 16 (over y, x).
Axes of the slice: x: 4, y: 4, z: 4, core: 2. Of those that a mesh axis runs over, the one named last changes fastest.
Arguments:
- solution: float32 [32768], P(('cell', 'tm')), may hold values from -6 to 6
- residual: float32 [32768], P(('cell', 'tm')), may hold values from -8 to 8
- direction: float32 [32768], P(('cell', 'tm')), may hold values from -8 to 8
- noise_var: float32 [32768], P(('cell', 'tm')), may hold values from 0.5 to 2
- footprints: bfloat16 [262144, 128], P(('cell', 'tm')), may hold values from -0.5 to 0.5
- tile_owner: int32 [262144, 1], P(('cell', 'tm')), may hold values from 0 to 127; in each aligned block of 2048 rows (0 to 2047, 2048 to 4095, ...) at most 32 rows name the same one
- tile_block: int32 [262144], P(('cell', 'tm')), may hold values from 0 to 8
- tile_step: int32 [262144], P(('cell', 'tm')), may hold values from 0 to 127
- tile_obs: int32 [262144], P(('cell', 'tm')), may hold values from 0 to 255
- cell_cov: bfloat16 [9216, 9216], P('cell'), may hold values from -2 to 7, as said below
- time_cov: bfloat16 [2048, 2048], P('tm'), may hold values from -2 to 7, as said below
Outputs:
- new_solution: float32 [32768], P(('cell', 'tm'))
- new_residual: float32 [32768], P(('cell', 'tm'))
- new_direction: float32 [32768], P(('cell', 'tm'))
The draws below stay inside these ranges and needn't reach their ends.
Inputs may be any that keep to these rules, and one draw needn't show every extreme that they name: `tile_owner`: among the 2048 tiles of one device, no owner is named by more than 32 of them. `cell_cov`: symmetric positive definite. `time_cov`: symmetric positive definite.
All inputs are finite; a program needn't handle non-finite values.
Results may differ from the reference program's by a relative error of at most 0.0021.
Values may be sent and summed in bfloat16 or wider, within the bound.
A program may use at most 128 MiB of HBM per device.

```python
import math
import jax
import jax.numpy as jnp
import numpy as np

BLK = 128
NC = 9216
NT = 2048
TPO = 8
OBS_DEV = 256
TILE_DEV = 2048
MOST = 32
CB_DEV = 9
T_DEV = 128
NOBS = 32768
NTILES = 262144
N_CELL = 8
N_TM = 16


def rising_vector(key, salt):
    key = jax.random.fold_in(key, salt)
    devices = NOBS // OBS_DEV
    position = (jnp.arange(NOBS) // OBS_DEV).astype(jnp.float32) / max(devices - 1, 1)
    values = jax.random.normal(key, (NOBS,), jnp.float32) * (0.6 + 1.2 * position)
    return jnp.clip(values, -8.0, 8.0)


def cov_matrix(key, order, salt):
    key = jax.random.fold_in(key, salt)
    key_scale, key_noise = jax.random.split(key)
    length = max(order / 4.0, 4.0)
    smooth_weight = 6.0 / math.sqrt(length + 4.0)
    ratio = math.exp(-2.0 / length)
    row_energy = 2.0 * ratio / (1.0 - ratio)
    noise_scale = 0.4 / math.sqrt(row_energy)
    scales = jnp.exp(jax.random.uniform(key_scale, (order,), jnp.float32, math.log(0.8), math.log(1.25)))
    position = jnp.arange(order).astype(jnp.float32)
    distance = jnp.abs(position[:, None] - position[None, :])
    decay = jnp.exp(-distance / length)
    identity = jnp.eye(order, dtype=jnp.float32)
    raw = jax.random.normal(key_noise, (order, order), jnp.float32)
    symmetric = jnp.clip((raw + raw.T) * 0.7071, -4.0, 4.0) * (1.0 - identity)
    core = 1.5 * identity + smooth_weight * decay + noise_scale * decay * symmetric
    return (scales[:, None] * core * scales[None, :]).astype(jnp.bfloat16)


def draw_residual(key, part):
    return rising_vector(key, 11)


def draw_direction(key, part):
    return rising_vector(key, 23)


def draw_cell_cov(key, part):
    return cov_matrix(key, NC, 37)


def draw_time_cov(key, part):
    return cov_matrix(key, NT, 41)


def plant(entries, key, low, largest):
    longest = entries.shape.index(max(entries.shape))
    spots = []
    for shift in (0, 1):
        where = [jax.random.randint(jax.random.fold_in(key, axis), (), 0, length) for axis, length in enumerate(entries.shape)]
        where[longest] = (where[longest] + shift) % entries.shape[longest]
        spots.append(tuple(where))
    return entries.at[spots[0]].set(low).at[spots[1]].set(largest)


def level_of(stream_key, shape, shards, least, largest):
    gain = 1.0
    for axis_at, blocks in shards:
        draws = jax.random.uniform(jax.random.fold_in(jax.random.fold_in(stream_key, 6), axis_at), (blocks,), jnp.float32, least / len(shards), largest / len(shards))
        gain = gain * jnp.repeat(jnp.exp(draws), shape[axis_at] // blocks).reshape((-1,) + (1,) * (len(shape) - 1 - axis_at))
    return gain


def deal_out(own_key, own, number, rows, amount, top, limit, lean):
    ranking = jax.random.permutation(own_key, amount)
    packed, ordinary = load_shares(amount, rows * top, limit, lean, True), load_shares(amount, rows * top, limit, lean, False)
    places = jnp.arange(amount)

    def named(sizes, rotation):
        used = int((sizes > 0).sum())
        fixed = max(1, used // 4)
        passed = fixed + (places - fixed + rotation * (used - fixed)) % max(1, amount - fixed)
        return jnp.zeros((amount,), jnp.int32).at[ranking[jnp.where(places < fixed, places, passed)]].set(jnp.asarray(sizes, jnp.int32))

    sizes = jnp.where(number % 4 == 0, named(packed, number // 4), named(ordinary, number - number // 4 - 1))
    mixed = jax.random.permutation(jax.random.fold_in(own, 3), amount)
    giver, sink = mixed[0:amount // 2 * 2:2], mixed[1:amount // 2 * 2:2]
    slack = jnp.minimum(sizes[giver] - 1, limit - sizes[sink]) // 2
    slack = jnp.where((giver == ranking[0]) | (sink == ranking[0]) | (sizes[sink] == 0), 0, jnp.maximum(slack, 0))
    passed = jax.random.randint(jax.random.fold_in(own, 4), (amount // 2,), 0, 1 << 20) % (slack + 1)
    sizes = sizes.at[giver].add(-passed).at[sink].add(passed)
    labels = jnp.searchsorted(jnp.cumsum(sizes), jnp.arange(rows * top), side="right").astype(jnp.int32)
    listing = labels.reshape(top, rows).T
    listing = listing[jax.random.permutation(jax.random.fold_in(own, 1), rows)]
    rotation = jax.random.randint(jax.random.fold_in(own, 2), (rows, 1), 0, top)
    return jnp.take_along_axis(listing, (jnp.arange(top)[None, :] + rotation) % top, axis=1)


def load_shares(amount, total, most, lean, full):
    loads = [(1 << 20) // math.isqrt(rank ** lean) + 1 for rank in range(1, amount + 1)]
    largest = most if full else min(most, max(-(-total // amount), total * loads[0] // sum(loads)))
    least = 1 if total - largest >= amount - 1 else 0
    counts, rest = [largest] + [least] * (amount - 1), total - largest - least * (amount - 1)
    while rest > 0:
        free = [i for i in range(1, amount) if counts[i] < largest] or [i for i in range(1, amount) if counts[i] < most]
        whole, left = sum([loads[i] for i in free]), rest
        for i in free:
            addition = min(most - counts[i], max(1, left * loads[i] // whole), rest)
            counts[i] = counts[i] + addition
            rest = rest - addition
    return np.array(counts)


def noise(rng, shape, deviation, most, cuts=(), kind=jnp.bfloat16):
    gain = level_of(rng, shape, cuts, -0.22, 0.18) if cuts else 1.0
    array = jax.random.normal(rng, shape, jnp.float32) * deviation * gain
    return jnp.minimum(jnp.maximum(array, -most), most).astype(kind)


def setup_inputs(seed: int = 0) -> dict:
    streams_of = jax.random.split(jax.random.key(seed), 12)
    solution = noise(streams_of[0], (NOBS,), 1.0, 6.0, ((0, 128),), jnp.float32)
    residual = draw_residual(jax.random.fold_in(streams_of[11], 71), 0)
    direction = draw_direction(jax.random.fold_in(streams_of[11], 71), 0)
    noise_var = jnp.clip(jnp.exp(math.log(2.0) - 1.3862944 * jax.random.uniform(streams_of[3], (NOBS,), jnp.float32) ** level_of(streams_of[3], (NOBS,), ((0, 128),), -0.2, 0.2)), 0.5, 2.0)
    footprints = noise(streams_of[4], (NTILES, BLK), ((BLK * TPO) ** -0.5), 0.5, ((0, 128),))
    tile_owner_keys = jax.random.split(jax.random.fold_in(streams_of[5], 1), NTILES // TILE_DEV)
    tile_owner_turns = jax.random.permutation(jax.random.fold_in(streams_of[5], 3), NTILES // TILE_DEV)
    tile_owner = jax.vmap(lambda own, number: deal_out(jax.random.fold_in(streams_of[5], 2), own, number, TILE_DEV, N_CELL * N_TM, 1, MOST, 2))(tile_owner_keys, tile_owner_turns).reshape((NTILES, 1))
    tile_block = plant(jax.random.randint(streams_of[6], (NTILES,), 0, CB_DEV), jax.random.fold_in(streams_of[6], 1), 0, CB_DEV - 1).astype(jnp.int32)
    tile_step = plant(jax.random.randint(streams_of[7], (NTILES,), 0, T_DEV), jax.random.fold_in(streams_of[7], 1), 0, T_DEV - 1).astype(jnp.int32)
    tile_obs = plant(jax.random.randint(streams_of[8], (NTILES,), 0, OBS_DEV), jax.random.fold_in(streams_of[8], 1), 0, OBS_DEV - 1).astype(jnp.int32)
    cell_cov = draw_cell_cov(jax.random.fold_in(streams_of[11], 71), 0)
    time_cov = draw_time_cov(jax.random.fold_in(streams_of[11], 71), 0)
    return dict(solution=solution, residual=residual, direction=direction, noise_var=noise_var, footprints=footprints, tile_owner=tile_owner, tile_block=tile_block, tile_step=tile_step, tile_obs=tile_obs, cell_cov=cell_cov, time_cov=time_cov)


def reference(solution, residual, direction, noise_var, footprints, tile_owner, tile_block, tile_step, tile_obs, cell_cov, time_cov):
    cell_local = NC // N_CELL
    time_local = NT // N_TM
    block_local = cell_local // BLK
    owner_dev = tile_owner[:, 0].astype(jnp.int32)
    source_dev = (jnp.arange(NTILES) // TILE_DEV).astype(jnp.int32)
    obs_index = (source_dev * OBS_DEV + tile_obs).astype(jnp.int32)
    dir_tile = direction[obs_index].astype(jnp.bfloat16).astype(jnp.float32)
    global_block = ((owner_dev // N_TM) * block_local + tile_block).astype(jnp.int32)
    global_time = ((owner_dev % N_TM) * time_local + tile_step).astype(jnp.int32)
    tile_values = footprints.astype(jnp.float32)
    flux_time = jnp.zeros((NT, NC // BLK, BLK), jnp.float32)
    flux_time = flux_time.at[global_time, global_block].add(dir_tile[:, None] * tile_values)
    flux_grid = flux_time.reshape(NT, NC).T.astype(jnp.bfloat16)
    mixed_cells = jnp.dot(cell_cov, flux_grid, preferred_element_type=jnp.float32).astype(jnp.bfloat16)
    smoothed = jnp.dot(mixed_cells, time_cov, preferred_element_type=jnp.float32).astype(jnp.bfloat16)
    columns = smoothed.T.reshape(NT, NC // BLK, BLK)[global_time, global_block].astype(jnp.float32)
    tile_dots = jnp.sum(tile_values * columns, axis=1)
    applied = jax.ops.segment_sum(tile_dots, obs_index, num_segments=NOBS) + noise_var * direction
    norm_now = jnp.sum(residual * residual)
    curvature = jnp.sum(direction * applied)
    step_size = norm_now / curvature
    new_solution = solution + step_size * direction
    new_residual = residual - step_size * applied
    norm_next = jnp.sum(new_residual * new_residual)
    new_direction = new_residual + (norm_next / norm_now) * direction
    return (new_solution, new_residual, new_direction)
```

```python
import functools

import jax
import jax.numpy as jnp
from jax import lax
from jax.experimental import pallas as pl
from jax.experimental.pallas import tpu as pltpu
from jax.sharding import PartitionSpec as P

MESH = pl.DeviceIdType.MESH
HIGHEST = lax.Precision.HIGHEST
CELL_TM = ("cell", "tm")
NN = (((1,), (0,)), ((), ()))
NT = (((1,), (1,)), ((), ()))
DEV = 128
CAP = 32
LANES = 128
OBS = 256
TILES = 2048
SLOTS = DEV * CAP
ROWS = 1152
BLOCKS = 9
HALF = ROWS // 2
QUARTER = ROWS // 4
BF16 = jnp.bfloat16
F32 = jnp.float32


def mul(a, b, dims=NN, precision=None):
    return lax.dot_general(a, b, dims, precision=precision, preferred_element_type=F32)


def sub_iota(rows, cols):
    return lax.broadcasted_iota(jnp.int32, (rows, cols), 0)


def hot_of(index, rows):
    return jnp.where(sub_iota(rows, index.shape[1]) == index, 1.0, 0.0)


def prep_kernel(
    owner_ref,
    block_ref,
    step_ref,
    obs_ref,
    dir_ref,
    foot_ref,
    values_ref,
    meta_ref,
    lane_ref,
    slot_vmem,
    slot_smem,
    wide,
    slots,
    sem,
):
    lane_base = (lax.axis_index("cell") * 16 + lax.axis_index("tm")) % 4 * CAP
    width = 256
    above = jnp.where(
        sub_iota(width, width) < lax.broadcasted_iota(jnp.int32, (width, width), 1), 1.0, 0.0
    ).astype(BF16)
    carry = jnp.zeros((DEV, 1), F32)
    ranks = []
    for at in range(0, TILES, width):
        hot = hot_of(owner_ref[:, at : at + width], DEV)
        before = mul(hot.astype(BF16), above) + carry
        ranks.append(jnp.sum(hot * before, axis=0, keepdims=True))
        carry = before[:, width - 1 : width] + hot[:, width - 1 : width]
    rank = jnp.concatenate(ranks, axis=1).astype(jnp.int32)
    slot_vmem[...] = owner_ref[...] * CAP + rank
    copy = pltpu.make_async_copy(slot_vmem, slot_smem, sem)
    copy.start()
    wide[...] = foot_ref[...].astype(F32)
    slots[...] = jnp.zeros_like(slots)
    lane = rank + lane_base
    lane_ref[...] = lane
    owner_hot = hot_of(owner_ref[...], DEV).astype(BF16)
    obs_hot = hot_of(obs_ref[...], OBS).astype(BF16)
    dir_row = jnp.broadcast_to(dir_ref[...], (8, OBS)).astype(BF16)
    dir_tile = mul(dir_row, obs_hot)[0:1, :]
    at_lane = sub_iota(LANES, TILES) == lane

    def placed(value):
        return mul(owner_hot, jnp.where(at_lane, value, 0.0).astype(BF16), NT)

    meta_ref[:, 0, :] = placed(dir_tile)
    meta_ref[:, 1, :] = (
        placed(block_ref[...].astype(F32)) * 128.0 + placed(step_ref[...].astype(F32))
    )
    copy.wait()

    def move(group, _):
        for k in range(8):
            i = group * 8 + k
            slots[pl.ds(slot_smem[0, i], 1), :] = wide[pl.ds(i, 1), :]
        return 0

    lax.fori_loop(0, TILES // 8, move, 0, unroll=4)
    values_ref[...] = slots[...].astype(BF16)


def prep(owner, block, step, obs, direction, footprints):
    return pl.pallas_call(
        prep_kernel,
        out_shape=(
            jax.ShapeDtypeStruct((SLOTS, LANES), BF16),
            jax.ShapeDtypeStruct((DEV, 2, LANES), F32),
            jax.ShapeDtypeStruct((1, TILES), jnp.int32),
        ),
        in_specs=[pl.BlockSpec(memory_space=pltpu.VMEM)] * 6,
        out_specs=(pl.BlockSpec(memory_space=pltpu.VMEM),) * 3,
        scratch_shapes=[
            pltpu.VMEM((1, TILES), jnp.int32),
            pltpu.SMEM((1, TILES), jnp.int32),
            pltpu.VMEM((TILES, LANES), F32),
            pltpu.VMEM((SLOTS, LANES), F32),
            pltpu.SemaphoreType.DMA,
        ],
        name="prep",
    )(owner, block, step, obs, direction, footprints)


def main_kernel(
    sol_ref,
    res_ref,
    dir_ref,
    noise_ref,
    owner_ref,
    obs_ref,
    lane_ref,
    values_ref,
    meta_ref,
    cov_hbm,
    time_ref,
    new_sol_ref,
    new_res_ref,
    new_dir_ref,
    cov,
    got,
    got_meta,
    acc,
    flux,
    mixed,
    mix_a,
    mix_b,
    time_a,
    time_b,
    part_a,
    part_b,
    in_a,
    in_b,
    smooth,
    dots,
    dots_back,
    sums,
    sums_in,
    cov_sem,
    tile_send,
    tile_recv,
    meta_send,
    meta_recv,
    z_send,
    z_recv,
    time_send,
    time_recv,
    ag_send,
    ag_recv,
    rs_send,
    rs_recv,
    back_send,
    back_recv,
    sum_send,
    sum_recv,
):
    cell, tm = lax.axis_index("cell"), lax.axis_index("tm")
    me = cell * 16 + tm
    z, core = cell // 2, cell % 2
    y, x = tm // 4, tm % 4

    def remote(src, dst, send, recv, to_cell, to_tm):
        return pltpu.make_async_remote_copy(
            src_ref=src,
            dst_ref=dst,
            send_sem=send,
            recv_sem=recv,
            device_id=(to_cell, to_tm),
            device_id_type=MESH,
        )

    def arrived(ref, sem):
        pltpu.make_async_copy(ref, ref, sem).wait()

    for k in range(8):
        rows = pl.ds(k * 144, 144)
        pltpu.make_async_copy(cov_hbm.at[rows], cov.at[rows], cov_sem).start()

    def send_tiles(k, _):
        peer = (me + k) % DEV
        remote(
            values_ref.at[peer], got.at[me], tile_send, tile_recv.at[cell], peer // 16, peer % 16
        ).start()
        remote(
            meta_ref.at[peer],
            got_meta.at[me],
            meta_send,
            meta_recv.at[cell],
            peer // 16,
            peer % 16,
        ).start()
        return 0

    lax.fori_loop(1, DEV, send_tiles, 0)
    pltpu.make_async_copy(values_ref.at[me], got.at[me], tile_recv.at[cell]).start()
    pltpu.make_async_copy(meta_ref.at[me], got_meta.at[me], meta_recv.at[cell]).start()

    def x_at(k):
        return (x + k) % 4

    def y_at(k):
        return (y + k) % 4

    def z_cell(k):
        return (z + k) % 4 * 2 + core

    time_sends = []
    for k in (1, 2, 3):
        peer = y_at(k)
        copy = remote(
            time_ref.at[:, pl.ds(pl.multiple_of(peer * 512, 512), 512)],
            time_a.at[y],
            time_send.at[k - 1],
            time_recv.at[k - 1],
            cell,
            peer * 4 + x,
        )
        copy.start()
        time_sends.append(copy)
        peer = x_at(k)
        for other in range(4):
            copy = remote(
                time_ref.at[:, pl.ds(pl.multiple_of((other * 4 + peer) * 128, 128), 128)],
                time_b.at[x, :, pl.ds(other * 128, 128)],
                time_send.at[3 * k + other + (k - 1)],
                time_recv.at[3 * k + other + (k - 1)],
                cell,
                y * 4 + peer,
            )
            copy.start()
            time_sends.append(copy)
    time_a[y] = time_ref[:, pl.ds(pl.multiple_of(y * 512, 512), 512)]
    for other in range(4):
        time_b[x, :, other * 128 : other * 128 + 128] = time_ref[
            :, pl.ds(pl.multiple_of((other * 4 + x) * 128, 128), 128)
        ]

    acc[...] = jnp.zeros_like(acc)
    row_of = sub_iota(LANES, LANES).astype(F32)

    def load_meta(group):
        rows = got_meta[pl.ds(group * 16, 16)]
        return jnp.sum(rows.reshape(4, 4, 2, LANES), axis=1)

    def add_group(k, _):
        group = (cell + k) % 8
        arrived(got.at[pl.ds(group * 16, 16)], tile_recv.at[group])
        arrived(got_meta.at[pl.ds(group * 16, 16)], meta_recv.at[group])
        meta = load_meta(group)
        tiles = got[pl.ds(group * 16, 16)].reshape(512, LANES)
        for b in range(BLOCKS):
            hot = jnp.concatenate(
                [
                    jnp.where(row_of + b * 128.0 == meta[q, 1:2, :], meta[q, 0:1, :], 0.0).astype(
                        BF16
                    )
                    for q in range(4)
                ],
                axis=1,
            )
            acc[b * 128 : b * 128 + 128, :] += mul(hot, tiles)
        return 0

    lax.fori_loop(0, 8, add_group, 0)
    for b in range(BLOCKS):
        flux[cell, :, b * 128 : b * 128 + 128] = acc[b * 128 : b * 128 + 128, :].astype(BF16)

    partner = z * 2 + 1 - core
    up, down, far = z_cell(1), z_cell(3), z_cell(2)
    low, high = pl.ds(0, 64), pl.ds(64, 64)
    z_copies = []

    def z_go(block, rows, to_cell, at):
        ref = flux.at[block, rows]
        copy = remote(ref, ref, z_send.at[at], z_recv.at[at], to_cell, tm)
        copy.start()
        z_copies.append(copy)

    def z_wait(block, rows, at):
        arrived(flux.at[block, rows], z_recv.at[at])

    full = pl.ds(0, 128)
    z_go(cell, full, up, 0)
    z_go(cell, full, down, 1)
    z_go(cell, full, partner, 2)

    arrived(cov, cov_sem)

    def other_core(c):
        return c // 2 * 2 + 1 - c % 2

    def mix(block, first=False):
        cols = pl.ds(pl.multiple_of(block * ROWS, 128), ROWS)
        product = mul(cov[:, cols], flux[block], NT)
        if first:
            mixed[...] = product
        else:
            mixed[...] += product

    z_wait(down, full, 0)
    z_go(down, low, up, 3)
    z_go(down, full, partner, 4)
    z_wait(up, full, 1)
    z_go(up, high, down, 5)
    z_go(up, full, partner, 6)
    mix(cell, True)
    z_wait(far, low, 3)
    z_go(far, low, partner, 7)
    z_wait(far, high, 5)
    z_go(far, high, partner, 8)
    mix(down)
    mix(up)
    z_wait(other_core(cell), full, 2)
    mix(other_core(cell))
    z_wait(other_core(down), full, 4)
    mix(other_core(down))
    z_wait(other_core(up), full, 6)
    mix(other_core(up))
    mix(far)
    z_wait(other_core(far), low, 7)
    z_wait(other_core(far), high, 8)
    mix(other_core(far))

    mix_a[:, pl.ds(pl.multiple_of(x * 128, 128), 128)] = mixed[:HALF, :].astype(BF16)
    mix_b[:, pl.ds(pl.multiple_of(y * 128, 128), 128)] = mixed[HALF:, :].astype(BF16)
    ag_copies = []

    def ag_go(buf, at_lane, rows, to_tm, at):
        ref = buf.at[rows, pl.ds(pl.multiple_of(at_lane * 128, 128), 128)]
        copy = remote(ref, ref, ag_send.at[at], ag_recv.at[at], cell, to_tm)
        copy.start()
        ag_copies.append(copy)

    def ag_wait(buf, at_lane, rows, at):
        arrived(buf.at[rows, pl.ds(pl.multiple_of(at_lane * 128, 128), 128)], ag_recv.at[at])

    every, first, second = pl.ds(0, HALF), pl.ds(0, QUARTER), pl.ds(QUARTER, QUARTER)
    x_up, x_down = y * 4 + x_at(1), y * 4 + x_at(3)
    y_up, y_down = y_at(1) * 4 + x, y_at(3) * 4 + x
    ag_go(mix_a, x, every, x_up, 0)
    ag_go(mix_a, x, every, x_down, 1)
    ag_go(mix_b, y, every, y_up, 2)
    ag_go(mix_b, y, every, y_down, 3)
    ag_wait(mix_a, x_at(3), every, 0)
    ag_go(mix_a, x_at(3), first, x_up, 4)
    ag_wait(mix_a, x_at(1), every, 1)
    ag_go(mix_a, x_at(1), second, x_down, 5)
    ag_wait(mix_b, y_at(3), every, 2)
    ag_go(mix_b, y_at(3), first, y_up, 6)
    ag_wait(mix_b, y_at(1), every, 3)
    ag_go(mix_b, y_at(1), second, y_down, 7)
    for k in (1, 2, 3):
        arrived(time_a.at[y_at(4 - k)], time_recv.at[k - 1])
        for other in range(4):
            arrived(
                time_b.at[x_at(4 - k), :, pl.ds(other * 128, 128)],
                time_recv.at[3 * k + other + (k - 1)],
            )
    ag_wait(mix_a, x_at(2), first, 4)
    ag_wait(mix_a, x_at(2), second, 5)
    rs_copies = []
    for k in (2, 1, 3):
        peer = y_at(k)
        part_a[k - 1] = mul(mix_a[...], time_a[peer], NT).astype(BF16)
        copy = remote(
            part_a.at[k - 1],
            in_a.at[k - 1],
            rs_send.at[k - 1],
            rs_recv.at[k - 1],
            cell,
            peer * 4 + x,
        )
        copy.start()
        rs_copies.append(copy)
    ag_wait(mix_b, y_at(2), first, 6)
    ag_wait(mix_b, y_at(2), second, 7)
    for k in (2, 1, 3):
        peer = x_at(k)
        part_b[k - 1] = mul(mix_b[...], time_b[peer], NT).astype(BF16)
        copy = remote(
            part_b.at[k - 1],
            in_b.at[k - 1],
            rs_send.at[k + 2],
            rs_recv.at[k + 2],
            cell,
            y * 4 + peer,
        )
        copy.start()
        rs_copies.append(copy)
    mixed[:HALF, :] = mul(mix_a[...], time_a[y], NT)
    mixed[HALF:, :] = mul(mix_b[...], time_b[x], NT)
    for k in (1, 3, 2):
        arrived(in_a.at[k - 1], rs_recv.at[k - 1])
        mixed[:HALF, :] += in_a[k - 1].astype(F32)
        arrived(in_b.at[k - 1], rs_recv.at[k + 2])
        mixed[HALF:, :] += in_b[k - 1].astype(F32)
    for b in range(BLOCKS):
        smooth[b] = mixed[b * 128 : b * 128 + 128, :].T.astype(BF16)

    def dot_group(k, _):
        group = (cell + k) % 8
        meta = load_meta(group)
        tiles = got[pl.ds(group * 16, 16)].reshape(512, LANES)
        picked = [jnp.zeros((LANES, LANES), F32) for _ in range(4)]
        for b in range(BLOCKS):
            product = mul(smooth[b], tiles, NT)
            for q in range(4):
                picked[q] += jnp.where(
                    row_of + b * 128.0 == meta[q, 1:2, :],
                    product[:, q * 128 : q * 128 + 128],
                    0.0,
                )
        for q in range(4):
            dots[group * 4 + q] = jnp.sum(picked[q], axis=0, keepdims=True)
        return 0

    lax.fori_loop(0, 8, dot_group, 0)

    def send_back(k, _):
        peer = (me + k) % DEV
        remote(
            dots.at[peer // 4], dots_back.at[me], back_send, back_recv, peer // 16, peer % 16
        ).start()
        return 0

    lax.fori_loop(1, DEV, send_back, 0)
    dots_back[me] = dots[me // 4]
    owner_hot = hot_of(owner_ref[...], DEV)
    obs_hot = hot_of(obs_ref[...], OBS)
    pltpu.make_async_copy(
        dots_back.at[pl.ds(0, DEV - 1)], dots_back.at[pl.ds(0, DEV - 1)], back_recv
    ).wait()
    by_lane = mul(dots_back[:, 0, :].T, owner_hot, precision=HIGHEST)
    tile_dots = jnp.sum(
        jnp.where(sub_iota(LANES, TILES) == lane_ref[...], by_lane, 0.0), axis=0, keepdims=True
    )
    direction, residual = dir_ref[...], res_ref[...]
    applied = mul(jnp.broadcast_to(tile_dots, (8, TILES)), obs_hot, NT, HIGHEST)[0:1, :]
    applied = applied + noise_ref[...] * direction

    lanes = lax.broadcasted_iota(jnp.int32, (1, LANES), 1)
    row = jnp.zeros((1, LANES), F32)
    for at, value in enumerate(
        (residual * residual, direction * applied, residual * applied, applied * applied)
    ):
        row = jnp.where(lanes == at, jnp.sum(value, axis=1, keepdims=True), row)
    sums[...] = row

    def send_sums(k, _):
        peer = (me + k) % DEV
        remote(sums, sums_in.at[me], sum_send, sum_recv, peer // 16, peer % 16).start()
        return 0

    lax.fori_loop(1, DEV, send_sums, 0)
    sums_in[me] = row
    pltpu.make_async_copy(
        sums_in.at[pl.ds(0, DEV - 1)], sums_in.at[pl.ds(0, DEV - 1)], sum_recv
    ).wait()
    total = jnp.sum(sums_in[...], axis=0)

    def total_of(at):
        return jnp.sum(jnp.where(lanes == at, total, 0.0), axis=1, keepdims=True)

    norm_now, curvature, cross_term, image_norm = (total_of(at) for at in range(4))
    step_size = norm_now / curvature
    new_res = residual - step_size * applied
    norm_next = norm_now - 2.0 * step_size * cross_term + step_size * step_size * image_norm
    new_sol_ref[...] = sol_ref[...] + step_size * direction
    new_res_ref[...] = new_res
    new_dir_ref[...] = new_res + norm_next / norm_now * direction

    arrived(values_ref.at[pl.ds(0, DEV - 1)], tile_send)
    arrived(meta_ref.at[pl.ds(0, DEV - 1)], meta_send)
    for copy in time_sends + z_copies + ag_copies + rs_copies:
        copy.wait_send()
    arrived(dots_back.at[pl.ds(0, DEV - 1)], back_send)
    arrived(sums_in.at[pl.ds(0, DEV - 1)], sum_send)


def whole(*operands):
    vmem = pl.BlockSpec(memory_space=pltpu.VMEM)
    dma = pltpu.SemaphoreType.DMA
    row = jax.ShapeDtypeStruct((1, OBS), F32)
    return pl.pallas_call(
        main_kernel,
        out_shape=(row, row, row),
        in_specs=[vmem] * 9 + [pl.BlockSpec(memory_space=pl.ANY), vmem],
        out_specs=(vmem, vmem, vmem),
        scratch_shapes=[
            pltpu.VMEM((ROWS, 8 * ROWS), BF16),
            pltpu.VMEM((DEV, CAP, LANES), BF16),
            pltpu.VMEM((DEV, 2, LANES), F32),
            pltpu.VMEM((ROWS, LANES), F32),
            pltpu.VMEM((8, LANES, ROWS), BF16),
            pltpu.VMEM((ROWS, LANES), F32),
            pltpu.VMEM((HALF, 512), BF16),
            pltpu.VMEM((HALF, 512), BF16),
            pltpu.VMEM((4, LANES, 512), BF16),
            pltpu.VMEM((4, LANES, 512), BF16),
            pltpu.VMEM((3, HALF, LANES), BF16),
            pltpu.VMEM((3, HALF, LANES), BF16),
            pltpu.VMEM((3, HALF, LANES), BF16),
            pltpu.VMEM((3, HALF, LANES), BF16),
            pltpu.VMEM((BLOCKS, LANES, LANES), BF16),
            pltpu.VMEM((DEV // 4, 1, LANES), F32),
            pltpu.VMEM((DEV, 1, LANES), F32),
            pltpu.VMEM((1, LANES), F32),
            pltpu.VMEM((DEV, 1, LANES), F32),
            dma,
            dma,
            dma((8,)),
            dma,
            dma((8,)),
            dma((9,)),
            dma((9,)),
            dma((15,)),
            dma((15,)),
            dma((8,)),
            dma((8,)),
            dma((6,)),
            dma((6,)),
            dma,
            dma,
            dma,
            dma,
        ],
        compiler_params=pltpu.CompilerParams(has_side_effects=True, vmem_limit_bytes=60 * 2**20),
        name="whole",
    )(*operands)


def local(
    solution,
    residual,
    direction,
    noise_var,
    footprints,
    tile_owner,
    tile_block,
    tile_step,
    tile_obs,
    cell_cov,
    time_cov,
):
    row = functools.partial(jnp.reshape, shape=(1, OBS))
    tile_row = functools.partial(jnp.reshape, shape=(1, TILES))
    owner, obs = tile_row(tile_owner), tile_row(tile_obs)
    values, meta, lane = prep(
        owner, tile_row(tile_block), tile_row(tile_step), obs, row(direction), footprints
    )
    outs = whole(
        row(solution),
        row(residual),
        row(direction),
        row(noise_var),
        owner,
        obs,
        lane,
        values.reshape(DEV, CAP, LANES),
        meta,
        cell_cov,
        time_cov,
    )
    return tuple(out.reshape(OBS) for out in outs)


def solution(mesh):
    both = P(CELL_TM)
    in_specs = (both,) * 4 + (P(CELL_TM, None),) * 2 + (both,) * 3
    in_specs += (P("cell", None), P("tm", None))
    return jax.shard_map(
        local, mesh=mesh, in_specs=in_specs, out_specs=(both,) * 3, check_vma=False
    )
```

```python
import functools

import jax
import jax.numpy as jnp
from jax import lax
from jax.experimental import pallas as pl
from jax.experimental.pallas import tpu as pltpu
from jax.sharding import PartitionSpec as P

MESH = pl.DeviceIdType.MESH
CELL_TM = ("cell", "tm")
NN = (((1,), (0,)), ((), ()))
NT = (((1,), (1,)), ((), ()))
DEV = 128
CAP = 32
LANES = 128
OBS = 256
TILES = 2048
SLOTS = DEV * CAP
ROWS = 1152
BLOCKS = 9
HALF = ROWS // 2
QUARTER = ROWS // 4
BF16 = jnp.bfloat16
F32 = jnp.float32


def mul(a, b, dims=NN):
    return lax.dot_general(a, b, dims, preferred_element_type=F32)


def sub_iota(rows, cols):
    return lax.broadcasted_iota(jnp.int32, (rows, cols), 0)


def hot_of(index, rows):
    return jnp.where(sub_iota(rows, index.shape[1]) == index, 1.0, 0.0)


def split3(value):
    high = value.astype(BF16)
    rest = value - high.astype(F32)
    middle = rest.astype(BF16)
    return high, middle, (rest - middle.astype(F32)).astype(BF16)


def main_kernel(
    res_ref,
    dir_ref,
    noise_ref,
    owner_ref,
    block_ref,
    step_ref,
    obs_ref,
    foot_ref,
    cov_hbm,
    time_ref,
    out_ref,
    rank_row,
    index_vmem,
    index_smem,
    wide,
    slots,
    values,
    meta,
    cov,
    got,
    got_meta,
    acc,
    flux,
    mixed,
    mix_a,
    mix_b,
    time_a,
    time_b,
    part_a,
    part_b,
    in_a,
    in_b,
    smooth,
    dots,
    dots_back,
    by_rank,
    sums,
    sums_in,
    index_sem,
    cov_sem,
    tile_send,
    tile_recv,
    meta_send,
    meta_recv,
    z_send,
    z_recv,
    time_send,
    time_recv,
    ag_send,
    ag_recv,
    rs_send,
    rs_recv,
    back_send,
    back_recv,
    sum_send,
    sum_recv,
):
    cell, tm = lax.axis_index("cell"), lax.axis_index("tm")
    me = cell * 16 + tm
    z, core = cell // 2, cell % 2
    y, x = tm // 4, tm % 4
    xs = [(x + k) % 4 for k in range(4)]
    ys = [(y + k) % 4 for k in range(4)]
    far_first = sorted(
        ((dy, dx) for dy in range(4) for dx in range(4)),
        key=lambda at: -(min(at[0], 4 - at[0]) + min(at[1], 4 - at[1])),
    )
    planes = [ys[dy] * 4 + xs[dx] for dy, dx in far_first]

    def x_at(k):
        return xs[k]

    def y_at(k):
        return ys[k]

    def z_cell(k):
        return (z + k) % 4 * 2 + core

    def remote(src, dst, send, recv, to_cell, to_tm):
        return pltpu.make_async_remote_copy(
            src_ref=src,
            dst_ref=dst,
            send_sem=send,
            recv_sem=recv,
            device_id=(to_cell, to_tm),
            device_id_type=MESH,
        )

    def arrived(ref, sem):
        pltpu.make_async_copy(ref, ref, sem).wait()

    def to_others(send):
        def at_cell(k, _):
            to_cell = (cell + 4 + k) % 8
            for to_tm in planes[:15]:
                send(to_cell, to_tm)

            @pl.when(k != 4)
            def _():
                send(to_cell, planes[15])

            return 0

        lax.fori_loop(0, 8, at_cell, 0)

    barrier = pltpu.get_barrier_semaphore()
    to_others(
        lambda to_cell, to_tm: pl.semaphore_signal(
            barrier, inc=1, device_id=(to_cell, to_tm), device_id_type=MESH
        )
    )
    for k in range(8):
        rows = pl.ds(k * 144, 144)
        pltpu.make_async_copy(cov_hbm.at[rows], cov.at[rows], cov_sem).start()

    width = 256
    above = jnp.where(
        sub_iota(width, width) < lax.broadcasted_iota(jnp.int32, (width, width), 1), 1.0, 0.0
    ).astype(BF16)
    carry = jnp.zeros((DEV, 1), F32)
    for at in range(0, TILES, width):
        hot = hot_of(owner_ref[:, at : at + width], DEV)
        before = mul(hot.astype(BF16), above) + carry
        rank_row[:, at : at + width] = jnp.sum(hot * before, axis=0, keepdims=True)
        carry = before[:, width - 1 : width] + hot[:, width - 1 : width]
    owner_hot = hot_of(owner_ref[...], DEV).astype(BF16)
    in_slot = sub_iota(CAP, TILES).astype(F32) == rank_row[...]
    tile = lax.broadcasted_iota(jnp.int32, (1, TILES), 1)

    def placed(*rows):
        placings = [jnp.where(in_slot, row, 0.0).astype(BF16) for row in rows]
        return mul(owner_hot, jnp.concatenate(placings, axis=0), NT)

    index = placed((tile // 256).astype(F32), (tile % 256).astype(F32))
    index = (index[:, :CAP] * 256.0 + index[:, CAP:]).astype(jnp.int32)
    index_vmem[...] = jnp.concatenate([index] * 4, axis=1)
    index_copy = pltpu.make_async_copy(index_vmem, index_smem, index_sem)
    index_copy.start()
    wide[...] = foot_ref[...].astype(F32)
    obs_hot = hot_of(obs_ref[...], OBS).astype(BF16)
    dir_tile = mul(jnp.broadcast_to(dir_ref[...], (8, OBS)).astype(BF16), obs_hot)[0:1, :]
    fields = placed(dir_tile, block_ref[...].astype(F32), step_ref[...].astype(F32)).astype(BF16)
    lane_base = x * CAP
    shift = jnp.where(
        sub_iota(CAP, LANES) + lane_base == lax.broadcasted_iota(jnp.int32, (CAP, LANES), 1),
        1.0,
        0.0,
    ).astype(BF16)
    meta[:, 0, :] = mul(fields[:, :CAP], shift)
    meta[:, 1, :] = (
        mul(fields[:, CAP : 2 * CAP], shift) * 128.0 + mul(fields[:, 2 * CAP :], shift)
    )
    index_copy.wait()

    def gather(owner, _):
        for k in range(CAP):
            at = jnp.minimum(jnp.maximum(index_smem[owner, k], 0), TILES - 1)
            slots[pl.ds(owner * CAP + k, 1), :] = wide[pl.ds(at, 1), :]
        return 0

    lax.fori_loop(0, DEV, gather, 0)
    values[...] = slots[...].reshape(DEV, CAP, LANES).astype(BF16)
    pl.semaphore_wait(barrier, DEV - 1)

    def send_tile(to_cell, to_tm):
        peer = to_cell * 16 + to_tm
        remote(
            values.at[peer], got.at[me], tile_send, tile_recv.at[cell], to_cell, to_tm
        ).start()
        remote(
            meta.at[peer], got_meta.at[me], meta_send, meta_recv.at[cell], to_cell, to_tm
        ).start()

    to_others(send_tile)
    pltpu.make_async_copy(values.at[me], got.at[me], tile_recv.at[cell]).start()
    pltpu.make_async_copy(meta.at[me], got_meta.at[me], meta_recv.at[cell]).start()

    acc[...] = jnp.zeros_like(acc)
    row_of = sub_iota(LANES, LANES).astype(F32)

    def load_meta(group):
        rows = got_meta[pl.ds(group * 16, 16)]
        return jnp.sum(rows.reshape(4, 4, 2, LANES), axis=1)

    def add_group(k, _):
        group = (cell + 12 - k) % 8
        arrived(got.at[pl.ds(group * 16, 16)], tile_recv.at[group])
        arrived(got_meta.at[pl.ds(group * 16, 16)], meta_recv.at[group])
        rows = load_meta(group)
        tiles = got[pl.ds(group * 16, 16)].reshape(512, LANES)
        for b in range(BLOCKS):
            hot = jnp.concatenate(
                [
                    jnp.where(row_of + b * 128.0 == rows[q, 1:2, :], rows[q, 0:1, :], 0.0).astype(
                        BF16
                    )
                    for q in range(4)
                ],
                axis=1,
            )
            acc[b * 128 : b * 128 + 128, :] += mul(hot, tiles)
        return 0

    lax.fori_loop(0, 8, add_group, 0)
    for b in range(BLOCKS):
        flux[cell, :, b * 128 : b * 128 + 128] = acc[b * 128 : b * 128 + 128, :].astype(BF16)

    partner = z * 2 + 1 - core
    up, down, far = z_cell(1), z_cell(3), z_cell(2)
    left, right, full = pl.ds(0, 512), pl.ds(512, ROWS - 512), pl.ds(0, ROWS)
    z_copies = []

    def z_go(block, cols, to_cell, at):
        ref = flux.at[block, :, cols]
        copy = remote(ref, ref, z_send.at[at], z_recv.at[at], to_cell, tm)
        copy.start()
        z_copies.append(copy)

    def z_wait(block, cols, at):
        arrived(flux.at[block, :, cols], z_recv.at[at])

    z_go(cell, left, up, 0)
    z_go(cell, right, down, 2)
    z_go(cell, right, up, 1)
    z_go(cell, left, down, 3)
    z_go(cell, full, partner, 4)

    time_sends = []
    for k in (1, 2, 3):
        peer = y_at(k)
        copy = remote(
            time_ref.at[:, pl.ds(pl.multiple_of(peer * 512, 512), 512)],
            time_a.at[y],
            time_send.at[k - 1],
            time_recv.at[k - 1],
            cell,
            peer * 4 + x,
        )
        copy.start()
        time_sends.append(copy)
        peer = x_at(k)
        for other in range(4):
            copy = remote(
                time_ref.at[:, pl.ds(pl.multiple_of((other * 4 + peer) * 128, 128), 128)],
                time_b.at[x, :, pl.ds(other * 128, 128)],
                time_send.at[3 * k + other + (k - 1)],
                time_recv.at[3 * k + other + (k - 1)],
                cell,
                y * 4 + peer,
            )
            copy.start()
            time_sends.append(copy)
    time_a[y] = time_ref[:, pl.ds(pl.multiple_of(y * 512, 512), 512)]
    for other in range(4):
        time_b[x, :, other * 128 : other * 128 + 128] = time_ref[
            :, pl.ds(pl.multiple_of((other * 4 + x) * 128, 128), 128)
        ]

    arrived(cov, cov_sem)

    def other_core(c):
        return c // 2 * 2 + 1 - c % 2

    def mix(block, first=False):
        cols = pl.ds(pl.multiple_of(block * ROWS, 128), ROWS)
        product = mul(cov[:, cols], flux[block], NT)
        if first:
            mixed[...] = product
        else:
            mixed[...] += product

    mix(cell, True)
    z_wait(down, left, 0)
    z_go(down, left, up, 5)
    z_go(down, left, partner, 7)
    z_wait(up, right, 2)
    z_go(up, right, down, 6)
    z_go(up, right, partner, 8)
    z_wait(other_core(cell), full, 4)
    mix(other_core(cell))
    z_wait(down, right, 1)
    z_go(down, right, partner, 9)
    z_wait(up, left, 3)
    z_go(up, left, partner, 10)
    mix(down)
    mix(up)
    z_wait(other_core(down), left, 7)
    z_wait(other_core(down), right, 9)
    mix(other_core(down))
    z_wait(other_core(up), right, 8)
    z_wait(other_core(up), left, 10)
    mix(other_core(up))
    z_wait(far, left, 5)
    z_go(far, left, partner, 11)
    z_wait(far, right, 6)
    z_go(far, right, partner, 12)
    mix(far)
    z_wait(other_core(far), left, 11)
    z_wait(other_core(far), right, 12)
    mix(other_core(far))

    mix_a[:, pl.ds(pl.multiple_of(x * 128, 128), 128)] = mixed[:HALF, :].astype(BF16)
    mix_b[:, pl.ds(pl.multiple_of(y * 128, 128), 128)] = mixed[HALF:, :].astype(BF16)
    ag_copies = []

    def ag_go(buf, at_lane, rows, to_tm, at):
        ref = buf.at[rows, pl.ds(pl.multiple_of(at_lane * 128, 128), 128)]
        copy = remote(ref, ref, ag_send.at[at], ag_recv.at[at], cell, to_tm)
        copy.start()
        ag_copies.append(copy)

    def ag_wait(buf, at_lane, rows, at):
        arrived(buf.at[rows, pl.ds(pl.multiple_of(at_lane * 128, 128), 128)], ag_recv.at[at])

    first, second = pl.ds(0, QUARTER), pl.ds(QUARTER, QUARTER)
    x_up, x_down = y * 4 + x_at(1), y * 4 + x_at(3)
    y_up, y_down = y_at(1) * 4 + x, y_at(3) * 4 + x
    ag_go(mix_a, x, first, x_up, 0)
    ag_go(mix_a, x, second, x_down, 1)
    ag_go(mix_b, y, first, y_up, 2)
    ag_go(mix_b, y, second, y_down, 3)
    ag_go(mix_a, x, second, x_up, 4)
    ag_go(mix_a, x, first, x_down, 5)
    ag_go(mix_b, y, second, y_up, 6)
    ag_go(mix_b, y, first, y_down, 7)
    ag_wait(mix_a, x_at(3), first, 0)
    ag_go(mix_a, x_at(3), first, x_up, 8)
    ag_wait(mix_a, x_at(1), second, 1)
    ag_go(mix_a, x_at(1), second, x_down, 9)
    ag_wait(mix_b, y_at(3), first, 2)
    ag_go(mix_b, y_at(3), first, y_up, 10)
    ag_wait(mix_b, y_at(1), second, 3)
    ag_go(mix_b, y_at(1), second, y_down, 11)
    for k in (1, 2, 3):
        arrived(time_a.at[y_at(4 - k)], time_recv.at[k - 1])
        for other in range(4):
            arrived(
                time_b.at[x_at(4 - k), :, pl.ds(other * 128, 128)],
                time_recv.at[3 * k + other + (k - 1)],
            )
    ag_wait(mix_a, x_at(3), second, 4)
    ag_wait(mix_a, x_at(1), first, 5)
    ag_wait(mix_b, y_at(3), second, 6)
    ag_wait(mix_b, y_at(1), first, 7)
    ag_wait(mix_a, x_at(2), first, 8)
    ag_wait(mix_a, x_at(2), second, 9)
    rs_copies = []
    for k in (2, 1, 3):
        peer = y_at(k)
        part_a[k - 1] = mul(mix_a[...], time_a[peer], NT).astype(BF16)
        copy = remote(
            part_a.at[k - 1],
            in_a.at[k - 1],
            rs_send.at[k - 1],
            rs_recv.at[k - 1],
            cell,
            peer * 4 + x,
        )
        copy.start()
        rs_copies.append(copy)
        if k == 2:
            ag_wait(mix_b, y_at(2), first, 10)
            ag_wait(mix_b, y_at(2), second, 11)
        peer = x_at(k)
        part_b[k - 1] = mul(mix_b[...], time_b[peer], NT).astype(BF16)
        copy = remote(
            part_b.at[k - 1],
            in_b.at[k - 1],
            rs_send.at[k + 2],
            rs_recv.at[k + 2],
            cell,
            y * 4 + peer,
        )
        copy.start()
        rs_copies.append(copy)
    mixed[:HALF, :] = mul(mix_a[...], time_a[y], NT)
    mixed[HALF:, :] = mul(mix_b[...], time_b[x], NT)
    for k in (1, 3, 2):
        arrived(in_a.at[k - 1], rs_recv.at[k - 1])
        mixed[:HALF, :] += in_a[k - 1].astype(F32)
        arrived(in_b.at[k - 1], rs_recv.at[k + 2])
        mixed[HALF:, :] += in_b[k - 1].astype(F32)
    for b in range(BLOCKS):
        smooth[b] = mixed[b * 128 : b * 128 + 128, :].T.astype(BF16)

    def dot_group(k, _):
        group = (cell + 4 + k) % 8
        rows = load_meta(group)
        tiles = got[pl.ds(group * 16, 16)].reshape(512, LANES)
        picked = [jnp.zeros((LANES, LANES), F32) for _ in range(4)]
        for b in range(BLOCKS):
            product = mul(smooth[b], tiles, NT)
            for q in range(4):
                picked[q] += jnp.where(
                    row_of + b * 128.0 == rows[q, 1:2, :],
                    product[:, q * 128 : q * 128 + 128],
                    0.0,
                )
        for q in range(4):
            dots[group * 4 + q] = jnp.sum(picked[q], axis=0, keepdims=True)

        def send_dots(to_tm):
            remote(
                dots.at[group * 4 + to_tm // 4],
                dots_back.at[me],
                back_send,
                back_recv,
                group,
                to_tm,
            ).start()

        for to_tm in planes[:15]:
            send_dots(to_tm)

        @pl.when(k != 4)
        def _():
            send_dots(planes[15])

        return 0

    lax.fori_loop(0, 8, dot_group, 0)
    dots_back[me] = dots[me // 4]
    owner_hot = hot_of(owner_ref[...], DEV).astype(BF16)
    obs_hot = hot_of(obs_ref[...], OBS).astype(BF16)
    in_slot = sub_iota(CAP, TILES).astype(F32) == rank_row[...]
    arrived(dots_back.at[pl.ds(0, DEV - 1)], back_recv)
    by_rank[...] = dots_back[:, 0, :].T
    own = jnp.concatenate(split3(by_rank[pl.ds(pl.multiple_of(lane_base, CAP), CAP), :]), axis=0)
    parts = mul(own, owner_hot)
    tile_dots = jnp.sum(
        jnp.where(in_slot, parts[:CAP] + parts[CAP : 2 * CAP] + parts[2 * CAP :], 0.0),
        axis=0,
        keepdims=True,
    )
    high, middle, low = split3(tile_dots)
    three = jnp.concatenate(
        [high.astype(F32), middle.astype(F32), low.astype(F32), jnp.zeros((5, TILES), F32)], axis=0
    ).astype(BF16)
    direction, residual = dir_ref[...], res_ref[...]
    applied = jnp.sum(mul(three, obs_hot, NT), axis=0, keepdims=True)
    applied = applied + noise_ref[...] * direction

    lanes = lax.broadcasted_iota(jnp.int32, (1, LANES), 1)
    row = jnp.zeros((1, LANES), F32)
    for at, value in enumerate(
        (residual * residual, direction * applied, residual * applied, applied * applied)
    ):
        row = jnp.where(lanes == at, jnp.sum(value, axis=1, keepdims=True), row)
    sums[...] = row
    to_others(
        lambda to_cell, to_tm: remote(
            sums, sums_in.at[me], sum_send, sum_recv, to_cell, to_tm
        ).start()
    )
    sums_in[me] = row
    arrived(sums_in.at[pl.ds(0, DEV - 1)], sum_recv)
    total = jnp.sum(sums_in[...], axis=0)

    def total_of(at):
        return jnp.sum(jnp.where(lanes == at, total, 0.0), axis=1, keepdims=True)

    norm_now, curvature, cross_term, image_norm = (total_of(at) for at in range(4))
    step_size = norm_now / curvature
    norm_next = norm_now - 2.0 * step_size * cross_term + step_size * step_size * image_norm
    out_ref[0:1, :] = applied
    out_ref[1:2, :] = jnp.broadcast_to(step_size, (1, OBS))
    out_ref[2:3, :] = jnp.broadcast_to(norm_next / norm_now, (1, OBS))

    arrived(values.at[pl.ds(0, DEV - 1)], tile_send)
    arrived(meta.at[pl.ds(0, DEV - 1)], meta_send)
    for copy in time_sends + z_copies + ag_copies + rs_copies:
        copy.wait_send()
    arrived(dots_back.at[pl.ds(0, DEV - 1)], back_send)
    arrived(sums_in.at[pl.ds(0, DEV - 1)], sum_send)


def whole(*operands):
    vmem = pl.BlockSpec(memory_space=pltpu.VMEM)
    dma = pltpu.SemaphoreType.DMA
    return pl.pallas_call(
        main_kernel,
        out_shape=jax.ShapeDtypeStruct((3, OBS), F32),
        in_specs=[vmem] * 8 + [pl.BlockSpec(memory_space=pl.ANY), vmem],
        out_specs=vmem,
        scratch_shapes=[
            pltpu.VMEM((1, TILES), F32),
            pltpu.VMEM((DEV, LANES), jnp.int32),
            pltpu.SMEM((DEV, LANES), jnp.int32),
            pltpu.VMEM((TILES, LANES), F32),
            pltpu.VMEM((SLOTS, LANES), F32),
            pltpu.VMEM((DEV, CAP, LANES), BF16),
            pltpu.VMEM((DEV, 2, LANES), F32),
            pltpu.VMEM((ROWS, 8 * ROWS), BF16),
            pltpu.VMEM((DEV, CAP, LANES), BF16),
            pltpu.VMEM((DEV, 2, LANES), F32),
            pltpu.VMEM((ROWS, LANES), F32),
            pltpu.VMEM((8, LANES, ROWS), BF16),
            pltpu.VMEM((ROWS, LANES), F32),
            pltpu.VMEM((HALF, 512), BF16),
            pltpu.VMEM((HALF, 512), BF16),
            pltpu.VMEM((4, LANES, 512), BF16),
            pltpu.VMEM((4, LANES, 512), BF16),
            pltpu.VMEM((3, HALF, LANES), BF16),
            pltpu.VMEM((3, HALF, LANES), BF16),
            pltpu.VMEM((3, HALF, LANES), BF16),
            pltpu.VMEM((3, HALF, LANES), BF16),
            pltpu.VMEM((BLOCKS, LANES, LANES), BF16),
            pltpu.VMEM((DEV // 4, 1, LANES), F32),
            pltpu.VMEM((DEV, 1, LANES), F32),
            pltpu.VMEM((LANES, DEV), F32),
            pltpu.VMEM((1, LANES), F32),
            pltpu.VMEM((DEV, 1, LANES), F32),
            dma,
            dma,
            dma,
            dma((8,)),
            dma,
            dma((8,)),
            dma((13,)),
            dma((13,)),
            dma((15,)),
            dma((15,)),
            dma((12,)),
            dma((12,)),
            dma((6,)),
            dma((6,)),
            dma,
            dma,
            dma,
            dma,
        ],
        compiler_params=pltpu.CompilerParams(
            collective_id=0, has_side_effects=True, vmem_limit_bytes=60 * 2**20
        ),
        name="whole",
    )(*operands)


def local(
    solution,
    residual,
    direction,
    noise_var,
    footprints,
    tile_owner,
    tile_block,
    tile_step,
    tile_obs,
    cell_cov,
    time_cov,
):
    row = functools.partial(jnp.reshape, shape=(1, OBS))
    tile_row = functools.partial(jnp.reshape, shape=(1, TILES))
    applied, step_size, ratio = whole(
        row(residual),
        row(direction),
        row(noise_var),
        tile_row(tile_owner),
        tile_row(tile_block),
        tile_row(tile_step),
        tile_row(tile_obs),
        footprints,
        cell_cov,
        time_cov,
    )
    new_residual = residual - step_size * applied
    return solution + step_size * direction, new_residual, new_residual + ratio * direction


def solution(mesh):
    both = P(CELL_TM)
    in_specs = (both,) * 4 + (P(CELL_TM, None),) * 2 + (both,) * 3
    in_specs += (P("cell", None), P("tm", None))
    return jax.shard_map(
        local, mesh=mesh, in_specs=in_specs, out_specs=(both,) * 3, check_vma=False
    )
```

```python
import functools

import jax
import jax.numpy as jnp
from jax import lax
from jax.experimental import pallas as pl
from jax.experimental.pallas import tpu as pltpu
from jax.sharding import PartitionSpec as P

MESH = pl.DeviceIdType.MESH
CELL_TM = ("cell", "tm")
NN = (((1,), (0,)), ((), ()))
NT = (((1,), (1,)), ((), ()))
DEV = 128
CAP = 32
LANES = 128
OBS = 256
TILES = 2048
SLOTS = DEV * CAP
ROWS = 1152
BLOCKS = 9
HALF = ROWS // 2
QUARTER = ROWS // 4
BF16 = jnp.bfloat16
F32 = jnp.float32


def mul(a, b, dims=NN):
    return lax.dot_general(a, b, dims, preferred_element_type=F32)


def sub_iota(rows, cols):
    return lax.broadcasted_iota(jnp.int32, (rows, cols), 0)


def hot_of(index, rows):
    return jnp.where(sub_iota(rows, index.shape[1]) == index, 1.0, 0.0)


def split3(value):
    high = value.astype(BF16)
    rest = value - high.astype(F32)
    middle = rest.astype(BF16)
    return high, middle, (rest - middle.astype(F32)).astype(BF16)


def prep_kernel(
    owner_ref, block_ref, step_ref, obs_ref, dir_ref, index_ref, meta_ref, rank_ref
):
    width = 256
    above = jnp.where(
        sub_iota(width, width) < lax.broadcasted_iota(jnp.int32, (width, width), 1), 1.0, 0.0
    ).astype(BF16)
    carry = jnp.zeros((DEV, 1), F32)
    for at in range(0, TILES, width):
        hot = hot_of(owner_ref[:, at : at + width], DEV)
        before = mul(hot.astype(BF16), above) + carry
        rank_ref[:, at : at + width] = jnp.sum(hot * before, axis=0, keepdims=True)
        carry = before[:, width - 1 : width] + hot[:, width - 1 : width]
    owner_hot = hot_of(owner_ref[...], DEV).astype(BF16)
    in_slot = sub_iota(CAP, TILES).astype(F32) == rank_ref[...]
    tile = lax.broadcasted_iota(jnp.int32, (1, TILES), 1)

    def placings(*rows):
        return jnp.concatenate([jnp.where(in_slot, row, 0.0).astype(BF16) for row in rows], axis=0)

    index = mul(placings((tile // 256).astype(F32), (tile % 256).astype(F32)), owner_hot, NT)
    index_ref[...] = (index[:CAP] * 256.0 + index[CAP:]).astype(jnp.int32)
    obs_hot = hot_of(obs_ref[...], OBS).astype(BF16)
    dir_tile = mul(jnp.broadcast_to(dir_ref[...], (8, OBS)).astype(BF16), obs_hot)[0:1, :]
    fields = mul(
        owner_hot,
        placings(dir_tile, block_ref[...].astype(F32), step_ref[...].astype(F32)),
        NT,
    ).astype(BF16)
    lane_base = lax.axis_index("tm") % 4 * CAP
    shift = jnp.where(
        sub_iota(CAP, LANES) + lane_base == lax.broadcasted_iota(jnp.int32, (CAP, LANES), 1),
        1.0,
        0.0,
    ).astype(BF16)
    meta_ref[:, 0, :] = mul(fields[:, :CAP], shift)
    meta_ref[:, 1, :] = (
        mul(fields[:, CAP : 2 * CAP], shift) * 128.0 + mul(fields[:, 2 * CAP :], shift)
    )


def prep(*operands):
    vmem = pl.BlockSpec(memory_space=pltpu.VMEM)
    return pl.pallas_call(
        prep_kernel,
        out_shape=(
            jax.ShapeDtypeStruct((CAP, DEV), jnp.int32),
            jax.ShapeDtypeStruct((DEV, 2, LANES), F32),
            jax.ShapeDtypeStruct((1, TILES), F32),
        ),
        in_specs=[vmem] * 5,
        out_specs=(vmem,) * 3,
        name="prep",
    )(*operands)


def main_kernel(
    res_ref,
    dir_ref,
    noise_ref,
    owner_ref,
    obs_ref,
    rank_ref,
    index_ref,
    meta_ref,
    foot_ref,
    cov_hbm,
    time_ref,
    applied_ref,
    step_ref,
    ratio_ref,
    wide,
    slots,
    values,
    cov,
    got,
    got_meta,
    acc,
    flux,
    mixed,
    mix_a,
    mix_b,
    time_a,
    time_b,
    part_a,
    part_b,
    in_a,
    in_b,
    smooth,
    dots,
    dots_back,
    by_rank,
    sums,
    sums_in,
    cov_sem,
    tile_send,
    tile_recv,
    meta_send,
    meta_recv,
    z_send,
    z_recv,
    time_send,
    time_recv,
    ag_send,
    ag_recv,
    rs_send,
    rs_recv,
    back_send,
    back_recv,
    sum_send,
    sum_recv,
):
    cell, tm = lax.axis_index("cell"), lax.axis_index("tm")
    me = cell * 16 + tm
    z, core = cell // 2, cell % 2
    y, x = tm // 4, tm % 4
    xs = [(x + k) % 4 for k in range(4)]
    ys = [(y + k) % 4 for k in range(4)]
    far_first = sorted(
        ((dy, dx) for dy in range(4) for dx in range(4)),
        key=lambda at: -(min(at[0], 4 - at[0]) + min(at[1], 4 - at[1])),
    )
    planes = [ys[dy] * 4 + xs[dx] for dy, dx in far_first]

    def x_at(k):
        return xs[k]

    def y_at(k):
        return ys[k]

    def z_cell(k):
        return (z + k) % 4 * 2 + core

    def remote(src, dst, send, recv, to_cell, to_tm):
        return pltpu.make_async_remote_copy(
            src_ref=src,
            dst_ref=dst,
            send_sem=send,
            recv_sem=recv,
            device_id=(to_cell, to_tm),
            device_id_type=MESH,
        )

    def arrived(ref, sem):
        pltpu.make_async_copy(ref, ref, sem).wait()

    def to_others(send):
        def at_cell(k, _):
            to_cell = (cell + 4 + k) % 8
            for to_tm in planes[:15]:
                send(to_cell, to_tm)

            @pl.when(k != 4)
            def _():
                send(to_cell, planes[15])

            return 0

        lax.fori_loop(0, 8, at_cell, 0)

    barrier = pltpu.get_barrier_semaphore()
    to_others(
        lambda to_cell, to_tm: pl.semaphore_signal(
            barrier, inc=1, device_id=(to_cell, to_tm), device_id_type=MESH
        )
    )
    for k in range(8):
        rows = pl.ds(k * 144, 144)
        pltpu.make_async_copy(cov_hbm.at[rows], cov.at[rows], cov_sem).start()

    wide[...] = foot_ref[...].astype(F32)
    pl.semaphore_wait(barrier, DEV - 1)

    def send_tile(to_cell, to_tm):
        peer = to_cell * 16 + to_tm
        remote(
            values.at[peer], got.at[me], tile_send, tile_recv.at[cell], to_cell, to_tm
        ).start()
        remote(
            meta_ref.at[peer], got_meta.at[me], meta_send, meta_recv.at[cell], to_cell, to_tm
        ).start()

    def gather_and_send(k, _):
        to_cell = (cell + 4 + k) % 8
        for j in range(16):
            peer = to_cell * 16 + planes[j]
            for r in range(CAP):
                slots[j, r : r + 1, :] = wide[pl.ds(index_ref[r, peer], 1), :]
            values[peer] = slots[j].astype(BF16)
            if j:
                send_tile(to_cell, planes[j - 1])

        @pl.when(k != 4)
        def _():
            send_tile(to_cell, planes[15])

        return 0

    lax.fori_loop(0, 8, gather_and_send, 0)
    pltpu.make_async_copy(values.at[me], got.at[me], tile_recv.at[cell]).start()
    pltpu.make_async_copy(meta_ref.at[me], got_meta.at[me], meta_recv.at[cell]).start()

    acc[...] = jnp.zeros_like(acc)
    row_of = sub_iota(LANES, LANES).astype(F32)

    def load_meta(group):
        rows = got_meta[pl.ds(group * 16, 16)]
        return jnp.sum(rows.reshape(4, 4, 2, LANES), axis=1)

    def add_group(k, _):
        group = (cell + 12 - k) % 8
        arrived(got.at[pl.ds(group * 16, 16)], tile_recv.at[group])
        arrived(got_meta.at[pl.ds(group * 16, 16)], meta_recv.at[group])
        rows = load_meta(group)
        tiles = got[pl.ds(group * 16, 16)].reshape(512, LANES)
        for b in range(BLOCKS):
            hot = jnp.concatenate(
                [
                    jnp.where(row_of + b * 128.0 == rows[q, 1:2, :], rows[q, 0:1, :], 0.0).astype(
                        BF16
                    )
                    for q in range(4)
                ],
                axis=1,
            )
            acc[b * 128 : b * 128 + 128, :] += mul(hot, tiles)
        return 0

    lax.fori_loop(0, 8, add_group, 0)
    for b in range(BLOCKS):
        flux[cell, :, b * 128 : b * 128 + 128] = acc[b * 128 : b * 128 + 128, :].astype(BF16)

    partner = z * 2 + 1 - core
    up, down, far = z_cell(1), z_cell(3), z_cell(2)
    left, right, full = pl.ds(0, 512), pl.ds(512, ROWS - 512), pl.ds(0, ROWS)
    z_copies = []

    def z_go(block, cols, to_cell, at):
        ref = flux.at[block, :, cols]
        copy = remote(ref, ref, z_send.at[at], z_recv.at[at], to_cell, tm)
        copy.start()
        z_copies.append(copy)

    def z_wait(block, cols, at):
        arrived(flux.at[block, :, cols], z_recv.at[at])

    z_go(cell, left, up, 0)
    z_go(cell, right, down, 2)
    z_go(cell, right, up, 1)
    z_go(cell, left, down, 3)
    z_go(cell, full, partner, 4)

    time_sends = []
    for k in (1, 2, 3):
        peer = y_at(k)
        copy = remote(
            time_ref.at[:, pl.ds(pl.multiple_of(peer * 512, 512), 512)],
            time_a.at[y],
            time_send.at[k - 1],
            time_recv.at[k - 1],
            cell,
            peer * 4 + x,
        )
        copy.start()
        time_sends.append(copy)
        peer = x_at(k)
        for other in range(4):
            copy = remote(
                time_ref.at[:, pl.ds(pl.multiple_of((other * 4 + peer) * 128, 128), 128)],
                time_b.at[x, :, pl.ds(other * 128, 128)],
                time_send.at[3 * k + other + (k - 1)],
                time_recv.at[3 * k + other + (k - 1)],
                cell,
                y * 4 + peer,
            )
            copy.start()
            time_sends.append(copy)
    time_a[y] = time_ref[:, pl.ds(pl.multiple_of(y * 512, 512), 512)]
    for other in range(4):
        time_b[x, :, other * 128 : other * 128 + 128] = time_ref[
            :, pl.ds(pl.multiple_of((other * 4 + x) * 128, 128), 128)
        ]

    arrived(cov, cov_sem)

    def other_core(c):
        return c // 2 * 2 + 1 - c % 2

    def mix(block, first=False):
        cols = pl.ds(pl.multiple_of(block * ROWS, 128), ROWS)
        product = mul(cov[:, cols], flux[block], NT)
        if first:
            mixed[...] = product
        else:
            mixed[...] += product

    mix(cell, True)
    z_wait(down, left, 0)
    z_go(down, left, up, 5)
    z_go(down, left, partner, 7)
    z_wait(up, right, 2)
    z_go(up, right, down, 6)
    z_go(up, right, partner, 8)
    z_wait(other_core(cell), full, 4)
    mix(other_core(cell))
    z_wait(down, right, 1)
    z_go(down, right, partner, 9)
    z_wait(up, left, 3)
    z_go(up, left, partner, 10)
    mix(down)
    mix(up)
    z_wait(other_core(down), left, 7)
    z_wait(other_core(down), right, 9)
    mix(other_core(down))
    z_wait(other_core(up), right, 8)
    z_wait(other_core(up), left, 10)
    mix(other_core(up))
    z_wait(far, left, 5)
    z_go(far, left, partner, 11)
    z_wait(far, right, 6)
    z_go(far, right, partner, 12)
    mix(far)
    z_wait(other_core(far), left, 11)
    z_wait(other_core(far), right, 12)
    mix(other_core(far))

    mix_a[:, pl.ds(pl.multiple_of(x * 128, 128), 128)] = mixed[:HALF, :].astype(BF16)
    mix_b[:, pl.ds(pl.multiple_of(y * 128, 128), 128)] = mixed[HALF:, :].astype(BF16)
    ag_copies = []

    def ag_go(buf, at_lane, rows, to_tm, at):
        ref = buf.at[rows, pl.ds(pl.multiple_of(at_lane * 128, 128), 128)]
        copy = remote(ref, ref, ag_send.at[at], ag_recv.at[at], cell, to_tm)
        copy.start()
        ag_copies.append(copy)

    def ag_wait(buf, at_lane, rows, at):
        arrived(buf.at[rows, pl.ds(pl.multiple_of(at_lane * 128, 128), 128)], ag_recv.at[at])

    first, second = pl.ds(0, QUARTER), pl.ds(QUARTER, QUARTER)
    x_up, x_down = y * 4 + x_at(1), y * 4 + x_at(3)
    y_up, y_down = y_at(1) * 4 + x, y_at(3) * 4 + x
    ag_go(mix_a, x, first, x_up, 0)
    ag_go(mix_a, x, second, x_down, 1)
    ag_go(mix_b, y, first, y_up, 2)
    ag_go(mix_b, y, second, y_down, 3)
    ag_go(mix_a, x, second, x_up, 4)
    ag_go(mix_a, x, first, x_down, 5)
    ag_go(mix_b, y, second, y_up, 6)
    ag_go(mix_b, y, first, y_down, 7)
    ag_wait(mix_a, x_at(3), first, 0)
    ag_go(mix_a, x_at(3), first, x_up, 8)
    ag_wait(mix_a, x_at(1), second, 1)
    ag_go(mix_a, x_at(1), second, x_down, 9)
    ag_wait(mix_b, y_at(3), first, 2)
    ag_go(mix_b, y_at(3), first, y_up, 10)
    ag_wait(mix_b, y_at(1), second, 3)
    ag_go(mix_b, y_at(1), second, y_down, 11)
    for k in (1, 2, 3):
        arrived(time_a.at[y_at(4 - k)], time_recv.at[k - 1])
        for other in range(4):
            arrived(
                time_b.at[x_at(4 - k), :, pl.ds(other * 128, 128)],
                time_recv.at[3 * k + other + (k - 1)],
            )
    ag_wait(mix_a, x_at(3), second, 4)
    ag_wait(mix_a, x_at(1), first, 5)
    ag_wait(mix_b, y_at(3), second, 6)
    ag_wait(mix_b, y_at(1), first, 7)
    ag_wait(mix_a, x_at(2), first, 8)
    ag_wait(mix_a, x_at(2), second, 9)
    rs_copies = []
    for k in (2, 1, 3):
        peer = y_at(k)
        part_a[k - 1] = mul(mix_a[...], time_a[peer], NT).astype(BF16)
        copy = remote(
            part_a.at[k - 1],
            in_a.at[k - 1],
            rs_send.at[k - 1],
            rs_recv.at[k - 1],
            cell,
            peer * 4 + x,
        )
        copy.start()
        rs_copies.append(copy)
        if k == 2:
            ag_wait(mix_b, y_at(2), first, 10)
            ag_wait(mix_b, y_at(2), second, 11)
        peer = x_at(k)
        part_b[k - 1] = mul(mix_b[...], time_b[peer], NT).astype(BF16)
        copy = remote(
            part_b.at[k - 1],
            in_b.at[k - 1],
            rs_send.at[k + 2],
            rs_recv.at[k + 2],
            cell,
            y * 4 + peer,
        )
        copy.start()
        rs_copies.append(copy)
    mixed[:HALF, :] = mul(mix_a[...], time_a[y], NT)
    mixed[HALF:, :] = mul(mix_b[...], time_b[x], NT)
    for k in (1, 3, 2):
        arrived(in_a.at[k - 1], rs_recv.at[k - 1])
        mixed[:HALF, :] += in_a[k - 1].astype(F32)
        arrived(in_b.at[k - 1], rs_recv.at[k + 2])
        mixed[HALF:, :] += in_b[k - 1].astype(F32)
    for b in range(BLOCKS):
        smooth[b] = mixed[b * 128 : b * 128 + 128, :].T.astype(BF16)

    def dot_group(k, _):
        group = (cell + 4 + k) % 8
        rows = load_meta(group)
        tiles = got[pl.ds(group * 16, 16)].reshape(512, LANES)
        picked = [jnp.zeros((LANES, LANES), F32) for _ in range(4)]
        for b in range(BLOCKS):
            product = mul(smooth[b], tiles, NT)
            for q in range(4):
                picked[q] += jnp.where(
                    row_of + b * 128.0 == rows[q, 1:2, :],
                    product[:, q * 128 : q * 128 + 128],
                    0.0,
                )
        for q in range(4):
            dots[group * 4 + q] = jnp.sum(picked[q], axis=0, keepdims=True)

        def send_dots(to_tm):
            remote(
                dots.at[group * 4 + to_tm // 4],
                dots_back.at[me],
                back_send,
                back_recv,
                group,
                to_tm,
            ).start()

        for to_tm in planes[:15]:
            send_dots(to_tm)

        @pl.when(k != 4)
        def _():
            send_dots(planes[15])

        return 0

    lax.fori_loop(0, 8, dot_group, 0)
    dots_back[me] = dots[me // 4]
    owner_hot = hot_of(owner_ref[...], DEV).astype(BF16)
    obs_hot = hot_of(obs_ref[...], OBS).astype(BF16)
    in_slot = sub_iota(CAP, TILES).astype(F32) == rank_ref[...]
    arrived(dots_back.at[pl.ds(0, DEV - 1)], back_recv)
    by_rank[...] = dots_back[:, 0, :].T
    lane_base = x * CAP
    own = jnp.concatenate(split3(by_rank[pl.ds(pl.multiple_of(lane_base, CAP), CAP), :]), axis=0)
    parts = mul(own, owner_hot)
    tile_dots = jnp.sum(
        jnp.where(in_slot, parts[:CAP] + parts[CAP : 2 * CAP] + parts[2 * CAP :], 0.0),
        axis=0,
        keepdims=True,
    )
    high, middle, low = split3(tile_dots)
    three = jnp.concatenate(
        [high.astype(F32), middle.astype(F32), low.astype(F32), jnp.zeros((5, TILES), F32)], axis=0
    ).astype(BF16)
    direction, residual = dir_ref[...], res_ref[...]
    applied = jnp.sum(mul(three, obs_hot, NT), axis=0, keepdims=True)
    applied = applied + noise_ref[...] * direction

    lanes = lax.broadcasted_iota(jnp.int32, (1, LANES), 1)
    row = jnp.zeros((1, LANES), F32)
    for at, value in enumerate(
        (residual * residual, direction * applied, residual * applied, applied * applied)
    ):
        row = jnp.where(lanes == at, jnp.sum(value, axis=1, keepdims=True), row)
    sums[...] = row
    to_others(
        lambda to_cell, to_tm: remote(
            sums, sums_in.at[me], sum_send, sum_recv, to_cell, to_tm
        ).start()
    )
    sums_in[me] = row
    arrived(sums_in.at[pl.ds(0, DEV - 1)], sum_recv)
    total = jnp.sum(sums_in[...], axis=0)

    def total_of(at):
        return jnp.sum(jnp.where(lanes == at, total, 0.0), axis=1, keepdims=True)

    norm_now, curvature, cross_term, image_norm = (total_of(at) for at in range(4))
    step_size = norm_now / curvature
    norm_next = norm_now - 2.0 * step_size * cross_term + step_size * step_size * image_norm
    applied_ref[...] = applied
    step_ref[...] = jnp.broadcast_to(step_size, (1, OBS))
    ratio_ref[...] = jnp.broadcast_to(norm_next / norm_now, (1, OBS))

    arrived(values.at[pl.ds(0, DEV - 1)], tile_send)
    arrived(meta_ref.at[pl.ds(0, DEV - 1)], meta_send)
    for copy in time_sends + z_copies + ag_copies + rs_copies:
        copy.wait_send()
    arrived(dots_back.at[pl.ds(0, DEV - 1)], back_send)
    arrived(sums_in.at[pl.ds(0, DEV - 1)], sum_send)


def whole(*operands):
    vmem = pl.BlockSpec(memory_space=pltpu.VMEM)
    dma = pltpu.SemaphoreType.DMA
    row = jax.ShapeDtypeStruct((1, OBS), F32)
    return pl.pallas_call(
        main_kernel,
        out_shape=(row, row, row),
        in_specs=[vmem] * 6
        + [pl.BlockSpec(memory_space=pltpu.SMEM), vmem, vmem]
        + [pl.BlockSpec(memory_space=pl.ANY), vmem],
        out_specs=(vmem,) * 3,
        scratch_shapes=[
            pltpu.VMEM((TILES, LANES), F32),
            pltpu.VMEM((16, CAP, LANES), F32),
            pltpu.VMEM((DEV, CAP, LANES), BF16),
            pltpu.VMEM((ROWS, 8 * ROWS), BF16),
            pltpu.VMEM((DEV, CAP, LANES), BF16),
            pltpu.VMEM((DEV, 2, LANES), F32),
            pltpu.VMEM((ROWS, LANES), F32),
            pltpu.VMEM((8, LANES, ROWS), BF16),
            pltpu.VMEM((ROWS, LANES), F32),
            pltpu.VMEM((HALF, 512), BF16),
            pltpu.VMEM((HALF, 512), BF16),
            pltpu.VMEM((4, LANES, 512), BF16),
            pltpu.VMEM((4, LANES, 512), BF16),
            pltpu.VMEM((3, HALF, LANES), BF16),
            pltpu.VMEM((3, HALF, LANES), BF16),
            pltpu.VMEM((3, HALF, LANES), BF16),
            pltpu.VMEM((3, HALF, LANES), BF16),
            pltpu.VMEM((BLOCKS, LANES, LANES), BF16),
            pltpu.VMEM((DEV // 4, 1, LANES), F32),
            pltpu.VMEM((DEV, 1, LANES), F32),
            pltpu.VMEM((LANES, DEV), F32),
            pltpu.VMEM((1, LANES), F32),
            pltpu.VMEM((DEV, 1, LANES), F32),
            dma,
            dma,
            dma((8,)),
            dma,
            dma((8,)),
            dma((13,)),
            dma((13,)),
            dma((15,)),
            dma((15,)),
            dma((12,)),
            dma((12,)),
            dma((6,)),
            dma((6,)),
            dma,
            dma,
            dma,
            dma,
        ],
        compiler_params=pltpu.CompilerParams(
            collective_id=0, has_side_effects=True, vmem_limit_bytes=60 * 2**20
        ),
        name="whole",
    )(*operands)


def local(
    solution,
    residual,
    direction,
    noise_var,
    footprints,
    tile_owner,
    tile_block,
    tile_step,
    tile_obs,
    cell_cov,
    time_cov,
):
    row = functools.partial(jnp.reshape, shape=(1, OBS))
    tile_row = functools.partial(jnp.reshape, shape=(1, TILES))
    owner, obs = tile_row(tile_owner), tile_row(tile_obs)
    index, meta, rank = prep(owner, tile_row(tile_block), tile_row(tile_step), obs, row(direction))
    outs = whole(
        row(residual),
        row(direction),
        row(noise_var),
        owner,
        obs,
        rank,
        index,
        meta,
        footprints,
        cell_cov,
        time_cov,
    )
    applied, step_size, ratio = (out.reshape(OBS) for out in outs)
    new_residual = residual - step_size * applied
    return solution + step_size * direction, new_residual, new_residual + ratio * direction


def solution(mesh):
    both = P(CELL_TM)
    in_specs = (both,) * 4 + (P(CELL_TM, None),) * 2 + (both,) * 3
    in_specs += (P("cell", None), P("tm", None))
    return jax.shard_map(
        local, mesh=mesh, in_specs=in_specs, out_specs=(both,) * 3, check_vma=False
    )
```

```python
import functools

import jax
import jax.numpy as jnp
from jax import lax
from jax.experimental import pallas as pl
from jax.experimental.pallas import tpu as pltpu
from jax.sharding import PartitionSpec as P

MESH = pl.DeviceIdType.MESH
CELL_TM = ("cell", "tm")
NN = (((1,), (0,)), ((), ()))
NT = (((1,), (1,)), ((), ()))
DEV = 128
CAP = 32
LANES = 128
OBS = 256
TILES = 2048
SLOTS = DEV * CAP
ROWS = 1152
BLOCKS = 9
HALF = ROWS // 2
QUARTER = ROWS // 4
BF16 = jnp.bfloat16
F32 = jnp.float32


def mul(a, b, dims=NN):
    return lax.dot_general(a, b, dims, preferred_element_type=F32)


def sub_iota(rows, cols):
    return lax.broadcasted_iota(jnp.int32, (rows, cols), 0)


def hot_of(index, rows):
    return jnp.where(sub_iota(rows, index.shape[1]) == index, 1.0, 0.0)


def split3(value):
    high = value.astype(BF16)
    rest = value - high.astype(F32)
    middle = rest.astype(BF16)
    return high, middle, (rest - middle.astype(F32)).astype(BF16)


def placings(rank, *rows):
    in_slot = sub_iota(CAP, TILES).astype(F32) == rank
    return jnp.concatenate([jnp.where(in_slot, row, 0.0).astype(BF16) for row in rows], axis=0)


def prep_kernel(owner_ref, index_ref, rank_ref):
    width = 256
    above = jnp.where(
        sub_iota(width, width) < lax.broadcasted_iota(jnp.int32, (width, width), 1), 1.0, 0.0
    ).astype(BF16)
    carry = jnp.zeros((DEV, 1), F32)
    for at in range(0, TILES, width):
        hot = hot_of(owner_ref[:, at : at + width], DEV)
        before = mul(hot.astype(BF16), above) + carry
        rank_ref[:, at : at + width] = jnp.sum(hot * before, axis=0, keepdims=True)
        carry = before[:, width - 1 : width] + hot[:, width - 1 : width]
    owner_hot = hot_of(owner_ref[...], DEV).astype(BF16)
    tile = lax.broadcasted_iota(jnp.int32, (1, TILES), 1)
    index = mul(
        placings(rank_ref[...], (tile // 256).astype(F32), (tile % 256).astype(F32)), owner_hot, NT
    )
    index_ref[...] = (index[:CAP] * 256.0 + index[CAP:]).astype(jnp.int32)


def prep(owner):
    vmem = pl.BlockSpec(memory_space=pltpu.VMEM)
    return pl.pallas_call(
        prep_kernel,
        out_shape=(
            jax.ShapeDtypeStruct((CAP, DEV), jnp.int32),
            jax.ShapeDtypeStruct((1, TILES), F32),
        ),
        in_specs=[vmem],
        out_specs=(vmem, vmem),
        name="prep",
    )(owner)


def main_kernel(
    res_ref,
    dir_ref,
    noise_ref,
    owner_ref,
    block_ref,
    step_ref,
    obs_ref,
    rank_ref,
    index_ref,
    foot_hbm,
    cov_hbm,
    time_hbm,
    applied_ref,
    size_ref,
    ratio_ref,
    foot_ref,
    time_ref,
    meta_ref,
    wide,
    slots,
    values,
    cov,
    got,
    got_meta,
    acc,
    flux,
    mixed,
    mix_a,
    mix_b,
    time_a,
    time_b,
    part_a,
    part_b,
    in_a,
    in_b,
    smooth,
    dots,
    dots_back,
    by_rank,
    sums,
    sums_in,
    ready,
    foot_sem,
    time_sem,
    cov_sem,
    tile_send,
    tile_recv,
    meta_send,
    meta_recv,
    z_send,
    z_recv,
    time_send,
    time_recv,
    ag_send,
    ag_recv,
    rs_send,
    rs_recv,
    back_send,
    back_recv,
    sum_send,
    sum_recv,
):
    cell, tm = lax.axis_index("cell"), lax.axis_index("tm")
    me = cell * 16 + tm
    z, core = cell // 2, cell % 2
    y, x = tm // 4, tm % 4
    xs = [(x + k) % 4 for k in range(4)]
    ys = [(y + k) % 4 for k in range(4)]
    far_first = sorted(
        ((dy, dx) for dy in range(4) for dx in range(4)),
        key=lambda at: -(min(at[0], 4 - at[0]) + min(at[1], 4 - at[1])),
    )
    planes = [ys[dy] * 4 + xs[dx] for dy, dx in far_first]

    def x_at(k):
        return xs[k]

    def y_at(k):
        return ys[k]

    def z_cell(k):
        return (z + k) % 4 * 2 + core

    def remote(src, dst, send, recv, to_cell, to_tm):
        return pltpu.make_async_remote_copy(
            src_ref=src,
            dst_ref=dst,
            send_sem=send,
            recv_sem=recv,
            device_id=(to_cell, to_tm),
            device_id_type=MESH,
        )

    def arrived(ref, sem):
        pltpu.make_async_copy(ref, ref, sem).wait()

    def to_others(send):
        def at_cell(k, _):
            to_cell = (cell + 4 + k) % 8
            for to_tm in planes[:15]:
                send(to_cell, to_tm)

            @pl.when(k != 4)
            def _():
                send(to_cell, planes[15])

            return 0

        lax.fori_loop(0, 8, at_cell, 0)

    barrier = pltpu.get_barrier_semaphore()
    columns = [(cell + k) % 8 for k in (4, 5, 3, 6, 2, 7, 1)]

    def signal(sem, to_cell, to_tm):
        pl.semaphore_signal(sem, inc=1, device_id=(to_cell, to_tm), device_id_type=MESH)

    for to_tm in planes[:15]:
        signal(barrier, cell, to_tm)
    for to_cell in columns:
        signal(barrier, to_cell, tm)
    foot_copy = pltpu.make_async_copy(foot_hbm, foot_ref, foot_sem)
    foot_copy.start()
    time_copy = pltpu.make_async_copy(time_hbm, time_ref, time_sem)
    time_copy.start()
    for k in range(8):
        rows = pl.ds(k * 144, 144)
        pltpu.make_async_copy(cov_hbm.at[rows], cov.at[rows], cov_sem).start()
    pl.semaphore_wait(barrier, 22)
    for to_cell in columns:
        signal(ready, to_cell, tm)

    owner_hot = hot_of(owner_ref[...], DEV).astype(BF16)
    obs_hot = hot_of(obs_ref[...], OBS).astype(BF16)
    dir_tile = mul(jnp.broadcast_to(dir_ref[...], (8, OBS)).astype(BF16), obs_hot)[0:1, :]
    fields = mul(
        owner_hot,
        placings(rank_ref[...], dir_tile, block_ref[...].astype(F32), step_ref[...].astype(F32)),
        NT,
    ).astype(BF16)
    lane_base = x * CAP
    shift = jnp.where(
        sub_iota(CAP, LANES) + lane_base == lax.broadcasted_iota(jnp.int32, (CAP, LANES), 1),
        1.0,
        0.0,
    ).astype(BF16)
    meta_ref[:, 0, :] = mul(fields[:, :CAP], shift)
    meta_ref[:, 1, :] = (
        mul(fields[:, CAP : 2 * CAP], shift) * 128.0 + mul(fields[:, 2 * CAP :], shift)
    )
    foot_copy.wait()
    wide[...] = foot_ref[...].astype(F32)
    pl.semaphore_wait(ready, 7)

    def send_tile(to_cell, to_tm):
        peer = to_cell * 16 + to_tm
        remote(
            values.at[peer], got.at[me], tile_send, tile_recv.at[cell], to_cell, to_tm
        ).start()
        remote(
            meta_ref.at[peer], got_meta.at[me], meta_send, meta_recv.at[cell], to_cell, to_tm
        ).start()

    def gather_and_send(k, _):
        to_cell = (cell + 4 + k) % 8
        for j in range(16):
            peer = to_cell * 16 + planes[j]
            for r in range(CAP):
                slots[j, r : r + 1, :] = wide[pl.ds(index_ref[r, peer], 1), :]
            values[peer] = slots[j].astype(BF16)
            if j:
                send_tile(to_cell, planes[j - 1])

        @pl.when(k != 4)
        def _():
            send_tile(to_cell, planes[15])

        return 0

    lax.fori_loop(0, 8, gather_and_send, 0)
    pltpu.make_async_copy(values.at[me], got.at[me], tile_recv.at[cell]).start()
    pltpu.make_async_copy(meta_ref.at[me], got_meta.at[me], meta_recv.at[cell]).start()

    acc[...] = jnp.zeros_like(acc)
    row_of = sub_iota(LANES, LANES).astype(F32)

    def load_meta(group):
        rows = got_meta[pl.ds(group * 16, 16)]
        return jnp.sum(rows.reshape(4, 4, 2, LANES), axis=1)

    def add_group(k, _):
        group = (cell + 12 - k) % 8
        arrived(got.at[pl.ds(group * 16, 16)], tile_recv.at[group])
        arrived(got_meta.at[pl.ds(group * 16, 16)], meta_recv.at[group])
        rows = load_meta(group)
        tiles = got[pl.ds(group * 16, 16)].reshape(512, LANES)
        for b in range(BLOCKS):
            hot = jnp.concatenate(
                [
                    jnp.where(row_of + b * 128.0 == rows[q, 1:2, :], rows[q, 0:1, :], 0.0).astype(
                        BF16
                    )
                    for q in range(4)
                ],
                axis=1,
            )
            acc[b * 128 : b * 128 + 128, :] += mul(hot, tiles)
        return 0

    lax.fori_loop(0, 8, add_group, 0)
    for b in range(BLOCKS):
        flux[cell, :, b * 128 : b * 128 + 128] = acc[b * 128 : b * 128 + 128, :].astype(BF16)

    partner = z * 2 + 1 - core
    up, down, far = z_cell(1), z_cell(3), z_cell(2)
    left, right, full = pl.ds(0, 512), pl.ds(512, ROWS - 512), pl.ds(0, ROWS)
    z_copies = []

    def z_go(block, cols, to_cell, at):
        ref = flux.at[block, :, cols]
        copy = remote(ref, ref, z_send.at[at], z_recv.at[at], to_cell, tm)
        copy.start()
        z_copies.append(copy)

    def z_wait(block, cols, at):
        arrived(flux.at[block, :, cols], z_recv.at[at])

    z_go(cell, left, up, 0)
    z_go(cell, right, down, 2)
    z_go(cell, right, up, 1)
    z_go(cell, left, down, 3)
    z_go(cell, full, partner, 4)

    time_copy.wait()
    time_sends = []
    for k in (1, 2, 3):
        peer = y_at(k)
        copy = remote(
            time_ref.at[:, pl.ds(pl.multiple_of(peer * 512, 512), 512)],
            time_a.at[y],
            time_send.at[k - 1],
            time_recv.at[k - 1],
            cell,
            peer * 4 + x,
        )
        copy.start()
        time_sends.append(copy)
        peer = x_at(k)
        for other in range(4):
            copy = remote(
                time_ref.at[:, pl.ds(pl.multiple_of((other * 4 + peer) * 128, 128), 128)],
                time_b.at[x, :, pl.ds(other * 128, 128)],
                time_send.at[3 * k + other + (k - 1)],
                time_recv.at[3 * k + other + (k - 1)],
                cell,
                y * 4 + peer,
            )
            copy.start()
            time_sends.append(copy)
    time_a[y] = time_ref[:, pl.ds(pl.multiple_of(y * 512, 512), 512)]
    for other in range(4):
        time_b[x, :, other * 128 : other * 128 + 128] = time_ref[
            :, pl.ds(pl.multiple_of((other * 4 + x) * 128, 128), 128)
        ]

    arrived(cov, cov_sem)

    def other_core(c):
        return c // 2 * 2 + 1 - c % 2

    def mix(block, first=False):
        cols = pl.ds(pl.multiple_of(block * ROWS, 128), ROWS)
        product = mul(cov[:, cols], flux[block], NT)
        if first:
            mixed[...] = product
        else:
            mixed[...] += product

    mix(cell, True)
    z_wait(down, left, 0)
    z_go(down, left, up, 5)
    z_go(down, left, partner, 7)
    z_wait(up, right, 2)
    z_go(up, right, down, 6)
    z_go(up, right, partner, 8)
    z_wait(other_core(cell), full, 4)
    mix(other_core(cell))
    z_wait(down, right, 1)
    z_go(down, right, partner, 9)
    z_wait(up, left, 3)
    z_go(up, left, partner, 10)
    mix(down)
    mix(up)
    z_wait(other_core(down), left, 7)
    z_wait(other_core(down), right, 9)
    mix(other_core(down))
    z_wait(other_core(up), right, 8)
    z_wait(other_core(up), left, 10)
    mix(other_core(up))
    z_wait(far, left, 5)
    z_go(far, left, partner, 11)
    z_wait(far, right, 6)
    z_go(far, right, partner, 12)
    mix(far)
    z_wait(other_core(far), left, 11)
    z_wait(other_core(far), right, 12)
    mix(other_core(far))

    mix_a[:, pl.ds(pl.multiple_of(x * 128, 128), 128)] = mixed[:HALF, :].astype(BF16)
    mix_b[:, pl.ds(pl.multiple_of(y * 128, 128), 128)] = mixed[HALF:, :].astype(BF16)
    ag_copies = []

    def ag_go(buf, at_lane, rows, to_tm, at):
        ref = buf.at[rows, pl.ds(pl.multiple_of(at_lane * 128, 128), 128)]
        copy = remote(ref, ref, ag_send.at[at], ag_recv.at[at], cell, to_tm)
        copy.start()
        ag_copies.append(copy)

    def ag_wait(buf, at_lane, rows, at):
        arrived(buf.at[rows, pl.ds(pl.multiple_of(at_lane * 128, 128), 128)], ag_recv.at[at])

    first, second = pl.ds(0, QUARTER), pl.ds(QUARTER, QUARTER)
    x_up, x_down = y * 4 + x_at(1), y * 4 + x_at(3)
    y_up, y_down = y_at(1) * 4 + x, y_at(3) * 4 + x
    ag_go(mix_a, x, first, x_up, 0)
    ag_go(mix_a, x, second, x_down, 1)
    ag_go(mix_b, y, first, y_up, 2)
    ag_go(mix_b, y, second, y_down, 3)
    ag_go(mix_a, x, second, x_up, 4)
    ag_go(mix_a, x, first, x_down, 5)
    ag_go(mix_b, y, second, y_up, 6)
    ag_go(mix_b, y, first, y_down, 7)
    ag_wait(mix_a, x_at(3), first, 0)
    ag_go(mix_a, x_at(3), first, x_up, 8)
    ag_wait(mix_a, x_at(1), second, 1)
    ag_go(mix_a, x_at(1), second, x_down, 9)
    ag_wait(mix_b, y_at(3), first, 2)
    ag_go(mix_b, y_at(3), first, y_up, 10)
    ag_wait(mix_b, y_at(1), second, 3)
    ag_go(mix_b, y_at(1), second, y_down, 11)
    for k in (1, 2, 3):
        arrived(time_a.at[y_at(4 - k)], time_recv.at[k - 1])
        for other in range(4):
            arrived(
                time_b.at[x_at(4 - k), :, pl.ds(other * 128, 128)],
                time_recv.at[3 * k + other + (k - 1)],
            )
    ag_wait(mix_a, x_at(3), second, 4)
    ag_wait(mix_a, x_at(1), first, 5)
    ag_wait(mix_b, y_at(3), second, 6)
    ag_wait(mix_b, y_at(1), first, 7)
    ag_wait(mix_a, x_at(2), first, 8)
    ag_wait(mix_a, x_at(2), second, 9)
    rs_copies = []
    for k in (2, 1, 3):
        peer = y_at(k)
        part_a[k - 1] = mul(mix_a[...], time_a[peer], NT).astype(BF16)
        copy = remote(
            part_a.at[k - 1],
            in_a.at[k - 1],
            rs_send.at[k - 1],
            rs_recv.at[k - 1],
            cell,
            peer * 4 + x,
        )
        copy.start()
        rs_copies.append(copy)
        if k == 2:
            ag_wait(mix_b, y_at(2), first, 10)
            ag_wait(mix_b, y_at(2), second, 11)
        peer = x_at(k)
        part_b[k - 1] = mul(mix_b[...], time_b[peer], NT).astype(BF16)
        copy = remote(
            part_b.at[k - 1],
            in_b.at[k - 1],
            rs_send.at[k + 2],
            rs_recv.at[k + 2],
            cell,
            y * 4 + peer,
        )
        copy.start()
        rs_copies.append(copy)
    mixed[:HALF, :] = mul(mix_a[...], time_a[y], NT)
    mixed[HALF:, :] = mul(mix_b[...], time_b[x], NT)
    for k in (1, 3, 2):
        arrived(in_a.at[k - 1], rs_recv.at[k - 1])
        mixed[:HALF, :] += in_a[k - 1].astype(F32)
        arrived(in_b.at[k - 1], rs_recv.at[k + 2])
        mixed[HALF:, :] += in_b[k - 1].astype(F32)
    for b in range(BLOCKS):
        smooth[b] = mixed[b * 128 : b * 128 + 128, :].T.astype(BF16)

    def dot_group(k, _):
        group = (cell + 4 + k) % 8
        rows = load_meta(group)
        tiles = got[pl.ds(group * 16, 16)].reshape(512, LANES)
        picked = [jnp.zeros((LANES, LANES), F32) for _ in range(4)]
        for b in range(BLOCKS):
            product = mul(smooth[b], tiles, NT)
            for q in range(4):
                picked[q] += jnp.where(
                    row_of + b * 128.0 == rows[q, 1:2, :],
                    product[:, q * 128 : q * 128 + 128],
                    0.0,
                )
        for q in range(4):
            dots[group * 4 + q] = jnp.sum(picked[q], axis=0, keepdims=True)

        def send_dots(to_tm):
            remote(
                dots.at[group * 4 + to_tm // 4],
                dots_back.at[me],
                back_send,
                back_recv,
                group,
                to_tm,
            ).start()

        for to_tm in planes[:15]:
            send_dots(to_tm)

        @pl.when(k != 4)
        def _():
            send_dots(planes[15])

        return 0

    lax.fori_loop(0, 8, dot_group, 0)
    dots_back[me] = dots[me // 4]
    owner_hot = hot_of(owner_ref[...], DEV).astype(BF16)
    obs_hot = hot_of(obs_ref[...], OBS).astype(BF16)
    in_slot = sub_iota(CAP, TILES).astype(F32) == rank_ref[...]
    arrived(dots_back.at[pl.ds(0, DEV - 1)], back_recv)
    by_rank[...] = dots_back[:, 0, :].T
    own = jnp.concatenate(split3(by_rank[pl.ds(pl.multiple_of(lane_base, CAP), CAP), :]), axis=0)
    parts = mul(own, owner_hot)
    tile_dots = jnp.sum(
        jnp.where(in_slot, parts[:CAP] + parts[CAP : 2 * CAP] + parts[2 * CAP :], 0.0),
        axis=0,
        keepdims=True,
    )
    high, middle, low = split3(tile_dots)
    three = jnp.concatenate(
        [high.astype(F32), middle.astype(F32), low.astype(F32), jnp.zeros((5, TILES), F32)], axis=0
    ).astype(BF16)
    direction, residual = dir_ref[...], res_ref[...]
    applied = jnp.sum(mul(three, obs_hot, NT), axis=0, keepdims=True)
    applied = applied + noise_ref[...] * direction

    lanes = lax.broadcasted_iota(jnp.int32, (1, LANES), 1)
    row = jnp.zeros((1, LANES), F32)
    for at, value in enumerate(
        (residual * residual, direction * applied, residual * applied, applied * applied)
    ):
        row = jnp.where(lanes == at, jnp.sum(value, axis=1, keepdims=True), row)
    sums[...] = row
    to_others(
        lambda to_cell, to_tm: remote(
            sums, sums_in.at[me], sum_send, sum_recv, to_cell, to_tm
        ).start()
    )
    sums_in[me] = row
    arrived(sums_in.at[pl.ds(0, DEV - 1)], sum_recv)
    total = jnp.sum(sums_in[...], axis=0)

    def total_of(at):
        return jnp.sum(jnp.where(lanes == at, total, 0.0), axis=1, keepdims=True)

    norm_now, curvature, cross_term, image_norm = (total_of(at) for at in range(4))
    step_size = norm_now / curvature
    norm_next = norm_now - 2.0 * step_size * cross_term + step_size * step_size * image_norm
    applied_ref[...] = applied
    size_ref[...] = jnp.broadcast_to(step_size, (1, OBS))
    ratio_ref[...] = jnp.broadcast_to(norm_next / norm_now, (1, OBS))

    arrived(values.at[pl.ds(0, DEV - 1)], tile_send)
    arrived(meta_ref.at[pl.ds(0, DEV - 1)], meta_send)
    for copy in time_sends + z_copies + ag_copies + rs_copies:
        copy.wait_send()
    arrived(dots_back.at[pl.ds(0, DEV - 1)], back_send)
    arrived(sums_in.at[pl.ds(0, DEV - 1)], sum_send)


def whole(*operands):
    vmem = pl.BlockSpec(memory_space=pltpu.VMEM)
    dma = pltpu.SemaphoreType.DMA
    row = jax.ShapeDtypeStruct((1, OBS), F32)
    return pl.pallas_call(
        main_kernel,
        out_shape=(row, row, row),
        in_specs=[vmem] * 8
        + [pl.BlockSpec(memory_space=pltpu.SMEM)]
        + [pl.BlockSpec(memory_space=pl.ANY)] * 3,
        out_specs=(vmem,) * 3,
        scratch_shapes=[
            pltpu.VMEM((TILES, LANES), BF16),
            pltpu.VMEM((LANES, 16 * LANES), BF16),
            pltpu.VMEM((DEV, 2, LANES), F32),
            pltpu.VMEM((TILES, LANES), F32),
            pltpu.VMEM((16, CAP, LANES), F32),
            pltpu.VMEM((DEV, CAP, LANES), BF16),
            pltpu.VMEM((ROWS, 8 * ROWS), BF16),
            pltpu.VMEM((DEV, CAP, LANES), BF16),
            pltpu.VMEM((DEV, 2, LANES), F32),
            pltpu.VMEM((ROWS, LANES), F32),
            pltpu.VMEM((8, LANES, ROWS), BF16),
            pltpu.VMEM((ROWS, LANES), F32),
            pltpu.VMEM((HALF, 512), BF16),
            pltpu.VMEM((HALF, 512), BF16),
            pltpu.VMEM((4, LANES, 512), BF16),
            pltpu.VMEM((4, LANES, 512), BF16),
            pltpu.VMEM((3, HALF, LANES), BF16),
            pltpu.VMEM((3, HALF, LANES), BF16),
            pltpu.VMEM((3, HALF, LANES), BF16),
            pltpu.VMEM((3, HALF, LANES), BF16),
            pltpu.VMEM((BLOCKS, LANES, LANES), BF16),
            pltpu.VMEM((DEV // 4, 1, LANES), F32),
            pltpu.VMEM((DEV, 1, LANES), F32),
            pltpu.VMEM((LANES, DEV), F32),
            pltpu.VMEM((1, LANES), F32),
            pltpu.VMEM((DEV, 1, LANES), F32),
            pltpu.SemaphoreType.REGULAR,
            dma,
            dma,
            dma,
            dma,
            dma((8,)),
            dma,
            dma((8,)),
            dma((13,)),
            dma((13,)),
            dma((15,)),
            dma((15,)),
            dma((12,)),
            dma((12,)),
            dma((6,)),
            dma((6,)),
            dma,
            dma,
            dma,
            dma,
        ],
        compiler_params=pltpu.CompilerParams(
            collective_id=0, has_side_effects=True, vmem_limit_bytes=60 * 2**20
        ),
        name="whole",
    )(*operands)


def local(
    solution,
    residual,
    direction,
    noise_var,
    footprints,
    tile_owner,
    tile_block,
    tile_step,
    tile_obs,
    cell_cov,
    time_cov,
):
    row = functools.partial(jnp.reshape, shape=(1, OBS))
    tile_row = functools.partial(jnp.reshape, shape=(1, TILES))
    owner = tile_row(tile_owner)
    index, rank = prep(owner)
    outs = whole(
        row(residual),
        row(direction),
        row(noise_var),
        owner,
        tile_row(tile_block),
        tile_row(tile_step),
        tile_row(tile_obs),
        rank,
        index,
        footprints,
        cell_cov,
        time_cov,
    )
    applied, step_size, ratio = (out.reshape(OBS) for out in outs)
    new_residual = residual - step_size * applied
    return solution + step_size * direction, new_residual, new_residual + ratio * direction


def solution(mesh):
    both = P(CELL_TM)
    in_specs = (both,) * 4 + (P(CELL_TM, None),) * 2 + (both,) * 3
    in_specs += (P("cell", None), P("tm", None))
    return jax.shard_map(
        local, mesh=mesh, in_specs=in_specs, out_specs=(both,) * 3, check_vma=False
    )
```

```python
import functools

import jax
import jax.numpy as jnp
from jax import lax
from jax.experimental import pallas as pl
from jax.experimental.pallas import tpu as pltpu
from jax.sharding import PartitionSpec as P

MESH = pl.DeviceIdType.MESH
CELL_TM = ("cell", "tm")
NN = (((1,), (0,)), ((), ()))
NT = (((1,), (1,)), ((), ()))
DEV = 128
CAP = 32
LANES = 128
OBS = 256
TILES = 2048
SLOTS = DEV * CAP
ROWS = 1152
BLOCKS = 9
HALF = ROWS // 2
QUARTER = ROWS // 4
BF16 = jnp.bfloat16
F32 = jnp.float32


def mul(a, b, dims=NN):
    return lax.dot_general(a, b, dims, preferred_element_type=F32)


def sub_iota(rows, cols):
    return lax.broadcasted_iota(jnp.int32, (rows, cols), 0)


def hot_of(index, rows):
    return jnp.where(sub_iota(rows, index.shape[1]) == index, 1.0, 0.0)


def split3(value):
    high = value.astype(BF16)
    rest = value - high.astype(F32)
    middle = rest.astype(BF16)
    return high, middle, (rest - middle.astype(F32)).astype(BF16)


def placings(rank, *rows):
    in_slot = sub_iota(CAP, TILES).astype(F32) == rank
    return jnp.concatenate([jnp.where(in_slot, row, 0.0).astype(BF16) for row in rows], axis=0)


def prep_kernel(owner_ref, index_ref, rank_ref):
    width = 256
    above = jnp.where(
        sub_iota(width, width) < lax.broadcasted_iota(jnp.int32, (width, width), 1), 1.0, 0.0
    ).astype(BF16)
    carry = jnp.zeros((DEV, 1), F32)
    for at in range(0, TILES, width):
        hot = hot_of(owner_ref[:, at : at + width], DEV)
        before = mul(hot.astype(BF16), above) + carry
        rank_ref[:, at : at + width] = jnp.sum(hot * before, axis=0, keepdims=True)
        carry = before[:, width - 1 : width] + hot[:, width - 1 : width]
    owner_hot = hot_of(owner_ref[...], DEV).astype(BF16)
    tile = lax.broadcasted_iota(jnp.int32, (1, TILES), 1)
    index = mul(
        placings(rank_ref[...], (tile // 256).astype(F32), (tile % 256).astype(F32)), owner_hot, NT
    )
    index_ref[...] = (index[:CAP] * 256.0 + index[CAP:]).astype(jnp.int32)


def prep(owner):
    vmem = pl.BlockSpec(memory_space=pltpu.VMEM)
    return pl.pallas_call(
        prep_kernel,
        out_shape=(
            jax.ShapeDtypeStruct((CAP, DEV), jnp.int32),
            jax.ShapeDtypeStruct((1, TILES), F32),
        ),
        in_specs=[vmem],
        out_specs=(vmem, vmem),
        name="prep",
    )(owner)


def main_kernel(
    res_ref,
    dir_ref,
    noise_ref,
    owner_ref,
    block_ref,
    step_ref,
    obs_ref,
    rank_ref,
    index_ref,
    foot_hbm,
    cov_hbm,
    time_hbm,
    applied_ref,
    size_ref,
    ratio_ref,
    foot_ref,
    time_ref,
    meta_ref,
    wide,
    slots,
    values,
    cov,
    got,
    got_meta,
    hots,
    acc,
    flux,
    mixed,
    mix_a,
    mix_b,
    time_a,
    time_b,
    part_a,
    part_b,
    in_a,
    in_b,
    smooth,
    products,
    dots,
    dots_back,
    by_rank,
    sums,
    sums_in,
    ready,
    foot_sem,
    time_sem,
    cov_sem,
    tile_send,
    tile_recv,
    meta_send,
    meta_recv,
    z_send,
    z_recv,
    time_send,
    time_recv,
    ag_send,
    ag_recv,
    rs_send,
    rs_recv,
    back_send,
    back_recv,
    sum_send,
    sum_recv,
):
    cell, tm = lax.axis_index("cell"), lax.axis_index("tm")
    me = cell * 16 + tm
    z, core = cell // 2, cell % 2
    y, x = tm // 4, tm % 4
    xs = [(x + k) % 4 for k in range(4)]
    ys = [(y + k) % 4 for k in range(4)]
    far_first = sorted(
        ((dy, dx) for dy in range(4) for dx in range(4)),
        key=lambda at: -(min(at[0], 4 - at[0]) + min(at[1], 4 - at[1])),
    )
    planes = [ys[dy] * 4 + xs[dx] for dy, dx in far_first]

    def x_at(k):
        return xs[k]

    def y_at(k):
        return ys[k]

    def z_cell(k):
        return (z + k) % 4 * 2 + core

    def remote(src, dst, send, recv, to_cell, to_tm):
        return pltpu.make_async_remote_copy(
            src_ref=src,
            dst_ref=dst,
            send_sem=send,
            recv_sem=recv,
            device_id=(to_cell, to_tm),
            device_id_type=MESH,
        )

    def arrived(ref, sem):
        pltpu.make_async_copy(ref, ref, sem).wait()

    def away(k):
        return (cell + 4 + (k % 2 * 2 - 1) * ((k + 1) // 2)) % 8

    def to_others(send):
        def at_cell(k, _):
            to_cell = away(k)
            for to_tm in planes:
                send(to_cell, to_tm)
            return 0

        lax.fori_loop(0, 7, at_cell, 0)
        for to_tm in planes[:15]:
            send(cell, to_tm)

    barrier = pltpu.get_barrier_semaphore()
    columns = [(cell + k) % 8 for k in (4, 5, 3, 6, 2, 7, 1)]

    def signal(sem, to_cell, to_tm):
        pl.semaphore_signal(sem, inc=1, device_id=(to_cell, to_tm), device_id_type=MESH)

    for to_tm in planes[:15]:
        signal(barrier, cell, to_tm)
    for to_cell in columns:
        signal(barrier, to_cell, tm)
    foot_copy = pltpu.make_async_copy(foot_hbm, foot_ref, foot_sem)
    foot_copy.start()
    time_copy = pltpu.make_async_copy(time_hbm, time_ref, time_sem)
    time_copy.start()
    for k in range(8):
        rows = pl.ds(k * 144, 144)
        pltpu.make_async_copy(cov_hbm.at[rows], cov.at[rows], cov_sem).start()
    pl.semaphore_wait(barrier, 22)
    for to_cell in columns:
        signal(ready, to_cell, tm)

    owner_hot = hot_of(owner_ref[...], DEV).astype(BF16)
    obs_hot = hot_of(obs_ref[...], OBS).astype(BF16)
    dir_tile = mul(jnp.broadcast_to(dir_ref[...], (8, OBS)).astype(BF16), obs_hot)[0:1, :]
    fields = mul(
        owner_hot,
        placings(rank_ref[...], dir_tile, block_ref[...].astype(F32), step_ref[...].astype(F32)),
        NT,
    ).astype(BF16)
    lane_base = x * CAP
    shift = jnp.where(
        sub_iota(CAP, LANES) + lane_base == lax.broadcasted_iota(jnp.int32, (CAP, LANES), 1),
        1.0,
        0.0,
    ).astype(BF16)
    meta_ref[:, 0, :] = mul(fields[:, :CAP], shift)
    meta_ref[:, 1, :] = (
        mul(fields[:, CAP : 2 * CAP], shift) * 128.0 + mul(fields[:, 2 * CAP :], shift)
    )
    foot_copy.wait()
    wide[...] = foot_ref[...].astype(F32)
    pl.semaphore_wait(ready, 7)

    def send_tile(to_cell, to_tm):
        peer = to_cell * 16 + to_tm
        remote(
            values.at[peer], got.at[me], tile_send, tile_recv.at[cell], to_cell, to_tm
        ).start()
        remote(
            meta_ref.at[peer], got_meta.at[me], meta_send, meta_recv.at[cell], to_cell, to_tm
        ).start()

    def turn(k):
        q = k % 4
        return 2 * (q + q // 2 - 2 * (q // 3)) + k // 4

    natural = [ys[dy] * 4 + xs[dx] for dy in range(4) for dx in range(4)]

    def gather(to_cell, j):
        peer = to_cell * 16 + natural[j]
        for r in range(CAP):
            slots[j, r : r + 1, :] = wide[pl.ds(index_ref[r, peer], 1), :]
        values[peer] = slots[j].astype(BF16)

    for j in range(16):
        gather(cell, j)
        if j > 1:
            send_tile(cell, natural[j - 1])
    send_tile(cell, natural[15])

    def gather_and_send(k, _):
        to_cell = (cell + turn(k)) % 8
        for j in range(16):
            gather(to_cell, j)
            if j:
                send_tile(to_cell, natural[j - 1])
        send_tile(to_cell, natural[15])
        return 0

    lax.fori_loop(1, 8, gather_and_send, 0)
    pltpu.make_async_copy(values.at[me], got.at[me], tile_recv.at[cell]).start()
    pltpu.make_async_copy(meta_ref.at[me], got_meta.at[me], meta_recv.at[cell]).start()

    acc[...] = jnp.zeros_like(acc)
    row_of = sub_iota(LANES, LANES).astype(F32)

    def load_meta(group):
        rows = got_meta[pl.ds(group * 16, 16)]
        return jnp.sum(rows.reshape(4, 4, 2, LANES), axis=1)

    def add_group(k, _):
        group = (cell + 8 - turn(k)) % 8
        arrived(got.at[pl.ds(group * 16, 16)], tile_recv.at[group])
        arrived(got_meta.at[pl.ds(group * 16, 16)], meta_recv.at[group])
        rows = load_meta(group)
        tiles = got[pl.ds(group * 16, 16)].reshape(512, LANES)
        for b in range(BLOCKS):
            for q in range(4):
                hots[b * 128 : b * 128 + 128, q * 128 : q * 128 + 128] = jnp.where(
                    row_of + b * 128.0 == rows[q, 1:2, :], rows[q, 0:1, :], 0.0
                ).astype(BF16)
        acc[...] += mul(hots[...], tiles)
        return 0

    lax.fori_loop(0, 8, add_group, 0)
    for b in range(BLOCKS):
        flux[cell, :, b * 128 : b * 128 + 128] = acc[b * 128 : b * 128 + 128, :].astype(BF16)

    partner = z * 2 + 1 - core
    up, down, far = z_cell(1), z_cell(3), z_cell(2)
    left, right, full = pl.ds(0, 512), pl.ds(512, ROWS - 512), pl.ds(0, ROWS)
    z_copies = []

    def z_go(block, cols, to_cell, at):
        ref = flux.at[block, :, cols]
        copy = remote(ref, ref, z_send.at[at], z_recv.at[at], to_cell, tm)
        copy.start()
        z_copies.append(copy)

    def z_wait(block, cols, at):
        arrived(flux.at[block, :, cols], z_recv.at[at])

    z_go(cell, left, up, 0)
    z_go(cell, right, down, 2)
    z_go(cell, right, up, 1)
    z_go(cell, left, down, 3)
    z_go(cell, full, partner, 4)

    time_copy.wait()
    time_sends = []
    for k in (1, 2, 3):
        peer = y_at(k)
        copy = remote(
            time_ref.at[:, pl.ds(pl.multiple_of(peer * 512, 512), 512)],
            time_a.at[y],
            time_send.at[k - 1],
            time_recv.at[k - 1],
            cell,
            peer * 4 + x,
        )
        copy.start()
        time_sends.append(copy)
        peer = x_at(k)
        for other in range(4):
            copy = remote(
                time_ref.at[:, pl.ds(pl.multiple_of((other * 4 + peer) * 128, 128), 128)],
                time_b.at[x, :, pl.ds(other * 128, 128)],
                time_send.at[3 * k + other + (k - 1)],
                time_recv.at[3 * k + other + (k - 1)],
                cell,
                y * 4 + peer,
            )
            copy.start()
            time_sends.append(copy)
    time_a[y] = time_ref[:, pl.ds(pl.multiple_of(y * 512, 512), 512)]
    for other in range(4):
        time_b[x, :, other * 128 : other * 128 + 128] = time_ref[
            :, pl.ds(pl.multiple_of((other * 4 + x) * 128, 128), 128)
        ]

    arrived(cov, cov_sem)

    def other_core(c):
        return c // 2 * 2 + 1 - c % 2

    def mix(block, first=False):
        cols = pl.ds(pl.multiple_of(block * ROWS, 128), ROWS)
        product = mul(cov[:, cols], flux[block], NT)
        if first:
            mixed[...] = product
        else:
            mixed[...] += product

    mix(cell, True)
    z_wait(down, left, 0)
    z_go(down, left, up, 5)
    z_go(down, left, partner, 7)
    z_wait(up, right, 2)
    z_go(up, right, down, 6)
    z_go(up, right, partner, 8)
    z_wait(other_core(cell), full, 4)
    mix(other_core(cell))
    z_wait(down, right, 1)
    z_go(down, right, partner, 9)
    z_wait(up, left, 3)
    z_go(up, left, partner, 10)
    mix(down)
    mix(up)
    z_wait(other_core(down), left, 7)
    z_wait(other_core(down), right, 9)
    mix(other_core(down))
    z_wait(other_core(up), right, 8)
    z_wait(other_core(up), left, 10)
    mix(other_core(up))
    z_wait(far, left, 5)
    z_go(far, left, partner, 11)
    z_wait(far, right, 6)
    z_go(far, right, partner, 12)
    mix(far)
    z_wait(other_core(far), left, 11)
    z_wait(other_core(far), right, 12)
    mix(other_core(far))

    mix_a[:, pl.ds(pl.multiple_of(x * 128, 128), 128)] = mixed[:HALF, :].astype(BF16)
    mix_b[:, pl.ds(pl.multiple_of(y * 128, 128), 128)] = mixed[HALF:, :].astype(BF16)
    ag_copies = []

    def ag_go(buf, at_lane, rows, to_tm, at):
        ref = buf.at[rows, pl.ds(pl.multiple_of(at_lane * 128, 128), 128)]
        copy = remote(ref, ref, ag_send.at[at], ag_recv.at[at], cell, to_tm)
        copy.start()
        ag_copies.append(copy)

    def ag_wait(buf, at_lane, rows, at):
        arrived(buf.at[rows, pl.ds(pl.multiple_of(at_lane * 128, 128), 128)], ag_recv.at[at])

    first, second = pl.ds(0, QUARTER), pl.ds(QUARTER, QUARTER)
    x_up, x_down = y * 4 + x_at(1), y * 4 + x_at(3)
    y_up, y_down = y_at(1) * 4 + x, y_at(3) * 4 + x
    ag_go(mix_a, x, first, x_up, 0)
    ag_go(mix_a, x, second, x_down, 1)
    ag_go(mix_b, y, first, y_up, 2)
    ag_go(mix_b, y, second, y_down, 3)
    ag_go(mix_a, x, second, x_up, 4)
    ag_go(mix_a, x, first, x_down, 5)
    ag_go(mix_b, y, second, y_up, 6)
    ag_go(mix_b, y, first, y_down, 7)
    ag_wait(mix_a, x_at(3), first, 0)
    ag_go(mix_a, x_at(3), first, x_up, 8)
    ag_wait(mix_a, x_at(1), second, 1)
    ag_go(mix_a, x_at(1), second, x_down, 9)
    ag_wait(mix_b, y_at(3), first, 2)
    ag_go(mix_b, y_at(3), first, y_up, 10)
    ag_wait(mix_b, y_at(1), second, 3)
    ag_go(mix_b, y_at(1), second, y_down, 11)
    for k in (1, 2, 3):
        arrived(time_a.at[y_at(4 - k)], time_recv.at[k - 1])
        for other in range(4):
            arrived(
                time_b.at[x_at(4 - k), :, pl.ds(other * 128, 128)],
                time_recv.at[3 * k + other + (k - 1)],
            )
    ag_wait(mix_a, x_at(3), second, 4)
    ag_wait(mix_a, x_at(1), first, 5)
    ag_wait(mix_b, y_at(3), second, 6)
    ag_wait(mix_b, y_at(1), first, 7)
    ag_wait(mix_a, x_at(2), first, 8)
    ag_wait(mix_a, x_at(2), second, 9)
    rs_copies = []
    for k in (2, 1, 3):
        peer = y_at(k)
        part_a[k - 1] = mul(mix_a[...], time_a[peer], NT).astype(BF16)
        copy = remote(
            part_a.at[k - 1],
            in_a.at[k - 1],
            rs_send.at[k - 1],
            rs_recv.at[k - 1],
            cell,
            peer * 4 + x,
        )
        copy.start()
        rs_copies.append(copy)
        if k == 2:
            ag_wait(mix_b, y_at(2), first, 10)
            ag_wait(mix_b, y_at(2), second, 11)
        peer = x_at(k)
        part_b[k - 1] = mul(mix_b[...], time_b[peer], NT).astype(BF16)
        copy = remote(
            part_b.at[k - 1],
            in_b.at[k - 1],
            rs_send.at[k + 2],
            rs_recv.at[k + 2],
            cell,
            y * 4 + peer,
        )
        copy.start()
        rs_copies.append(copy)
    mixed[:HALF, :] = mul(mix_a[...], time_a[y], NT)
    mixed[HALF:, :] = mul(mix_b[...], time_b[x], NT)
    for k in (1, 3, 2):
        arrived(in_a.at[k - 1], rs_recv.at[k - 1])
        mixed[:HALF, :] += in_a[k - 1].astype(F32)
        arrived(in_b.at[k - 1], rs_recv.at[k + 2])
        mixed[HALF:, :] += in_b[k - 1].astype(F32)
    for b in range(BLOCKS):
        smooth[b * 128 : b * 128 + 128, :] = mixed[b * 128 : b * 128 + 128, :].T.astype(BF16)

    def dot_group(k):
        group = away(k)
        rows = load_meta(group)
        products[...] = mul(smooth[...], got[pl.ds(group * 16, 16)].reshape(512, LANES), NT)
        for q in range(4):
            picked = jnp.zeros((LANES, LANES), F32)
            for b in range(BLOCKS):
                picked += jnp.where(
                    row_of + b * 128.0 == rows[q, 1:2, :],
                    products[b * 128 : b * 128 + 128, q * 128 : q * 128 + 128],
                    0.0,
                )
            dots[group * 4 + q] = jnp.sum(picked, axis=0, keepdims=True)

    def send_dots(k, peers):
        group = away(k)
        for to_tm in peers:
            remote(
                dots.at[group * 4 + to_tm // 4], dots_back.at[me], back_send, back_recv, group, to_tm
            ).start()

    dot_group(0)

    def dots_and_send(k, _):
        send_dots(k - 1, planes)
        dot_group(k)
        return 0

    lax.fori_loop(1, 8, dots_and_send, 0)
    send_dots(7, planes[:15])
    dots_back[me] = dots[me // 4]
    owner_hot = hot_of(owner_ref[...], DEV).astype(BF16)
    obs_hot = hot_of(obs_ref[...], OBS).astype(BF16)
    in_slot = sub_iota(CAP, TILES).astype(F32) == rank_ref[...]
    arrived(dots_back.at[pl.ds(0, DEV - 1)], back_recv)
    by_rank[...] = dots_back[:, 0, :].T
    own = jnp.concatenate(split3(by_rank[pl.ds(pl.multiple_of(lane_base, CAP), CAP), :]), axis=0)
    parts = mul(own, owner_hot)
    tile_dots = jnp.sum(
        jnp.where(in_slot, parts[:CAP] + parts[CAP : 2 * CAP] + parts[2 * CAP :], 0.0),
        axis=0,
        keepdims=True,
    )
    high, middle, low = split3(tile_dots)
    three = jnp.concatenate(
        [high.astype(F32), middle.astype(F32), low.astype(F32), jnp.zeros((5, TILES), F32)], axis=0
    ).astype(BF16)
    direction, residual = dir_ref[...], res_ref[...]
    applied = jnp.sum(mul(three, obs_hot, NT), axis=0, keepdims=True)
    applied = applied + noise_ref[...] * direction

    lanes = lax.broadcasted_iota(jnp.int32, (1, LANES), 1)
    row = jnp.zeros((1, LANES), F32)
    for at, value in enumerate(
        (residual * residual, direction * applied, residual * applied, applied * applied)
    ):
        row = jnp.where(lanes == at, jnp.sum(value, axis=1, keepdims=True), row)
    sums[...] = row
    to_others(
        lambda to_cell, to_tm: remote(
            sums, sums_in.at[me], sum_send, sum_recv, to_cell, to_tm
        ).start()
    )
    sums_in[me] = row
    arrived(sums_in.at[pl.ds(0, DEV - 1)], sum_recv)
    total = jnp.sum(sums_in[...], axis=0)

    def total_of(at):
        return jnp.sum(jnp.where(lanes == at, total, 0.0), axis=1, keepdims=True)

    norm_now, curvature, cross_term, image_norm = (total_of(at) for at in range(4))
    step_size = norm_now / curvature
    norm_next = norm_now - 2.0 * step_size * cross_term + step_size * step_size * image_norm
    applied_ref[...] = applied
    size_ref[...] = jnp.broadcast_to(step_size, (1, OBS))
    ratio_ref[...] = jnp.broadcast_to(norm_next / norm_now, (1, OBS))

    arrived(values.at[pl.ds(0, DEV - 1)], tile_send)
    arrived(meta_ref.at[pl.ds(0, DEV - 1)], meta_send)
    for copy in time_sends + z_copies + ag_copies + rs_copies:
        copy.wait_send()
    arrived(dots_back.at[pl.ds(0, DEV - 1)], back_send)
    arrived(sums_in.at[pl.ds(0, DEV - 1)], sum_send)


def whole(*operands):
    vmem = pl.BlockSpec(memory_space=pltpu.VMEM)
    dma = pltpu.SemaphoreType.DMA
    row = jax.ShapeDtypeStruct((1, OBS), F32)
    return pl.pallas_call(
        main_kernel,
        out_shape=(row, row, row),
        in_specs=[vmem] * 8
        + [pl.BlockSpec(memory_space=pltpu.SMEM)]
        + [pl.BlockSpec(memory_space=pl.ANY)] * 3,
        out_specs=(vmem,) * 3,
        scratch_shapes=[
            pltpu.VMEM((TILES, LANES), BF16),
            pltpu.VMEM((LANES, 16 * LANES), BF16),
            pltpu.VMEM((DEV, 2, LANES), F32),
            pltpu.VMEM((TILES, LANES), F32),
            pltpu.VMEM((16, CAP, LANES), F32),
            pltpu.VMEM((DEV, CAP, LANES), BF16),
            pltpu.VMEM((ROWS, 8 * ROWS), BF16),
            pltpu.VMEM((DEV, CAP, LANES), BF16),
            pltpu.VMEM((DEV, 2, LANES), F32),
            pltpu.VMEM((ROWS, 512), BF16),
            pltpu.VMEM((ROWS, LANES), F32),
            pltpu.VMEM((8, LANES, ROWS), BF16),
            pltpu.VMEM((ROWS, LANES), F32),
            pltpu.VMEM((HALF, 512), BF16),
            pltpu.VMEM((HALF, 512), BF16),
            pltpu.VMEM((4, LANES, 512), BF16),
            pltpu.VMEM((4, LANES, 512), BF16),
            pltpu.VMEM((3, HALF, LANES), BF16),
            pltpu.VMEM((3, HALF, LANES), BF16),
            pltpu.VMEM((3, HALF, LANES), BF16),
            pltpu.VMEM((3, HALF, LANES), BF16),
            pltpu.VMEM((ROWS, LANES), BF16),
            pltpu.VMEM((ROWS, 512), F32),
            pltpu.VMEM((DEV // 4, 1, LANES), F32),
            pltpu.VMEM((DEV, 1, LANES), F32),
            pltpu.VMEM((LANES, DEV), F32),
            pltpu.VMEM((1, LANES), F32),
            pltpu.VMEM((DEV, 1, LANES), F32),
            pltpu.SemaphoreType.REGULAR,
            dma,
            dma,
            dma,
            dma,
            dma((8,)),
            dma,
            dma((8,)),
            dma((13,)),
            dma((13,)),
            dma((15,)),
            dma((15,)),
            dma((12,)),
            dma((12,)),
            dma((6,)),
            dma((6,)),
            dma,
            dma,
            dma,
            dma,
        ],
        compiler_params=pltpu.CompilerParams(
            collective_id=0, has_side_effects=True, vmem_limit_bytes=60 * 2**20
        ),
        name="whole",
    )(*operands)


def local(
    solution,
    residual,
    direction,
    noise_var,
    footprints,
    tile_owner,
    tile_block,
    tile_step,
    tile_obs,
    cell_cov,
    time_cov,
):
    row = functools.partial(jnp.reshape, shape=(1, OBS))
    tile_row = functools.partial(jnp.reshape, shape=(1, TILES))
    owner = tile_row(tile_owner)
    index, rank = prep(owner)
    outs = whole(
        row(residual),
        row(direction),
        row(noise_var),
        owner,
        tile_row(tile_block),
        tile_row(tile_step),
        tile_row(tile_obs),
        rank,
        index,
        footprints,
        cell_cov,
        time_cov,
    )
    applied, step_size, ratio = (out.reshape(OBS) for out in outs)
    new_residual = residual - step_size * applied
    return solution + step_size * direction, new_residual, new_residual + ratio * direction


def solution(mesh):
    both = P(CELL_TM)
    in_specs = (both,) * 4 + (P(CELL_TM, None),) * 2 + (both,) * 3
    in_specs += (P("cell", None), P("tm", None))
    return jax.shard_map(
        local, mesh=mesh, in_specs=in_specs, out_specs=(both,) * 3, check_vma=False
    )
```

```python
import functools

import jax
import jax.numpy as jnp
from jax import lax
from jax.experimental import pallas as pl
from jax.experimental.pallas import tpu as pltpu
from jax.sharding import PartitionSpec as P

MESH = pl.DeviceIdType.MESH
CELL_TM = ("cell", "tm")
NN = (((1,), (0,)), ((), ()))
NT = (((1,), (1,)), ((), ()))
DEV = 128
CAP = 32
LANES = 128
OBS = 256
TILES = 2048
SLOTS = DEV * CAP
ROWS = 1152
BLOCKS = 9
HALF = ROWS // 2
QUARTER = ROWS // 4
BF16 = jnp.bfloat16
F32 = jnp.float32


def mul(a, b, dims=NN):
    return lax.dot_general(a, b, dims, preferred_element_type=F32)


def sub_iota(rows, cols):
    return lax.broadcasted_iota(jnp.int32, (rows, cols), 0)


def hot_of(index, rows):
    return jnp.where(sub_iota(rows, index.shape[1]) == index, 1.0, 0.0)


def split3(value):
    high = value.astype(BF16)
    rest = value - high.astype(F32)
    middle = rest.astype(BF16)
    return high, middle, (rest - middle.astype(F32)).astype(BF16)


def placings(rank, *rows):
    in_slot = sub_iota(CAP, TILES).astype(F32) == rank
    return jnp.concatenate([jnp.where(in_slot, row, 0.0).astype(BF16) for row in rows], axis=0)


def prep_kernel(owner_ref, index_ref, rank_ref):
    width = 256
    above = jnp.where(
        sub_iota(width, width) < lax.broadcasted_iota(jnp.int32, (width, width), 1), 1.0, 0.0
    ).astype(BF16)
    carry = jnp.zeros((DEV, 1), F32)
    for at in range(0, TILES, width):
        hot = hot_of(owner_ref[:, at : at + width], DEV)
        before = mul(hot.astype(BF16), above) + carry
        rank_ref[:, at : at + width] = jnp.sum(hot * before, axis=0, keepdims=True)
        carry = before[:, width - 1 : width] + hot[:, width - 1 : width]
    owner_hot = hot_of(owner_ref[...], DEV).astype(BF16)
    tile = lax.broadcasted_iota(jnp.int32, (1, TILES), 1)
    index = mul(
        placings(rank_ref[...], (tile // 256).astype(F32), (tile % 256).astype(F32)), owner_hot, NT
    )
    index_ref[...] = (index[:CAP] * 256.0 + index[CAP:]).astype(jnp.int32)


def prep(owner):
    vmem = pl.BlockSpec(memory_space=pltpu.VMEM)
    return pl.pallas_call(
        prep_kernel,
        out_shape=(
            jax.ShapeDtypeStruct((CAP, DEV), jnp.int32),
            jax.ShapeDtypeStruct((1, TILES), F32),
        ),
        in_specs=[vmem],
        out_specs=(vmem, vmem),
        name="prep",
    )(owner)


def main_kernel(
    res_ref,
    dir_ref,
    noise_ref,
    owner_ref,
    block_ref,
    step_ref,
    obs_ref,
    rank_ref,
    index_ref,
    foot_hbm,
    cov_hbm,
    time_hbm,
    applied_ref,
    size_ref,
    ratio_ref,
    foot_ref,
    time_ref,
    meta_ref,
    wide,
    slots,
    values,
    cov,
    got,
    got_meta,
    hots,
    acc,
    flux,
    mixed,
    mix_a,
    mix_b,
    time_a,
    time_b,
    part_a,
    part_b,
    in_a,
    in_b,
    smooth,
    products,
    dots,
    dots_back,
    by_rank,
    sums,
    sums_in,
    ready,
    foot_sem,
    time_sem,
    cov_sem,
    tile_send,
    tile_recv,
    meta_send,
    meta_recv,
    z_send,
    z_recv,
    time_send,
    time_recv,
    ag_send,
    ag_recv,
    rs_send,
    rs_recv,
    back_send,
    back_recv,
    sum_send,
    sum_recv,
):
    cell, tm = lax.axis_index("cell"), lax.axis_index("tm")
    me = cell * 16 + tm
    z, core = cell // 2, cell % 2
    y, x = tm // 4, tm % 4
    xs = [(x + k) % 4 for k in range(4)]
    ys = [(y + k) % 4 for k in range(4)]
    far_first = sorted(
        ((dy, dx) for dy in range(4) for dx in range(4)),
        key=lambda at: -(min(at[0], 4 - at[0]) + min(at[1], 4 - at[1])),
    )
    planes = [ys[dy] * 4 + xs[dx] for dy, dx in far_first]

    def x_at(k):
        return xs[k]

    def y_at(k):
        return ys[k]

    def z_cell(k):
        return (z + k) % 4 * 2 + core

    def remote(src, dst, send, recv, to_cell, to_tm):
        return pltpu.make_async_remote_copy(
            src_ref=src,
            dst_ref=dst,
            send_sem=send,
            recv_sem=recv,
            device_id=(to_cell, to_tm),
            device_id_type=MESH,
        )

    def arrived(ref, sem):
        pltpu.make_async_copy(ref, ref, sem).wait()

    def away(k):
        return (cell + 4 + (k % 2 * 2 - 1) * ((k + 1) // 2)) % 8

    def to_others(send):
        def at_cell(k, _):
            to_cell = away(k)
            for to_tm in planes:
                send(to_cell, to_tm)
            return 0

        lax.fori_loop(0, 7, at_cell, 0)
        for to_tm in planes[:15]:
            send(cell, to_tm)

    barrier = pltpu.get_barrier_semaphore()
    columns = [(cell + k) % 8 for k in (4, 5, 3, 6, 2, 7, 1)]

    def signal(sem, to_cell, to_tm):
        pl.semaphore_signal(sem, inc=1, device_id=(to_cell, to_tm), device_id_type=MESH)

    for to_tm in planes[:15]:
        signal(barrier, cell, to_tm)
    for to_cell in columns:
        signal(barrier, to_cell, tm)
    foot_copy = pltpu.make_async_copy(foot_hbm, foot_ref, foot_sem)
    foot_copy.start()
    time_copy = pltpu.make_async_copy(time_hbm, time_ref, time_sem)
    time_copy.start()
    for k in range(8):
        rows = pl.ds(k * 144, 144)
        pltpu.make_async_copy(cov_hbm.at[rows], cov.at[rows], cov_sem).start()
    pl.semaphore_wait(barrier, 22)
    for to_cell in columns:
        signal(ready, to_cell, tm)

    owner_hot = hot_of(owner_ref[...], DEV).astype(BF16)
    obs_hot = hot_of(obs_ref[...], OBS).astype(BF16)
    dir_tile = mul(jnp.broadcast_to(dir_ref[...], (8, OBS)).astype(BF16), obs_hot)[0:1, :]
    fields = mul(
        owner_hot,
        placings(rank_ref[...], dir_tile, block_ref[...].astype(F32), step_ref[...].astype(F32)),
        NT,
    ).astype(BF16)
    lane_base = x * CAP
    lane = lax.broadcasted_iota(jnp.int32, (CAP, LANES), 1)

    def to_quarter(value, quarter):
        hot = jnp.where(sub_iota(CAP, LANES) + quarter * CAP == lane, 1.0, 0.0)
        return mul(value, hot.astype(BF16))

    meta_ref[:, 0, :] = (
        to_quarter(fields[:, :CAP], x)
        + to_quarter(fields[:, CAP : 2 * CAP], xs[2]) * 128.0
        + to_quarter(fields[:, 2 * CAP :], xs[2])
    )
    foot_copy.wait()
    wide[...] = foot_ref[...].astype(F32)
    pl.semaphore_wait(ready, 7)

    def send_tile(to_cell, to_tm):
        peer = to_cell * 16 + to_tm
        remote(
            values.at[peer], got.at[me], tile_send, tile_recv.at[cell], to_cell, to_tm
        ).start()
        remote(
            meta_ref.at[peer], got_meta.at[me], meta_send, meta_recv.at[cell], to_cell, to_tm
        ).start()

    def turn(k):
        q = k % 4
        return 2 * (q + q // 2 - 2 * (q // 3)) + k // 4

    natural = [ys[dy] * 4 + xs[dx] for dy in range(4) for dx in range(4)]

    def gather(to_cell, j):
        peer = to_cell * 16 + natural[j]
        for r in range(CAP):
            slots[j, r : r + 1, :] = wide[pl.ds(index_ref[r, peer], 1), :]
        values[peer] = slots[j].astype(BF16)

    for j in range(16):
        gather(cell, j)
        if j > 1:
            send_tile(cell, natural[j - 1])
    send_tile(cell, natural[15])

    def gather_and_send(k, _):
        to_cell = (cell + turn(k)) % 8
        for j in range(16):
            gather(to_cell, j)
            if j:
                send_tile(to_cell, natural[j - 1])
        send_tile(to_cell, natural[15])
        return 0

    lax.fori_loop(1, 8, gather_and_send, 0)
    pltpu.make_async_copy(values.at[me], got.at[me], tile_recv.at[cell]).start()
    pltpu.make_async_copy(meta_ref.at[me], got_meta.at[me], meta_recv.at[cell]).start()

    acc[...] = jnp.zeros_like(acc)
    row_of = sub_iota(LANES, LANES).astype(F32)

    quarter_of = lax.broadcasted_iota(jnp.int32, (1, LANES), 1) // CAP

    def load_meta(group):
        rows = got_meta[pl.ds(group * 16, 16)].reshape(4, 4, LANES)
        out = []
        for q in range(4):
            direction = place = jnp.zeros((1, LANES), F32)
            for j in range(4):
                row = rows[q, j : j + 1, :]
                direction = jnp.where(quarter_of == j, row, direction)
                place = jnp.where(quarter_of == (j + 2) % 4, row, place)
            place = jnp.concatenate([place[:, 64:], place[:, :64]], axis=1)
            block = jnp.floor(place * (1.0 / 128.0))
            out.append((direction, block, place - block * 128.0))
        return out

    def add_group(k, _):
        group = (cell + 8 - turn(k)) % 8
        arrived(got.at[pl.ds(group * 16, 16)], tile_recv.at[group])
        arrived(got_meta.at[pl.ds(group * 16, 16)], meta_recv.at[group])
        rows = load_meta(group)
        tiles = got[pl.ds(group * 16, 16)].reshape(512, LANES)
        for q, (direction, block, step) in enumerate(rows):
            hot = jnp.where(row_of == step, direction, 0.0).astype(BF16)
            for b in range(BLOCKS):
                hots[b * 128 : b * 128 + 128, q * 128 : q * 128 + 128] = hot * jnp.where(
                    block == b, 1.0, 0.0
                ).astype(BF16)
        acc[...] += mul(hots[...], tiles)
        return 0

    lax.fori_loop(0, 8, add_group, 0)
    for b in range(BLOCKS):
        flux[cell, :, b * 128 : b * 128 + 128] = acc[b * 128 : b * 128 + 128, :].astype(BF16)

    partner = z * 2 + 1 - core
    up, down, far = z_cell(1), z_cell(3), z_cell(2)
    left, right, full = pl.ds(0, 512), pl.ds(512, ROWS - 512), pl.ds(0, ROWS)
    z_copies = []

    def z_go(block, cols, to_cell, at):
        ref = flux.at[block, :, cols]
        copy = remote(ref, ref, z_send.at[at], z_recv.at[at], to_cell, tm)
        copy.start()
        z_copies.append(copy)

    def z_wait(block, cols, at):
        arrived(flux.at[block, :, cols], z_recv.at[at])

    z_go(cell, left, up, 0)
    z_go(cell, right, down, 2)
    z_go(cell, right, up, 1)
    z_go(cell, left, down, 3)
    z_go(cell, full, partner, 4)

    time_copy.wait()
    time_sends = []
    for k in (1, 2, 3):
        peer = y_at(k)
        copy = remote(
            time_ref.at[:, pl.ds(pl.multiple_of(peer * 512, 512), 512)],
            time_a.at[y],
            time_send.at[k - 1],
            time_recv.at[k - 1],
            cell,
            peer * 4 + x,
        )
        copy.start()
        time_sends.append(copy)
        peer = x_at(k)
        for other in range(4):
            copy = remote(
                time_ref.at[:, pl.ds(pl.multiple_of((other * 4 + peer) * 128, 128), 128)],
                time_b.at[x, :, pl.ds(other * 128, 128)],
                time_send.at[3 * k + other + (k - 1)],
                time_recv.at[3 * k + other + (k - 1)],
                cell,
                y * 4 + peer,
            )
            copy.start()
            time_sends.append(copy)
    time_a[y] = time_ref[:, pl.ds(pl.multiple_of(y * 512, 512), 512)]
    for other in range(4):
        time_b[x, :, other * 128 : other * 128 + 128] = time_ref[
            :, pl.ds(pl.multiple_of((other * 4 + x) * 128, 128), 128)
        ]

    arrived(cov, cov_sem)

    def other_core(c):
        return c // 2 * 2 + 1 - c % 2

    def mix(block, first=False):
        cols = pl.ds(pl.multiple_of(block * ROWS, 128), ROWS)
        product = mul(cov[:, cols], flux[block], NT)
        if first:
            mixed[...] = product
        else:
            mixed[...] += product

    mix(cell, True)
    z_wait(down, left, 0)
    z_go(down, left, up, 5)
    z_go(down, left, partner, 7)
    z_wait(up, right, 2)
    z_go(up, right, down, 6)
    z_go(up, right, partner, 8)
    z_wait(other_core(cell), full, 4)
    mix(other_core(cell))
    z_wait(down, right, 1)
    z_go(down, right, partner, 9)
    z_wait(up, left, 3)
    z_go(up, left, partner, 10)
    mix(down)
    mix(up)
    z_wait(other_core(down), left, 7)
    z_wait(other_core(down), right, 9)
    mix(other_core(down))
    z_wait(other_core(up), right, 8)
    z_wait(other_core(up), left, 10)
    mix(other_core(up))
    z_wait(far, left, 5)
    z_go(far, left, partner, 11)
    z_wait(far, right, 6)
    z_go(far, right, partner, 12)
    mix(far)
    z_wait(other_core(far), left, 11)
    z_wait(other_core(far), right, 12)
    mix(other_core(far))

    mix_a[:, pl.ds(pl.multiple_of(x * 128, 128), 128)] = mixed[:HALF, :].astype(BF16)
    mix_b[:, pl.ds(pl.multiple_of(y * 128, 128), 128)] = mixed[HALF:, :].astype(BF16)
    ag_copies = []

    def ag_go(buf, at_lane, rows, to_tm, at):
        ref = buf.at[rows, pl.ds(pl.multiple_of(at_lane * 128, 128), 128)]
        copy = remote(ref, ref, ag_send.at[at], ag_recv.at[at], cell, to_tm)
        copy.start()
        ag_copies.append(copy)

    def ag_wait(buf, at_lane, rows, at):
        arrived(buf.at[rows, pl.ds(pl.multiple_of(at_lane * 128, 128), 128)], ag_recv.at[at])

    first, second = pl.ds(0, QUARTER), pl.ds(QUARTER, QUARTER)
    x_up, x_down = y * 4 + x_at(1), y * 4 + x_at(3)
    y_up, y_down = y_at(1) * 4 + x, y_at(3) * 4 + x
    ag_go(mix_a, x, first, x_up, 0)
    ag_go(mix_a, x, second, x_down, 1)
    ag_go(mix_b, y, first, y_up, 2)
    ag_go(mix_b, y, second, y_down, 3)
    ag_go(mix_a, x, second, x_up, 4)
    ag_go(mix_a, x, first, x_down, 5)
    ag_go(mix_b, y, second, y_up, 6)
    ag_go(mix_b, y, first, y_down, 7)
    ag_wait(mix_a, x_at(3), first, 0)
    ag_go(mix_a, x_at(3), first, x_up, 8)
    ag_wait(mix_a, x_at(1), second, 1)
    ag_go(mix_a, x_at(1), second, x_down, 9)
    ag_wait(mix_b, y_at(3), first, 2)
    ag_go(mix_b, y_at(3), first, y_up, 10)
    ag_wait(mix_b, y_at(1), second, 3)
    ag_go(mix_b, y_at(1), second, y_down, 11)
    for k in (1, 2, 3):
        arrived(time_a.at[y_at(4 - k)], time_recv.at[k - 1])
        for other in range(4):
            arrived(
                time_b.at[x_at(4 - k), :, pl.ds(other * 128, 128)],
                time_recv.at[3 * k + other + (k - 1)],
            )
    ag_wait(mix_a, x_at(3), second, 4)
    ag_wait(mix_a, x_at(1), first, 5)
    ag_wait(mix_b, y_at(3), second, 6)
    ag_wait(mix_b, y_at(1), first, 7)
    ag_wait(mix_a, x_at(2), first, 8)
    ag_wait(mix_a, x_at(2), second, 9)
    rs_copies = []
    for k in (2, 1, 3):
        peer = y_at(k)
        part_a[k - 1] = mul(mix_a[...], time_a[peer], NT).astype(BF16)
        copy = remote(
            part_a.at[k - 1],
            in_a.at[k - 1],
            rs_send.at[k - 1],
            rs_recv.at[k - 1],
            cell,
            peer * 4 + x,
        )
        copy.start()
        rs_copies.append(copy)
        if k == 2:
            ag_wait(mix_b, y_at(2), first, 10)
            ag_wait(mix_b, y_at(2), second, 11)
        peer = x_at(k)
        part_b[k - 1] = mul(mix_b[...], time_b[peer], NT).astype(BF16)
        copy = remote(
            part_b.at[k - 1],
            in_b.at[k - 1],
            rs_send.at[k + 2],
            rs_recv.at[k + 2],
            cell,
            y * 4 + peer,
        )
        copy.start()
        rs_copies.append(copy)
    mixed[:HALF, :] = mul(mix_a[...], time_a[y], NT)
    mixed[HALF:, :] = mul(mix_b[...], time_b[x], NT)
    for k in (1, 3, 2):
        arrived(in_a.at[k - 1], rs_recv.at[k - 1])
        mixed[:HALF, :] += in_a[k - 1].astype(F32)
        arrived(in_b.at[k - 1], rs_recv.at[k + 2])
        mixed[HALF:, :] += in_b[k - 1].astype(F32)
    for b in range(BLOCKS):
        smooth[b * 128 : b * 128 + 128, :] = mixed[b * 128 : b * 128 + 128, :].T.astype(BF16)

    def dot_group(k):
        group = away(k)
        rows = load_meta(group)
        products[...] = mul(smooth[...], got[pl.ds(group * 16, 16)].reshape(512, LANES), NT)
        for q, (_, block, step) in enumerate(rows):
            cols = slice(q * 128, q * 128 + 128)
            picked = products[0:128, cols]
            for b in range(1, BLOCKS):
                picked = jnp.where(block == b, products[b * 128 : b * 128 + 128, cols], picked)
            picked = jnp.where(row_of == step, picked, 0.0)
            dots[group * 4 + q] = jnp.sum(picked, axis=0, keepdims=True)

    def send_dots(k, peers):
        group = away(k)
        for to_tm in peers:
            remote(
                dots.at[group * 4 + to_tm // 4], dots_back.at[me], back_send, back_recv, group, to_tm
            ).start()

    dot_group(0)

    def dots_and_send(k, _):
        send_dots(k - 1, planes)
        dot_group(k)
        return 0

    lax.fori_loop(1, 8, dots_and_send, 0)
    send_dots(7, planes[:15])
    dots_back[me] = dots[me // 4]
    owner_hot = hot_of(owner_ref[...], DEV).astype(BF16)
    obs_hot = hot_of(obs_ref[...], OBS).astype(BF16)
    in_slot = sub_iota(CAP, TILES).astype(F32) == rank_ref[...]
    arrived(dots_back.at[pl.ds(0, DEV - 1)], back_recv)
    by_rank[...] = dots_back[:, 0, :].T
    own = jnp.concatenate(split3(by_rank[pl.ds(pl.multiple_of(lane_base, CAP), CAP), :]), axis=0)
    parts = mul(own, owner_hot)
    tile_dots = jnp.sum(
        jnp.where(in_slot, parts[:CAP] + parts[CAP : 2 * CAP] + parts[2 * CAP :], 0.0),
        axis=0,
        keepdims=True,
    )
    high, middle, low = split3(tile_dots)
    three = jnp.concatenate(
        [high.astype(F32), middle.astype(F32), low.astype(F32), jnp.zeros((5, TILES), F32)], axis=0
    ).astype(BF16)
    direction, residual = dir_ref[...], res_ref[...]
    applied = jnp.sum(mul(three, obs_hot, NT), axis=0, keepdims=True)
    applied = applied + noise_ref[...] * direction

    lanes = lax.broadcasted_iota(jnp.int32, (1, LANES), 1)
    row = jnp.zeros((1, LANES), F32)
    for at, value in enumerate(
        (residual * residual, direction * applied, residual * applied, applied * applied)
    ):
        row = jnp.where(lanes == at, jnp.sum(value, axis=1, keepdims=True), row)
    sums[...] = row
    to_others(
        lambda to_cell, to_tm: remote(
            sums, sums_in.at[me], sum_send, sum_recv, to_cell, to_tm
        ).start()
    )
    sums_in[me] = row
    arrived(sums_in.at[pl.ds(0, DEV - 1)], sum_recv)
    total = jnp.sum(sums_in[...], axis=0)

    def total_of(at):
        return jnp.sum(jnp.where(lanes == at, total, 0.0), axis=1, keepdims=True)

    norm_now, curvature, cross_term, image_norm = (total_of(at) for at in range(4))
    step_size = norm_now / curvature
    norm_next = norm_now - 2.0 * step_size * cross_term + step_size * step_size * image_norm
    applied_ref[...] = applied
    size_ref[...] = jnp.broadcast_to(step_size, (1, OBS))
    ratio_ref[...] = jnp.broadcast_to(norm_next / norm_now, (1, OBS))

    arrived(values.at[pl.ds(0, DEV - 1)], tile_send)
    arrived(meta_ref.at[pl.ds(0, DEV - 1)], meta_send)
    for copy in time_sends + z_copies + ag_copies + rs_copies:
        copy.wait_send()
    arrived(dots_back.at[pl.ds(0, DEV - 1)], back_send)
    arrived(sums_in.at[pl.ds(0, DEV - 1)], sum_send)


def whole(*operands):
    vmem = pl.BlockSpec(memory_space=pltpu.VMEM)
    dma = pltpu.SemaphoreType.DMA
    row = jax.ShapeDtypeStruct((1, OBS), F32)
    return pl.pallas_call(
        main_kernel,
        out_shape=(row, row, row),
        in_specs=[vmem] * 8
        + [pl.BlockSpec(memory_space=pltpu.SMEM)]
        + [pl.BlockSpec(memory_space=pl.ANY)] * 3,
        out_specs=(vmem,) * 3,
        scratch_shapes=[
            pltpu.VMEM((TILES, LANES), BF16),
            pltpu.VMEM((LANES, 16 * LANES), BF16),
            pltpu.VMEM((DEV, 1, LANES), F32),
            pltpu.VMEM((TILES, LANES), F32),
            pltpu.VMEM((16, CAP, LANES), F32),
            pltpu.VMEM((DEV, CAP, LANES), BF16),
            pltpu.VMEM((ROWS, 8 * ROWS), BF16),
            pltpu.VMEM((DEV, CAP, LANES), BF16),
            pltpu.VMEM((DEV, 1, LANES), F32),
            pltpu.VMEM((ROWS, 512), BF16),
            pltpu.VMEM((ROWS, LANES), F32),
            pltpu.VMEM((8, LANES, ROWS), BF16),
            pltpu.VMEM((ROWS, LANES), F32),
            pltpu.VMEM((HALF, 512), BF16),
            pltpu.VMEM((HALF, 512), BF16),
            pltpu.VMEM((4, LANES, 512), BF16),
            pltpu.VMEM((4, LANES, 512), BF16),
            pltpu.VMEM((3, HALF, LANES), BF16),
            pltpu.VMEM((3, HALF, LANES), BF16),
            pltpu.VMEM((3, HALF, LANES), BF16),
            pltpu.VMEM((3, HALF, LANES), BF16),
            pltpu.VMEM((ROWS, LANES), BF16),
            pltpu.VMEM((ROWS, 512), F32),
            pltpu.VMEM((DEV // 4, 1, LANES), F32),
            pltpu.VMEM((DEV, 1, LANES), F32),
            pltpu.VMEM((LANES, DEV), F32),
            pltpu.VMEM((1, LANES), F32),
            pltpu.VMEM((DEV, 1, LANES), F32),
            pltpu.SemaphoreType.REGULAR,
            dma,
            dma,
            dma,
            dma,
            dma((8,)),
            dma,
            dma((8,)),
            dma((13,)),
            dma((13,)),
            dma((15,)),
            dma((15,)),
            dma((12,)),
            dma((12,)),
            dma((6,)),
            dma((6,)),
            dma,
            dma,
            dma,
            dma,
        ],
        compiler_params=pltpu.CompilerParams(
            collective_id=0, has_side_effects=True, vmem_limit_bytes=60 * 2**20
        ),
        name="whole",
    )(*operands)


def local(
    solution,
    residual,
    direction,
    noise_var,
    footprints,
    tile_owner,
    tile_block,
    tile_step,
    tile_obs,
    cell_cov,
    time_cov,
):
    row = functools.partial(jnp.reshape, shape=(1, OBS))
    tile_row = functools.partial(jnp.reshape, shape=(1, TILES))
    owner = tile_row(tile_owner)
    index, rank = prep(owner)
    outs = whole(
        row(residual),
        row(direction),
        row(noise_var),
        owner,
        tile_row(tile_block),
        tile_row(tile_step),
        tile_row(tile_obs),
        rank,
        index,
        footprints,
        cell_cov,
        time_cov,
    )
    applied, step_size, ratio = (out.reshape(OBS) for out in outs)
    new_residual = residual - step_size * applied
    return solution + step_size * direction, new_residual, new_residual + ratio * direction


def solution(mesh):
    both = P(CELL_TM)
    in_specs = (both,) * 4 + (P(CELL_TM, None),) * 2 + (both,) * 3
    in_specs += (P("cell", None), P("tm", None))
    return jax.shard_map(
        local, mesh=mesh, in_specs=in_specs, out_specs=(both,) * 3, check_vma=False
    )
```

```python
import functools

import jax
import jax.numpy as jnp
from jax import lax
from jax.experimental import pallas as pl
from jax.experimental.pallas import tpu as pltpu
from jax.sharding import PartitionSpec as P

MESH = pl.DeviceIdType.MESH
CELL_TM = ("cell", "tm")
NN = (((1,), (0,)), ((), ()))
NT = (((1,), (1,)), ((), ()))
DEV = 128
CAP = 32
LANES = 128
OBS = 256
TILES = 2048
SLOTS = DEV * CAP
ROWS = 1152
BLOCKS = 9
HALF = ROWS // 2
QUARTER = ROWS // 4
BF16 = jnp.bfloat16
F32 = jnp.float32


def mul(a, b, dims=NN):
    return lax.dot_general(a, b, dims, preferred_element_type=F32)


def sub_iota(rows, cols):
    return lax.broadcasted_iota(jnp.int32, (rows, cols), 0)


def hot_of(index, rows):
    return jnp.where(sub_iota(rows, index.shape[1]) == index, 1.0, 0.0)


def split3(value):
    high = value.astype(BF16)
    rest = value - high.astype(F32)
    middle = rest.astype(BF16)
    return high, middle, (rest - middle.astype(F32)).astype(BF16)


def placings(rank, *rows):
    in_slot = sub_iota(CAP, TILES).astype(F32) == rank
    return jnp.concatenate([jnp.where(in_slot, row, 0.0).astype(BF16) for row in rows], axis=0)


def prep_kernel(owner_ref, index_ref, rank_ref):
    width = 256
    above = jnp.where(
        sub_iota(width, width) < lax.broadcasted_iota(jnp.int32, (width, width), 1), 1.0, 0.0
    ).astype(BF16)
    carry = jnp.zeros((DEV, 1), F32)
    for at in range(0, TILES, width):
        hot = hot_of(owner_ref[:, at : at + width], DEV)
        before = mul(hot.astype(BF16), above) + carry
        rank_ref[:, at : at + width] = jnp.sum(hot * before, axis=0, keepdims=True)
        carry = before[:, width - 1 : width] + hot[:, width - 1 : width]
    owner_hot = hot_of(owner_ref[...], DEV).astype(BF16)
    tile = lax.broadcasted_iota(jnp.int32, (1, TILES), 1)
    index = mul(
        placings(rank_ref[...], (tile // 256).astype(F32), (tile % 256).astype(F32)), owner_hot, NT
    )
    index_ref[...] = (index[:CAP] * 256.0 + index[CAP:]).astype(jnp.int32)


def prep(owner):
    vmem = pl.BlockSpec(memory_space=pltpu.VMEM)
    return pl.pallas_call(
        prep_kernel,
        out_shape=(
            jax.ShapeDtypeStruct((CAP, DEV), jnp.int32),
            jax.ShapeDtypeStruct((1, TILES), F32),
        ),
        in_specs=[vmem],
        out_specs=(vmem, vmem),
        name="prep",
    )(owner)


def main_kernel(
    res_ref,
    dir_ref,
    noise_ref,
    owner_ref,
    block_ref,
    step_ref,
    obs_ref,
    rank_ref,
    index_ref,
    foot_hbm,
    cov_hbm,
    time_hbm,
    applied_ref,
    size_ref,
    ratio_ref,
    foot_ref,
    time_ref,
    meta_ref,
    wide,
    slots,
    values,
    cov,
    got,
    got_meta,
    places,
    hots,
    acc,
    flux,
    mixed,
    mix_a,
    mix_b,
    time_a,
    time_b,
    part_a,
    part_b,
    in_a,
    in_b,
    smooth,
    products,
    dots,
    dots_back,
    by_rank,
    sums,
    sums_in,
    ready,
    foot_sem,
    time_sem,
    cov_sem,
    tile_send,
    tile_recv,
    meta_send,
    meta_recv,
    z_send,
    z_recv,
    time_send,
    time_recv,
    ag_send,
    ag_recv,
    rs_send,
    rs_recv,
    back_send,
    back_recv,
    sum_send,
    sum_recv,
):
    cell, tm = lax.axis_index("cell"), lax.axis_index("tm")
    me = cell * 16 + tm
    z, core = cell // 2, cell % 2
    y, x = tm // 4, tm % 4
    xs = [(x + k) % 4 for k in range(4)]
    ys = [(y + k) % 4 for k in range(4)]
    far_first = sorted(
        ((dy, dx) for dy in range(4) for dx in range(4)),
        key=lambda at: -(min(at[0], 4 - at[0]) + min(at[1], 4 - at[1])),
    )
    planes = [ys[dy] * 4 + xs[dx] for dy, dx in far_first]

    def x_at(k):
        return xs[k]

    def y_at(k):
        return ys[k]

    def z_cell(k):
        return (z + k) % 4 * 2 + core

    def remote(src, dst, send, recv, to_cell, to_tm):
        return pltpu.make_async_remote_copy(
            src_ref=src,
            dst_ref=dst,
            send_sem=send,
            recv_sem=recv,
            device_id=(to_cell, to_tm),
            device_id_type=MESH,
        )

    def arrived(ref, sem):
        pltpu.make_async_copy(ref, ref, sem).wait()

    def away(k):
        return (cell + 4 + (k % 2 * 2 - 1) * ((k + 1) // 2)) % 8

    def to_others(send):
        def at_cell(k, _):
            to_cell = away(k)
            for to_tm in planes:
                send(to_cell, to_tm)
            return 0

        lax.fori_loop(0, 7, at_cell, 0)
        for to_tm in planes[:15]:
            send(cell, to_tm)

    barrier = pltpu.get_barrier_semaphore()
    columns = [(cell + k) % 8 for k in (4, 5, 3, 6, 2, 7, 1)]

    def signal(sem, to_cell, to_tm):
        pl.semaphore_signal(sem, inc=1, device_id=(to_cell, to_tm), device_id_type=MESH)

    for to_tm in planes[:15]:
        signal(barrier, cell, to_tm)
    for to_cell in columns:
        signal(barrier, to_cell, tm)
    foot_copy = pltpu.make_async_copy(foot_hbm, foot_ref, foot_sem)
    foot_copy.start()
    time_copy = pltpu.make_async_copy(time_hbm, time_ref, time_sem)
    time_copy.start()
    for k in range(8):
        rows = pl.ds(k * 144, 144)
        pltpu.make_async_copy(cov_hbm.at[rows], cov.at[rows], cov_sem).start()
    pl.semaphore_wait(barrier, 22)
    for to_cell in columns:
        signal(ready, to_cell, tm)

    owner_hot = hot_of(owner_ref[...], DEV).astype(BF16)
    obs_hot = hot_of(obs_ref[...], OBS).astype(BF16)
    dir_tile = mul(jnp.broadcast_to(dir_ref[...], (8, OBS)).astype(BF16), obs_hot)[0:1, :]
    fields = mul(
        owner_hot,
        placings(rank_ref[...], dir_tile, block_ref[...].astype(F32), step_ref[...].astype(F32)),
        NT,
    ).astype(BF16)
    lane_base = x * CAP
    lane = lax.broadcasted_iota(jnp.int32, (CAP, LANES), 1)

    def to_quarter(value, quarter):
        hot = jnp.where(sub_iota(CAP, LANES) + quarter * CAP == lane, 1.0, 0.0)
        return mul(value, hot.astype(BF16))

    meta_ref[:, 0, :] = (
        to_quarter(fields[:, :CAP], x)
        + to_quarter(fields[:, CAP : 2 * CAP], xs[2]) * 128.0
        + to_quarter(fields[:, 2 * CAP :], xs[2])
    )
    foot_copy.wait()
    wide[...] = foot_ref[...].astype(F32)
    pl.semaphore_wait(ready, 7)

    def send_tile(to_cell, to_tm):
        peer = to_cell * 16 + to_tm
        remote(
            values.at[peer], got.at[me], tile_send, tile_recv.at[cell], to_cell, to_tm
        ).start()
        remote(
            meta_ref.at[peer], got_meta.at[me], meta_send, meta_recv.at[cell], to_cell, to_tm
        ).start()

    def turn(k):
        q = k % 4
        return 2 * (q + q // 2 - 2 * (q // 3)) + k // 4

    natural = [ys[dy] * 4 + xs[dx] for dy in range(4) for dx in range(4)]

    def gather(to_cell, j):
        peer = to_cell * 16 + natural[j]
        for r in range(CAP):
            slots[j, r : r + 1, :] = wide[pl.ds(index_ref[r, peer], 1), :]
        values[peer] = slots[j].astype(BF16)

    for j in range(16):
        gather(cell, j)
        if j > 1:
            send_tile(cell, natural[j - 1])
    send_tile(cell, natural[15])

    def gather_and_send(k, _):
        to_cell = (cell + turn(k)) % 8
        for j in range(16):
            gather(to_cell, j)
            if j:
                send_tile(to_cell, natural[j - 1])
        send_tile(to_cell, natural[15])
        return 0

    lax.fori_loop(1, 8, gather_and_send, 0)
    pltpu.make_async_copy(values.at[me], got.at[me], tile_recv.at[cell]).start()
    pltpu.make_async_copy(meta_ref.at[me], got_meta.at[me], meta_recv.at[cell]).start()

    acc[...] = jnp.zeros_like(acc)
    row_of = sub_iota(LANES, LANES).astype(F32)

    quarter_of = lax.broadcasted_iota(jnp.int32, (1, LANES), 1) // CAP

    def load_meta(group):
        rows = got_meta[pl.ds(group * 16, 16)].reshape(4, 4, LANES)
        out = []
        for q in range(4):
            direction = place = jnp.zeros((1, LANES), F32)
            for j in range(4):
                row = rows[q, j : j + 1, :]
                direction = jnp.where(quarter_of == j, row, direction)
                place = jnp.where(quarter_of == (j + 2) % 4, row, place)
            place = jnp.concatenate([place[:, 64:], place[:, :64]], axis=1)
            block = jnp.floor(place * (1.0 / 128.0))
            out.append((direction, block, place - block * 128.0))
        return out

    def add_group(k, _):
        group = (cell + 8 - turn(k)) % 8
        arrived(got.at[pl.ds(group * 16, 16)], tile_recv.at[group])
        arrived(got_meta.at[pl.ds(group * 16, 16)], meta_recv.at[group])
        rows = load_meta(group)
        tiles = got[pl.ds(group * 16, 16)].reshape(512, LANES)
        for q, (direction, block, step) in enumerate(rows):
            places[group * 4 + q, 0:1, :] = block
            places[group * 4 + q, 1:2, :] = step
            hot = jnp.where(row_of == step, direction, 0.0).astype(BF16)
            for b in range(BLOCKS):
                hots[b * 128 : b * 128 + 128, q * 128 : q * 128 + 128] = hot * jnp.where(
                    block == b, 1.0, 0.0
                ).astype(BF16)
        acc[...] += mul(hots[...], tiles)
        return 0

    lax.fori_loop(0, 8, add_group, 0)
    for b in range(BLOCKS):
        flux[cell, :, b * 128 : b * 128 + 128] = acc[b * 128 : b * 128 + 128, :].astype(BF16)

    partner = z * 2 + 1 - core
    up, down, far = z_cell(1), z_cell(3), z_cell(2)
    full = pl.ds(0, ROWS)
    pieces = [pl.ds(0, 256), pl.ds(256, 256), pl.ds(512, 384), pl.ds(896, 256)]
    z_copies = []

    def z_go(block, cols, to_cell, at):
        ref = flux.at[block, :, cols]
        copy = remote(ref, ref, z_send.at[at], z_recv.at[at], to_cell, tm)
        copy.start()
        z_copies.append(copy)

    def z_wait(block, cols, at):
        arrived(flux.at[block, :, cols], z_recv.at[at])

    for i in range(4):
        z_go(cell, pieces[i], up, i)
        z_go(cell, pieces[3 - i], down, 7 - i)
    z_go(cell, full, partner, 12)

    time_copy.wait()
    time_sends = []
    for k in (1, 2, 3):
        peer = y_at(k)
        copy = remote(
            time_ref.at[:, pl.ds(pl.multiple_of(peer * 512, 512), 512)],
            time_a.at[y],
            time_send.at[k - 1],
            time_recv.at[k - 1],
            cell,
            peer * 4 + x,
        )
        copy.start()
        time_sends.append(copy)
        peer = x_at(k)
        for other in range(4):
            copy = remote(
                time_ref.at[:, pl.ds(pl.multiple_of((other * 4 + peer) * 128, 128), 128)],
                time_b.at[x, :, pl.ds(other * 128, 128)],
                time_send.at[3 * k + other + (k - 1)],
                time_recv.at[3 * k + other + (k - 1)],
                cell,
                y * 4 + peer,
            )
            copy.start()
            time_sends.append(copy)
    time_a[y] = time_ref[:, pl.ds(pl.multiple_of(y * 512, 512), 512)]
    for other in range(4):
        time_b[x, :, other * 128 : other * 128 + 128] = time_ref[
            :, pl.ds(pl.multiple_of((other * 4 + x) * 128, 128), 128)
        ]

    arrived(cov, cov_sem)

    def other_core(c):
        return c // 2 * 2 + 1 - c % 2

    def mix(block, piece=full, first=False):
        cols = pl.ds(pl.multiple_of(block * ROWS + piece.start, 128), piece.size)
        product = mul(cov[:, cols], flux[block, :, piece], NT)
        if first:
            mixed[...] = product
        else:
            mixed[...] += product

    mix(cell, first=True)
    for i in (0, 1):
        z_wait(down, pieces[i], i)
        z_go(down, pieces[i], up, 8 + i)
        z_go(down, pieces[i], partner, 13 + i)
        z_wait(up, pieces[3 - i], 7 - i)
        z_go(up, pieces[3 - i], down, 11 - i)
        z_go(up, pieces[3 - i], partner, 20 - i)
    z_wait(other_core(cell), full, 12)
    mix(other_core(cell))
    for i in (2, 3):
        z_wait(down, pieces[i], i)
        z_go(down, pieces[i], partner, 13 + i)
        z_wait(up, pieces[3 - i], 7 - i)
        z_go(up, pieces[3 - i], partner, 20 - i)
    mix(down)
    mix(up)
    for block, at in ((other_core(down), 13), (other_core(up), 17)):
        for i in range(4):
            z_wait(block, pieces[i], at + i)
        mix(block)
    for i in (0, 3, 1, 2):
        z_wait(far, pieces[i], 8 + i)
        z_go(far, pieces[i], partner, 21 + i)
        mix(far, pieces[i])
    for i in (0, 3, 1, 2):
        z_wait(other_core(far), pieces[i], 21 + i)
        mix(other_core(far), pieces[i])

    mix_a[:, pl.ds(pl.multiple_of(x * 128, 128), 128)] = mixed[:HALF, :].astype(BF16)
    mix_b[:, pl.ds(pl.multiple_of(y * 128, 128), 128)] = mixed[HALF:, :].astype(BF16)
    ag_copies = []

    def ag_go(buf, at_lane, rows, to_tm, at):
        ref = buf.at[rows, pl.ds(pl.multiple_of(at_lane * 128, 128), 128)]
        copy = remote(ref, ref, ag_send.at[at], ag_recv.at[at], cell, to_tm)
        copy.start()
        ag_copies.append(copy)

    def ag_wait(buf, at_lane, rows, at):
        arrived(buf.at[rows, pl.ds(pl.multiple_of(at_lane * 128, 128), 128)], ag_recv.at[at])

    first, second = pl.ds(0, QUARTER), pl.ds(QUARTER, QUARTER)
    x_up, x_down = y * 4 + x_at(1), y * 4 + x_at(3)
    y_up, y_down = y_at(1) * 4 + x, y_at(3) * 4 + x
    ag_go(mix_a, x, first, x_up, 0)
    ag_go(mix_a, x, second, x_down, 1)
    ag_go(mix_b, y, first, y_up, 2)
    ag_go(mix_b, y, second, y_down, 3)
    ag_go(mix_a, x, second, x_up, 4)
    ag_go(mix_a, x, first, x_down, 5)
    ag_go(mix_b, y, second, y_up, 6)
    ag_go(mix_b, y, first, y_down, 7)
    ag_wait(mix_a, x_at(3), first, 0)
    ag_go(mix_a, x_at(3), first, x_up, 8)
    ag_wait(mix_a, x_at(1), second, 1)
    ag_go(mix_a, x_at(1), second, x_down, 9)
    ag_wait(mix_b, y_at(3), first, 2)
    ag_go(mix_b, y_at(3), first, y_up, 10)
    ag_wait(mix_b, y_at(1), second, 3)
    ag_go(mix_b, y_at(1), second, y_down, 11)
    for k in (1, 2, 3):
        arrived(time_a.at[y_at(4 - k)], time_recv.at[k - 1])
        for other in range(4):
            arrived(
                time_b.at[x_at(4 - k), :, pl.ds(other * 128, 128)],
                time_recv.at[3 * k + other + (k - 1)],
            )
    ag_wait(mix_a, x_at(3), second, 4)
    ag_wait(mix_a, x_at(1), first, 5)
    ag_wait(mix_b, y_at(3), second, 6)
    ag_wait(mix_b, y_at(1), first, 7)
    ag_wait(mix_a, x_at(2), first, 8)
    ag_wait(mix_a, x_at(2), second, 9)
    rs_copies = []
    for k in (2, 1, 3):
        peer = y_at(k)
        part_a[k - 1] = mul(mix_a[...], time_a[peer], NT).astype(BF16)
        copy = remote(
            part_a.at[k - 1],
            in_a.at[k - 1],
            rs_send.at[k - 1],
            rs_recv.at[k - 1],
            cell,
            peer * 4 + x,
        )
        copy.start()
        rs_copies.append(copy)
        if k == 2:
            ag_wait(mix_b, y_at(2), first, 10)
            ag_wait(mix_b, y_at(2), second, 11)
        peer = x_at(k)
        part_b[k - 1] = mul(mix_b[...], time_b[peer], NT).astype(BF16)
        copy = remote(
            part_b.at[k - 1],
            in_b.at[k - 1],
            rs_send.at[k + 2],
            rs_recv.at[k + 2],
            cell,
            y * 4 + peer,
        )
        copy.start()
        rs_copies.append(copy)
    mixed[:HALF, :] = mul(mix_a[...], time_a[y], NT)
    mixed[HALF:, :] = mul(mix_b[...], time_b[x], NT)
    for k in (1, 3, 2):
        arrived(in_a.at[k - 1], rs_recv.at[k - 1])
        mixed[:HALF, :] += in_a[k - 1].astype(F32)
        arrived(in_b.at[k - 1], rs_recv.at[k + 2])
        mixed[HALF:, :] += in_b[k - 1].astype(F32)
    for b in range(BLOCKS):
        smooth[b * 128 : b * 128 + 128, :] = mixed[b * 128 : b * 128 + 128, :].T.astype(BF16)

    def dot_group(k):
        group = away(k)
        products[...] = mul(smooth[...], got[pl.ds(group * 16, 16)].reshape(512, LANES), NT)
        for q in range(4):
            block, step = places[group * 4 + q, 0:1, :], places[group * 4 + q, 1:2, :]
            cols = slice(q * 128, q * 128 + 128)
            picked = products[0:128, cols]
            for b in range(1, BLOCKS):
                picked = jnp.where(block == b, products[b * 128 : b * 128 + 128, cols], picked)
            picked = jnp.where(row_of == step, picked, 0.0)
            dots[group * 4 + q] = jnp.sum(picked, axis=0, keepdims=True)

    def send_dots(k, peers):
        group = away(k)
        for to_tm in peers:
            remote(
                dots.at[group * 4 + to_tm // 4], dots_back.at[me], back_send, back_recv, group, to_tm
            ).start()

    dot_group(0)

    def dots_and_send(k, _):
        send_dots(k - 1, planes)
        dot_group(k)
        return 0

    lax.fori_loop(1, 8, dots_and_send, 0)
    send_dots(7, planes[:15])
    dots_back[me] = dots[me // 4]
    owner_hot = hot_of(owner_ref[...], DEV).astype(BF16)
    obs_hot = hot_of(obs_ref[...], OBS).astype(BF16)
    in_slot = sub_iota(CAP, TILES).astype(F32) == rank_ref[...]
    arrived(dots_back.at[pl.ds(0, DEV - 1)], back_recv)
    by_rank[...] = dots_back[:, 0, :].T
    own = jnp.concatenate(split3(by_rank[pl.ds(pl.multiple_of(lane_base, CAP), CAP), :]), axis=0)
    parts = mul(own, owner_hot)
    tile_dots = jnp.sum(
        jnp.where(in_slot, parts[:CAP] + parts[CAP : 2 * CAP] + parts[2 * CAP :], 0.0),
        axis=0,
        keepdims=True,
    )
    high, middle, low = split3(tile_dots)
    three = jnp.concatenate(
        [high.astype(F32), middle.astype(F32), low.astype(F32), jnp.zeros((5, TILES), F32)], axis=0
    ).astype(BF16)
    direction, residual = dir_ref[...], res_ref[...]
    applied = jnp.sum(mul(three, obs_hot, NT), axis=0, keepdims=True)
    applied = applied + noise_ref[...] * direction

    lanes = lax.broadcasted_iota(jnp.int32, (1, LANES), 1)
    row = jnp.zeros((1, LANES), F32)
    for at, value in enumerate(
        (residual * residual, direction * applied, residual * applied, applied * applied)
    ):
        row = jnp.where(lanes == at, jnp.sum(value, axis=1, keepdims=True), row)
    sums[...] = row
    to_others(
        lambda to_cell, to_tm: remote(
            sums, sums_in.at[me], sum_send, sum_recv, to_cell, to_tm
        ).start()
    )
    sums_in[me] = row
    arrived(sums_in.at[pl.ds(0, DEV - 1)], sum_recv)
    total = jnp.sum(sums_in[...], axis=0)

    def total_of(at):
        return jnp.sum(jnp.where(lanes == at, total, 0.0), axis=1, keepdims=True)

    norm_now, curvature, cross_term, image_norm = (total_of(at) for at in range(4))
    step_size = norm_now / curvature
    norm_next = norm_now - 2.0 * step_size * cross_term + step_size * step_size * image_norm
    applied_ref[...] = applied
    size_ref[...] = jnp.broadcast_to(step_size, (1, OBS))
    ratio_ref[...] = jnp.broadcast_to(norm_next / norm_now, (1, OBS))

    arrived(values.at[pl.ds(0, DEV - 1)], tile_send)
    arrived(meta_ref.at[pl.ds(0, DEV - 1)], meta_send)
    for copy in time_sends + z_copies + ag_copies + rs_copies:
        copy.wait_send()
    arrived(dots_back.at[pl.ds(0, DEV - 1)], back_send)
    arrived(sums_in.at[pl.ds(0, DEV - 1)], sum_send)


def whole(*operands):
    vmem = pl.BlockSpec(memory_space=pltpu.VMEM)
    dma = pltpu.SemaphoreType.DMA
    row = jax.ShapeDtypeStruct((1, OBS), F32)
    return pl.pallas_call(
        main_kernel,
        out_shape=(row, row, row),
        in_specs=[vmem] * 8
        + [pl.BlockSpec(memory_space=pltpu.SMEM)]
        + [pl.BlockSpec(memory_space=pl.ANY)] * 3,
        out_specs=(vmem,) * 3,
        scratch_shapes=[
            pltpu.VMEM((TILES, LANES), BF16),
            pltpu.VMEM((LANES, 16 * LANES), BF16),
            pltpu.VMEM((DEV, 1, LANES), F32),
            pltpu.VMEM((TILES, LANES), F32),
            pltpu.VMEM((16, CAP, LANES), F32),
            pltpu.VMEM((DEV, CAP, LANES), BF16),
            pltpu.VMEM((ROWS, 8 * ROWS), BF16),
            pltpu.VMEM((DEV, CAP, LANES), BF16),
            pltpu.VMEM((DEV, 1, LANES), F32),
            pltpu.VMEM((DEV // 4, 2, LANES), F32),
            pltpu.VMEM((ROWS, 512), BF16),
            pltpu.VMEM((ROWS, LANES), F32),
            pltpu.VMEM((8, LANES, ROWS), BF16),
            pltpu.VMEM((ROWS, LANES), F32),
            pltpu.VMEM((HALF, 512), BF16),
            pltpu.VMEM((HALF, 512), BF16),
            pltpu.VMEM((4, LANES, 512), BF16),
            pltpu.VMEM((4, LANES, 512), BF16),
            pltpu.VMEM((3, HALF, LANES), BF16),
            pltpu.VMEM((3, HALF, LANES), BF16),
            pltpu.VMEM((3, HALF, LANES), BF16),
            pltpu.VMEM((3, HALF, LANES), BF16),
            pltpu.VMEM((ROWS, LANES), BF16),
            pltpu.VMEM((ROWS, 512), F32),
            pltpu.VMEM((DEV // 4, 1, LANES), F32),
            pltpu.VMEM((DEV, 1, LANES), F32),
            pltpu.VMEM((LANES, DEV), F32),
            pltpu.VMEM((1, LANES), F32),
            pltpu.VMEM((DEV, 1, LANES), F32),
            pltpu.SemaphoreType.REGULAR,
            dma,
            dma,
            dma,
            dma,
            dma((8,)),
            dma,
            dma((8,)),
            dma((25,)),
            dma((25,)),
            dma((15,)),
            dma((15,)),
            dma((12,)),
            dma((12,)),
            dma((6,)),
            dma((6,)),
            dma,
            dma,
            dma,
            dma,
        ],
        compiler_params=pltpu.CompilerParams(
            collective_id=0, has_side_effects=True, vmem_limit_bytes=60 * 2**20
        ),
        name="whole",
    )(*operands)


def local(
    solution,
    residual,
    direction,
    noise_var,
    footprints,
    tile_owner,
    tile_block,
    tile_step,
    tile_obs,
    cell_cov,
    time_cov,
):
    row = functools.partial(jnp.reshape, shape=(1, OBS))
    tile_row = functools.partial(jnp.reshape, shape=(1, TILES))
    owner = tile_row(tile_owner)
    index, rank = prep(owner)
    outs = whole(
        row(residual),
        row(direction),
        row(noise_var),
        owner,
        tile_row(tile_block),
        tile_row(tile_step),
        tile_row(tile_obs),
        rank,
        index,
        footprints,
        cell_cov,
        time_cov,
    )
    applied, step_size, ratio = (out.reshape(OBS) for out in outs)
    new_residual = residual - step_size * applied
    return solution + step_size * direction, new_residual, new_residual + ratio * direction


def solution(mesh):
    both = P(CELL_TM)
    in_specs = (both,) * 4 + (P(CELL_TM, None),) * 2 + (both,) * 3
    in_specs += (P("cell", None), P("tm", None))
    return jax.shard_map(
        local, mesh=mesh, in_specs=in_specs, out_specs=(both,) * 3, check_vma=False
    )
```

```python
import functools

import jax
import jax.numpy as jnp
from jax import lax
from jax.experimental import pallas as pl
from jax.experimental.pallas import tpu as pltpu
from jax.sharding import PartitionSpec as P

MESH = pl.DeviceIdType.MESH
CELL_TM = ("cell", "tm")
NN = (((1,), (0,)), ((), ()))
NT = (((1,), (1,)), ((), ()))
DEV = 128
CAP = 32
LANES = 128
OBS = 256
TILES = 2048
SLOTS = DEV * CAP
ROWS = 1152
BLOCKS = 9
HALF = ROWS // 2
QUARTER = ROWS // 4
BF16 = jnp.bfloat16
F32 = jnp.float32


def mul(a, b, dims=NN):
    return lax.dot_general(a, b, dims, preferred_element_type=F32)


def sub_iota(rows, cols):
    return lax.broadcasted_iota(jnp.int32, (rows, cols), 0)


def hot_of(index, rows):
    return jnp.where(sub_iota(rows, index.shape[1]) == index, 1.0, 0.0)


def split3(value):
    high = value.astype(BF16)
    rest = value - high.astype(F32)
    middle = rest.astype(BF16)
    return high, middle, (rest - middle.astype(F32)).astype(BF16)


def placings(rank, *rows):
    in_slot = sub_iota(CAP, TILES).astype(F32) == rank
    return jnp.concatenate([jnp.where(in_slot, row, 0.0).astype(BF16) for row in rows], axis=0)


def prep_kernel(owner_ref, index_ref, rank_ref):
    width = 256
    above = jnp.where(
        sub_iota(width, width) < lax.broadcasted_iota(jnp.int32, (width, width), 1), 1.0, 0.0
    ).astype(BF16)
    carry = jnp.zeros((DEV, 1), F32)
    for at in range(0, TILES, width):
        hot = hot_of(owner_ref[:, at : at + width], DEV)
        before = mul(hot.astype(BF16), above) + carry
        rank_ref[:, at : at + width] = jnp.sum(hot * before, axis=0, keepdims=True)
        carry = before[:, width - 1 : width] + hot[:, width - 1 : width]
    owner_hot = hot_of(owner_ref[...], DEV).astype(BF16)
    tile = lax.broadcasted_iota(jnp.int32, (1, TILES), 1)
    index = mul(
        placings(rank_ref[...], (tile // 256).astype(F32), (tile % 256).astype(F32)), owner_hot, NT
    )
    index_ref[...] = (index[:CAP] * 256.0 + index[CAP:]).astype(jnp.int32)


def prep(owner):
    vmem = pl.BlockSpec(memory_space=pltpu.VMEM)
    return pl.pallas_call(
        prep_kernel,
        out_shape=(
            jax.ShapeDtypeStruct((CAP, DEV), jnp.int32),
            jax.ShapeDtypeStruct((1, TILES), F32),
        ),
        in_specs=[vmem],
        out_specs=(vmem, vmem),
        name="prep",
    )(owner)


def main_kernel(
    res_ref,
    dir_ref,
    noise_ref,
    owner_ref,
    block_ref,
    step_ref,
    obs_ref,
    rank_ref,
    index_ref,
    foot_hbm,
    cov_hbm,
    time_hbm,
    applied_ref,
    size_ref,
    ratio_ref,
    foot_ref,
    time_ref,
    meta_ref,
    wide,
    slots,
    values,
    cov,
    got,
    got_meta,
    places,
    hots,
    acc,
    flux,
    mixed,
    mix_a,
    mix_b,
    time_a,
    time_b,
    part_a,
    part_b,
    in_a,
    in_b,
    smooth,
    products,
    dots,
    dots_back,
    by_rank,
    sums,
    sums_in,
    foot_sem,
    time_sem,
    cov_sem,
    tile_send,
    tile_recv,
    meta_send,
    meta_recv,
    z_send,
    z_recv,
    time_send,
    time_recv,
    ag_send,
    ag_recv,
    rs_send,
    rs_recv,
    back_send,
    back_recv,
    sum_send,
    sum_recv,
):
    cell, tm = lax.axis_index("cell"), lax.axis_index("tm")
    me = cell * 16 + tm
    z, core = cell // 2, cell % 2
    y, x = tm // 4, tm % 4
    xs = [(x + k) % 4 for k in range(4)]
    ys = [(y + k) % 4 for k in range(4)]
    far_first = sorted(
        ((dy, dx) for dy in range(4) for dx in range(4)),
        key=lambda at: -(min(at[0], 4 - at[0]) + min(at[1], 4 - at[1])),
    )
    planes = [ys[dy] * 4 + xs[dx] for dy, dx in far_first]

    def x_at(k):
        return xs[k]

    def y_at(k):
        return ys[k]

    def z_cell(k):
        return (z + k) % 4 * 2 + core

    def remote(src, dst, send, recv, to_cell, to_tm):
        return pltpu.make_async_remote_copy(
            src_ref=src,
            dst_ref=dst,
            send_sem=send,
            recv_sem=recv,
            device_id=(to_cell, to_tm),
            device_id_type=MESH,
        )

    def arrived(ref, sem):
        pltpu.make_async_copy(ref, ref, sem).wait()

    def away(k):
        return (cell + 4 + (k % 2 * 2 - 1) * ((k + 1) // 2)) % 8

    def to_others(send):
        def at_cell(k, _):
            to_cell = away(k)
            for to_tm in planes:
                send(to_cell, to_tm)
            return 0

        lax.fori_loop(0, 7, at_cell, 0)
        for to_tm in planes[:15]:
            send(cell, to_tm)

    barrier = pltpu.get_barrier_semaphore()

    def signal(sem, to_cell, to_tm):
        pl.semaphore_signal(sem, inc=1, device_id=(to_cell, to_tm), device_id_type=MESH)

    to_others(lambda to_cell, to_tm: signal(barrier, to_cell, to_tm))
    foot_copy = pltpu.make_async_copy(foot_hbm, foot_ref, foot_sem)
    foot_copy.start()
    time_copy = pltpu.make_async_copy(time_hbm, time_ref, time_sem)
    time_copy.start()
    for k in range(8):
        rows = pl.ds(k * 144, 144)
        pltpu.make_async_copy(cov_hbm.at[rows], cov.at[rows], cov_sem).start()

    owner_hot = hot_of(owner_ref[...], DEV).astype(BF16)
    obs_hot = hot_of(obs_ref[...], OBS).astype(BF16)
    dir_tile = mul(jnp.broadcast_to(dir_ref[...], (8, OBS)).astype(BF16), obs_hot)[0:1, :]
    fields = mul(
        owner_hot,
        placings(rank_ref[...], dir_tile, block_ref[...].astype(F32), step_ref[...].astype(F32)),
        NT,
    ).astype(BF16)
    lane_base = x * CAP
    lane = lax.broadcasted_iota(jnp.int32, (CAP, LANES), 1)

    def to_quarter(value, quarter):
        hot = jnp.where(sub_iota(CAP, LANES) + quarter * CAP == lane, 1.0, 0.0)
        return mul(value, hot.astype(BF16))

    meta_ref[:, 0, :] = (
        to_quarter(fields[:, :CAP], x)
        + to_quarter(fields[:, CAP : 2 * CAP], xs[2]) * 128.0
        + to_quarter(fields[:, 2 * CAP :], xs[2])
    )
    foot_copy.wait()
    wide[...] = foot_ref[...].astype(F32)
    pl.semaphore_wait(barrier, DEV - 1)

    def send_tile(to_cell, to_tm):
        peer = to_cell * 16 + to_tm
        remote(
            values.at[peer], got.at[me], tile_send, tile_recv.at[cell], to_cell, to_tm
        ).start()
        remote(
            meta_ref.at[peer], got_meta.at[me], meta_send, meta_recv.at[cell], to_cell, to_tm
        ).start()

    def turn(k):
        q = k % 4
        return 2 * (q + q // 2 - 2 * (q // 3)) + k // 4

    natural = [ys[dy] * 4 + xs[dx] for dy in range(4) for dx in range(4)]

    def gather(to_cell, j):
        peer = to_cell * 16 + natural[j]
        for r in range(CAP):
            slots[j, r : r + 1, :] = wide[pl.ds(index_ref[r, peer], 1), :]
        values[peer] = slots[j].astype(BF16)

    for j in range(16):
        gather(cell, j)
        if j > 1:
            send_tile(cell, natural[j - 1])
    send_tile(cell, natural[15])

    def gather_and_send(k, _):
        to_cell = (cell + turn(k)) % 8
        for j in range(16):
            gather(to_cell, j)
            if j:
                send_tile(to_cell, natural[j - 1])
        send_tile(to_cell, natural[15])
        return 0

    lax.fori_loop(1, 8, gather_and_send, 0)
    pltpu.make_async_copy(values.at[me], got.at[me], tile_recv.at[cell]).start()
    pltpu.make_async_copy(meta_ref.at[me], got_meta.at[me], meta_recv.at[cell]).start()

    acc[...] = jnp.zeros_like(acc)
    row_of = sub_iota(LANES, LANES).astype(F32)

    quarter_of = lax.broadcasted_iota(jnp.int32, (1, LANES), 1) // CAP

    def load_meta(group):
        rows = got_meta[pl.ds(group * 16, 16)].reshape(4, 4, LANES)
        out = []
        for q in range(4):
            direction = place = jnp.zeros((1, LANES), F32)
            for j in range(4):
                row = rows[q, j : j + 1, :]
                direction = jnp.where(quarter_of == j, row, direction)
                place = jnp.where(quarter_of == (j + 2) % 4, row, place)
            place = jnp.concatenate([place[:, 64:], place[:, :64]], axis=1)
            block = jnp.floor(place * (1.0 / 128.0))
            out.append((direction, block, place - block * 128.0))
        return out

    def add_group(k, _):
        group = (cell + 8 - turn(k)) % 8
        arrived(got.at[pl.ds(group * 16, 16)], tile_recv.at[group])
        arrived(got_meta.at[pl.ds(group * 16, 16)], meta_recv.at[group])
        rows = load_meta(group)
        tiles = got[pl.ds(group * 16, 16)].reshape(512, LANES)
        for q, (direction, block, step) in enumerate(rows):
            places[group * 4 + q, 0:1, :] = block
            places[group * 4 + q, 1:2, :] = step
            hot = jnp.where(row_of == step, direction, 0.0).astype(BF16)
            for b in range(BLOCKS):
                hots[b * 128 : b * 128 + 128, q * 128 : q * 128 + 128] = hot * jnp.where(
                    block == b, 1.0, 0.0
                ).astype(BF16)
        acc[...] += mul(hots[...], tiles)
        return 0

    lax.fori_loop(0, 8, add_group, 0)
    for b in range(BLOCKS):
        flux[cell, :, b * 128 : b * 128 + 128] = acc[b * 128 : b * 128 + 128, :].astype(BF16)

    partner = z * 2 + 1 - core
    up, down, far = z_cell(1), z_cell(3), z_cell(2)
    left, right, full = pl.ds(0, 512), pl.ds(512, ROWS - 512), pl.ds(0, ROWS)
    z_copies = []

    def z_go(block, cols, to_cell, at):
        ref = flux.at[block, :, cols]
        copy = remote(ref, ref, z_send.at[at], z_recv.at[at], to_cell, tm)
        copy.start()
        z_copies.append(copy)

    def z_wait(block, cols, at):
        arrived(flux.at[block, :, cols], z_recv.at[at])

    z_go(cell, left, up, 0)
    z_go(cell, right, down, 2)
    z_go(cell, right, up, 1)
    z_go(cell, left, down, 3)
    z_go(cell, full, partner, 4)

    time_copy.wait()
    time_sends = []
    for k in (1, 2, 3):
        peer = y_at(k)
        copy = remote(
            time_ref.at[:, pl.ds(pl.multiple_of(peer * 512, 512), 512)],
            time_a.at[y],
            time_send.at[k - 1],
            time_recv.at[k - 1],
            cell,
            peer * 4 + x,
        )
        copy.start()
        time_sends.append(copy)
        peer = x_at(k)
        for other in range(4):
            copy = remote(
                time_ref.at[:, pl.ds(pl.multiple_of((other * 4 + peer) * 128, 128), 128)],
                time_b.at[x, :, pl.ds(other * 128, 128)],
                time_send.at[3 * k + other + (k - 1)],
                time_recv.at[3 * k + other + (k - 1)],
                cell,
                y * 4 + peer,
            )
            copy.start()
            time_sends.append(copy)
    time_a[y] = time_ref[:, pl.ds(pl.multiple_of(y * 512, 512), 512)]
    for other in range(4):
        time_b[x, :, other * 128 : other * 128 + 128] = time_ref[
            :, pl.ds(pl.multiple_of((other * 4 + x) * 128, 128), 128)
        ]

    arrived(cov, cov_sem)

    def other_core(c):
        return c // 2 * 2 + 1 - c % 2

    def mix(block, first=False):
        cols = pl.ds(pl.multiple_of(block * ROWS, 128), ROWS)
        product = mul(cov[:, cols], flux[block], NT)
        if first:
            mixed[...] = product
        else:
            mixed[...] += product

    mix(cell, True)
    z_wait(down, left, 0)
    z_go(down, left, up, 5)
    z_go(down, left, partner, 7)
    z_wait(up, right, 2)
    z_go(up, right, down, 6)
    z_go(up, right, partner, 8)
    z_wait(other_core(cell), full, 4)
    mix(other_core(cell))
    z_wait(down, right, 1)
    z_go(down, right, partner, 9)
    z_wait(up, left, 3)
    z_go(up, left, partner, 10)
    mix(down)
    mix(up)
    z_wait(other_core(down), left, 7)
    z_wait(other_core(down), right, 9)
    mix(other_core(down))
    z_wait(other_core(up), right, 8)
    z_wait(other_core(up), left, 10)
    mix(other_core(up))
    z_wait(far, left, 5)
    z_go(far, left, partner, 11)
    z_wait(far, right, 6)
    z_go(far, right, partner, 12)
    mix(far)
    z_wait(other_core(far), left, 11)
    z_wait(other_core(far), right, 12)
    mix(other_core(far))

    mix_a[:, pl.ds(pl.multiple_of(x * 128, 128), 128)] = mixed[:HALF, :].astype(BF16)
    mix_b[:, pl.ds(pl.multiple_of(y * 128, 128), 128)] = mixed[HALF:, :].astype(BF16)
    ag_copies = []

    def ag_go(buf, at_lane, rows, to_tm, at):
        ref = buf.at[rows, pl.ds(pl.multiple_of(at_lane * 128, 128), 128)]
        copy = remote(ref, ref, ag_send.at[at], ag_recv.at[at], cell, to_tm)
        copy.start()
        ag_copies.append(copy)

    def ag_wait(buf, at_lane, rows, at):
        arrived(buf.at[rows, pl.ds(pl.multiple_of(at_lane * 128, 128), 128)], ag_recv.at[at])

    first, second = pl.ds(0, QUARTER), pl.ds(QUARTER, QUARTER)
    x_up, x_down = y * 4 + x_at(1), y * 4 + x_at(3)
    y_up, y_down = y_at(1) * 4 + x, y_at(3) * 4 + x
    ag_go(mix_a, x, first, x_up, 0)
    ag_go(mix_a, x, second, x_down, 1)
    ag_go(mix_b, y, first, y_up, 2)
    ag_go(mix_b, y, second, y_down, 3)
    ag_go(mix_a, x, second, x_up, 4)
    ag_go(mix_a, x, first, x_down, 5)
    ag_go(mix_b, y, second, y_up, 6)
    ag_go(mix_b, y, first, y_down, 7)
    ag_wait(mix_a, x_at(3), first, 0)
    ag_go(mix_a, x_at(3), first, x_up, 8)
    ag_wait(mix_a, x_at(1), second, 1)
    ag_go(mix_a, x_at(1), second, x_down, 9)
    ag_wait(mix_b, y_at(3), first, 2)
    ag_go(mix_b, y_at(3), first, y_up, 10)
    ag_wait(mix_b, y_at(1), second, 3)
    ag_go(mix_b, y_at(1), second, y_down, 11)
    for k in (1, 2, 3):
        arrived(time_a.at[y_at(4 - k)], time_recv.at[k - 1])
        for other in range(4):
            arrived(
                time_b.at[x_at(4 - k), :, pl.ds(other * 128, 128)],
                time_recv.at[3 * k + other + (k - 1)],
            )
    ag_wait(mix_a, x_at(3), second, 4)
    ag_wait(mix_a, x_at(1), first, 5)
    ag_wait(mix_b, y_at(3), second, 6)
    ag_wait(mix_b, y_at(1), first, 7)
    ag_wait(mix_a, x_at(2), first, 8)
    ag_wait(mix_a, x_at(2), second, 9)
    rs_copies = []
    for k in (2, 1, 3):
        peer = y_at(k)
        part_a[k - 1] = mul(mix_a[...], time_a[peer], NT).astype(BF16)
        copy = remote(
            part_a.at[k - 1],
            in_a.at[k - 1],
            rs_send.at[k - 1],
            rs_recv.at[k - 1],
            cell,
            peer * 4 + x,
        )
        copy.start()
        rs_copies.append(copy)
        if k == 2:
            ag_wait(mix_b, y_at(2), first, 10)
            ag_wait(mix_b, y_at(2), second, 11)
        peer = x_at(k)
        part_b[k - 1] = mul(mix_b[...], time_b[peer], NT).astype(BF16)
        copy = remote(
            part_b.at[k - 1],
            in_b.at[k - 1],
            rs_send.at[k + 2],
            rs_recv.at[k + 2],
            cell,
            y * 4 + peer,
        )
        copy.start()
        rs_copies.append(copy)
    mixed[:HALF, :] = mul(mix_a[...], time_a[y], NT)
    mixed[HALF:, :] = mul(mix_b[...], time_b[x], NT)
    for k in (1, 3, 2):
        arrived(in_a.at[k - 1], rs_recv.at[k - 1])
        mixed[:HALF, :] += in_a[k - 1].astype(F32)
        arrived(in_b.at[k - 1], rs_recv.at[k + 2])
        mixed[HALF:, :] += in_b[k - 1].astype(F32)
    for b in range(BLOCKS):
        smooth[b * 128 : b * 128 + 128, :] = mixed[b * 128 : b * 128 + 128, :].T.astype(BF16)

    def dot_group(k):
        group = away(k)
        products[...] = mul(smooth[...], got[pl.ds(group * 16, 16)].reshape(512, LANES), NT)
        for q in range(4):
            block, step = places[group * 4 + q, 0:1, :], places[group * 4 + q, 1:2, :]
            cols = slice(q * 128, q * 128 + 128)
            picked = products[0:128, cols]
            for b in range(1, BLOCKS):
                picked = jnp.where(block == b, products[b * 128 : b * 128 + 128, cols], picked)
            picked = jnp.where(row_of == step, picked, 0.0)
            dots[group * 4 + q] = jnp.sum(picked, axis=0, keepdims=True)

    def send_dots(k, peers):
        group = away(k)
        for to_tm in peers:
            remote(
                dots.at[group * 4 + to_tm // 4], dots_back.at[me], back_send, back_recv, group, to_tm
            ).start()

    dot_group(0)

    def dots_and_send(k, _):
        send_dots(k - 1, planes)
        dot_group(k)
        return 0

    lax.fori_loop(1, 8, dots_and_send, 0)
    send_dots(7, planes[:15])
    dots_back[me] = dots[me // 4]
    owner_hot = hot_of(owner_ref[...], DEV).astype(BF16)
    obs_hot = hot_of(obs_ref[...], OBS).astype(BF16)
    in_slot = sub_iota(CAP, TILES).astype(F32) == rank_ref[...]
    arrived(dots_back.at[pl.ds(0, DEV - 1)], back_recv)
    by_rank[...] = dots_back[:, 0, :].T
    own = jnp.concatenate(split3(by_rank[pl.ds(pl.multiple_of(lane_base, CAP), CAP), :]), axis=0)
    parts = mul(own, owner_hot)
    tile_dots = jnp.sum(
        jnp.where(in_slot, parts[:CAP] + parts[CAP : 2 * CAP] + parts[2 * CAP :], 0.0),
        axis=0,
        keepdims=True,
    )
    high, middle, low = split3(tile_dots)
    three = jnp.concatenate(
        [high.astype(F32), middle.astype(F32), low.astype(F32), jnp.zeros((5, TILES), F32)], axis=0
    ).astype(BF16)
    direction, residual = dir_ref[...], res_ref[...]
    applied = jnp.sum(mul(three, obs_hot, NT), axis=0, keepdims=True)
    applied = applied + noise_ref[...] * direction

    lanes = lax.broadcasted_iota(jnp.int32, (1, LANES), 1)
    row = jnp.zeros((1, LANES), F32)
    for at, value in enumerate(
        (residual * residual, direction * applied, residual * applied, applied * applied)
    ):
        row = jnp.where(lanes == at, jnp.sum(value, axis=1, keepdims=True), row)
    sums[...] = row
    to_others(
        lambda to_cell, to_tm: remote(
            sums, sums_in.at[me], sum_send, sum_recv, to_cell, to_tm
        ).start()
    )
    sums_in[me] = row
    arrived(sums_in.at[pl.ds(0, DEV - 1)], sum_recv)
    total = jnp.sum(sums_in[...], axis=0)

    def total_of(at):
        return jnp.sum(jnp.where(lanes == at, total, 0.0), axis=1, keepdims=True)

    norm_now, curvature, cross_term, image_norm = (total_of(at) for at in range(4))
    step_size = norm_now / curvature
    norm_next = norm_now - 2.0 * step_size * cross_term + step_size * step_size * image_norm
    applied_ref[...] = applied
    size_ref[...] = jnp.broadcast_to(step_size, (1, OBS))
    ratio_ref[...] = jnp.broadcast_to(norm_next / norm_now, (1, OBS))

    arrived(values.at[pl.ds(0, DEV - 1)], tile_send)
    arrived(meta_ref.at[pl.ds(0, DEV - 1)], meta_send)
    for copy in time_sends + z_copies + ag_copies + rs_copies:
        copy.wait_send()
    arrived(dots_back.at[pl.ds(0, DEV - 1)], back_send)
    arrived(sums_in.at[pl.ds(0, DEV - 1)], sum_send)


def whole(*operands):
    vmem = pl.BlockSpec(memory_space=pltpu.VMEM)
    dma = pltpu.SemaphoreType.DMA
    row = jax.ShapeDtypeStruct((1, OBS), F32)
    return pl.pallas_call(
        main_kernel,
        out_shape=(row, row, row),
        in_specs=[vmem] * 8
        + [pl.BlockSpec(memory_space=pltpu.SMEM)]
        + [pl.BlockSpec(memory_space=pl.ANY)] * 3,
        out_specs=(vmem,) * 3,
        scratch_shapes=[
            pltpu.VMEM((TILES, LANES), BF16),
            pltpu.VMEM((LANES, 16 * LANES), BF16),
            pltpu.VMEM((DEV, 1, LANES), F32),
            pltpu.VMEM((TILES, LANES), F32),
            pltpu.VMEM((16, CAP, LANES), F32),
            pltpu.VMEM((DEV, CAP, LANES), BF16),
            pltpu.VMEM((ROWS, 8 * ROWS), BF16),
            pltpu.VMEM((DEV, CAP, LANES), BF16),
            pltpu.VMEM((DEV, 1, LANES), F32),
            pltpu.VMEM((DEV // 4, 2, LANES), F32),
            pltpu.VMEM((ROWS, 512), BF16),
            pltpu.VMEM((ROWS, LANES), F32),
            pltpu.VMEM((8, LANES, ROWS), BF16),
            pltpu.VMEM((ROWS, LANES), F32),
            pltpu.VMEM((HALF, 512), BF16),
            pltpu.VMEM((HALF, 512), BF16),
            pltpu.VMEM((4, LANES, 512), BF16),
            pltpu.VMEM((4, LANES, 512), BF16),
            pltpu.VMEM((3, HALF, LANES), BF16),
            pltpu.VMEM((3, HALF, LANES), BF16),
            pltpu.VMEM((3, HALF, LANES), BF16),
            pltpu.VMEM((3, HALF, LANES), BF16),
            pltpu.VMEM((ROWS, LANES), BF16),
            pltpu.VMEM((ROWS, 512), F32),
            pltpu.VMEM((DEV // 4, 1, LANES), F32),
            pltpu.VMEM((DEV, 1, LANES), F32),
            pltpu.VMEM((LANES, DEV), F32),
            pltpu.VMEM((1, LANES), F32),
            pltpu.VMEM((DEV, 1, LANES), F32),
            dma,
            dma,
            dma,
            dma,
            dma((8,)),
            dma,
            dma((8,)),
            dma((13,)),
            dma((13,)),
            dma((15,)),
            dma((15,)),
            dma((12,)),
            dma((12,)),
            dma((6,)),
            dma((6,)),
            dma,
            dma,
            dma,
            dma,
        ],
        compiler_params=pltpu.CompilerParams(
            collective_id=0, has_side_effects=True, vmem_limit_bytes=60 * 2**20
        ),
        name="whole",
    )(*operands)


def local(
    solution,
    residual,
    direction,
    noise_var,
    footprints,
    tile_owner,
    tile_block,
    tile_step,
    tile_obs,
    cell_cov,
    time_cov,
):
    row = functools.partial(jnp.reshape, shape=(1, OBS))
    tile_row = functools.partial(jnp.reshape, shape=(1, TILES))
    owner = tile_row(tile_owner)
    index, rank = prep(owner)
    outs = whole(
        row(residual),
        row(direction),
        row(noise_var),
        owner,
        tile_row(tile_block),
        tile_row(tile_step),
        tile_row(tile_obs),
        rank,
        index,
        footprints,
        cell_cov,
        time_cov,
    )
    applied, step_size, ratio = (out.reshape(OBS) for out in outs)
    new_residual = residual - step_size * applied
    return solution + step_size * direction, new_residual, new_residual + ratio * direction


def solution(mesh):
    both = P(CELL_TM)
    in_specs = (both,) * 4 + (P(CELL_TM, None),) * 2 + (both,) * 3
    in_specs += (P("cell", None), P("tm", None))
    return jax.shard_map(
        local, mesh=mesh, in_specs=in_specs, out_specs=(both,) * 3, check_vma=False
    )
```

```python
import functools

import jax
import jax.numpy as jnp
from jax import lax
from jax.experimental import pallas as pl
from jax.experimental.pallas import tpu as pltpu
from jax.sharding import PartitionSpec as P

MESH = pl.DeviceIdType.MESH
CELL_TM = ("cell", "tm")
NN = (((1,), (0,)), ((), ()))
NT = (((1,), (1,)), ((), ()))
DEV = 128
CAP = 32
LANES = 128
OBS = 256
TILES = 2048
SLOTS = DEV * CAP
ROWS = 1152
BLOCKS = 9
HALF = ROWS // 2
QUARTER = ROWS // 4
BF16 = jnp.bfloat16
F32 = jnp.float32


def mul(a, b, dims=NN):
    return lax.dot_general(a, b, dims, preferred_element_type=F32)


def sub_iota(rows, cols):
    return lax.broadcasted_iota(jnp.int32, (rows, cols), 0)


def hot_of(index, rows):
    return jnp.where(sub_iota(rows, index.shape[1]) == index, 1.0, 0.0)


def split3(value):
    high = value.astype(BF16)
    rest = value - high.astype(F32)
    middle = rest.astype(BF16)
    return high, middle, (rest - middle.astype(F32)).astype(BF16)


def placings(rank, *rows):
    in_slot = sub_iota(CAP, TILES).astype(F32) == rank
    return jnp.concatenate([jnp.where(in_slot, row, 0.0).astype(BF16) for row in rows], axis=0)


def prep_kernel(owner_ref, index_ref, rank_ref):
    width = 256
    above = jnp.where(
        sub_iota(width, width) < lax.broadcasted_iota(jnp.int32, (width, width), 1), 1.0, 0.0
    ).astype(BF16)
    carry = jnp.zeros((DEV, 1), F32)
    for at in range(0, TILES, width):
        hot = hot_of(owner_ref[:, at : at + width], DEV)
        before = mul(hot.astype(BF16), above) + carry
        rank_ref[:, at : at + width] = jnp.sum(hot * before, axis=0, keepdims=True)
        carry = before[:, width - 1 : width] + hot[:, width - 1 : width]
    owner_hot = hot_of(owner_ref[...], DEV).astype(BF16)
    tile = lax.broadcasted_iota(jnp.int32, (1, TILES), 1)
    index = mul(
        placings(rank_ref[...], (tile // 256).astype(F32), (tile % 256).astype(F32)), owner_hot, NT
    )
    index_ref[...] = (index[:CAP] * 256.0 + index[CAP:]).astype(jnp.int32)


def prep(owner):
    vmem = pl.BlockSpec(memory_space=pltpu.VMEM)
    return pl.pallas_call(
        prep_kernel,
        out_shape=(
            jax.ShapeDtypeStruct((CAP, DEV), jnp.int32),
            jax.ShapeDtypeStruct((1, TILES), F32),
        ),
        in_specs=[vmem],
        out_specs=(vmem, vmem),
        name="prep",
    )(owner)


def main_kernel(
    res_ref,
    dir_ref,
    noise_ref,
    owner_ref,
    block_ref,
    step_ref,
    obs_ref,
    rank_ref,
    index_ref,
    foot_hbm,
    cov_hbm,
    time_hbm,
    applied_ref,
    size_ref,
    ratio_ref,
    foot_ref,
    time_ref,
    meta_ref,
    wide,
    slots,
    values,
    cov,
    got,
    got_meta,
    places,
    hots,
    acc,
    flux,
    mixed,
    mix_a,
    mix_b,
    time_a,
    time_b,
    part_a,
    part_b,
    in_a,
    in_b,
    smooth,
    products,
    dots,
    dots_back,
    by_rank,
    sums,
    sums_in,
    foot_sem,
    time_sem,
    cov_sem,
    tile_send,
    tile_recv,
    meta_send,
    meta_recv,
    z_send,
    z_recv,
    time_send,
    time_recv,
    ag_send,
    ag_recv,
    rs_send,
    rs_recv,
    back_send,
    back_recv,
    sum_send,
    sum_recv,
):
    cell, tm = lax.axis_index("cell"), lax.axis_index("tm")
    me = cell * 16 + tm
    z, core = cell // 2, cell % 2
    y, x = tm // 4, tm % 4
    xs = [(x + k) % 4 for k in range(4)]
    ys = [(y + k) % 4 for k in range(4)]
    far_first = sorted(
        ((dy, dx) for dy in range(4) for dx in range(4)),
        key=lambda at: -(min(at[0], 4 - at[0]) + min(at[1], 4 - at[1])),
    )
    planes = [ys[dy] * 4 + xs[dx] for dy, dx in far_first]

    def x_at(k):
        return xs[k]

    def y_at(k):
        return ys[k]

    def z_cell(k):
        return (z + k) % 4 * 2 + core

    def remote(src, dst, send, recv, to_cell, to_tm):
        return pltpu.make_async_remote_copy(
            src_ref=src,
            dst_ref=dst,
            send_sem=send,
            recv_sem=recv,
            device_id=(to_cell, to_tm),
            device_id_type=MESH,
        )

    def arrived(ref, sem):
        pltpu.make_async_copy(ref, ref, sem).wait()

    def away(k):
        return (cell + 4 + (k % 2 * 2 - 1) * ((k + 1) // 2)) % 8

    def to_others(send):
        for k in range(7):
            to_cell = away(k)
            for to_tm in planes:
                send(to_cell, to_tm)
        for to_tm in planes[:15]:
            send(cell, to_tm)

    barrier = pltpu.get_barrier_semaphore()

    def signal(sem, to_cell, to_tm):
        pl.semaphore_signal(sem, inc=1, device_id=(to_cell, to_tm), device_id_type=MESH)

    to_others(lambda to_cell, to_tm: signal(barrier, to_cell, to_tm))
    foot_copy = pltpu.make_async_copy(foot_hbm, foot_ref, foot_sem)
    foot_copy.start()
    time_copy = pltpu.make_async_copy(time_hbm, time_ref, time_sem)
    time_copy.start()
    for k in range(8):
        rows = pl.ds(k * 144, 144)
        pltpu.make_async_copy(cov_hbm.at[rows], cov.at[rows], cov_sem).start()

    owner_hot = hot_of(owner_ref[...], DEV).astype(BF16)
    obs_hot = hot_of(obs_ref[...], OBS).astype(BF16)
    dir_tile = mul(jnp.broadcast_to(dir_ref[...], (8, OBS)).astype(BF16), obs_hot)[0:1, :]
    fields = mul(
        owner_hot,
        placings(rank_ref[...], dir_tile, block_ref[...].astype(F32), step_ref[...].astype(F32)),
        NT,
    ).astype(BF16)
    lane_base = x * CAP
    lane = lax.broadcasted_iota(jnp.int32, (CAP, LANES), 1)

    def to_quarter(value, quarter):
        hot = jnp.where(sub_iota(CAP, LANES) + quarter * CAP == lane, 1.0, 0.0)
        return mul(value, hot.astype(BF16))

    meta_ref[:, 0, :] = (
        to_quarter(fields[:, :CAP], x)
        + to_quarter(fields[:, CAP : 2 * CAP], xs[2]) * 128.0
        + to_quarter(fields[:, 2 * CAP :], xs[2])
    )
    foot_copy.wait()
    wide[...] = foot_ref[...].astype(F32)
    pl.semaphore_wait(barrier, DEV - 1)

    def send_tile(to_cell, to_tm):
        peer = to_cell * 16 + to_tm
        remote(
            values.at[peer], got.at[me], tile_send, tile_recv.at[cell], to_cell, to_tm
        ).start()
        remote(
            meta_ref.at[peer], got_meta.at[me], meta_send, meta_recv.at[cell], to_cell, to_tm
        ).start()

    def turn(k):
        q = k % 4
        return 2 * (q + q // 2 - 2 * (q // 3)) + k // 4

    natural = [ys[dy] * 4 + xs[dx] for dy in range(4) for dx in range(4)]

    def gather(to_cell, j):
        peer = to_cell * 16 + natural[j]
        for r in range(CAP):
            slots[j, r : r + 1, :] = wide[pl.ds(index_ref[r, peer], 1), :]
        values[peer] = slots[j].astype(BF16)

    for j in range(16):
        gather(cell, j)
        if j > 1:
            send_tile(cell, natural[j - 1])
    send_tile(cell, natural[15])

    def gather_and_send(k, _):
        to_cell = (cell + turn(k)) % 8
        for j in range(16):
            gather(to_cell, j)
            if j:
                send_tile(to_cell, natural[j - 1])
        send_tile(to_cell, natural[15])
        return 0

    lax.fori_loop(1, 8, gather_and_send, 0)
    pltpu.make_async_copy(values.at[me], got.at[me], tile_recv.at[cell]).start()
    pltpu.make_async_copy(meta_ref.at[me], got_meta.at[me], meta_recv.at[cell]).start()

    acc[...] = jnp.zeros_like(acc)
    row_of = sub_iota(LANES, LANES).astype(F32)

    quarter_of = lax.broadcasted_iota(jnp.int32, (1, LANES), 1) // CAP

    def load_meta(group):
        rows = got_meta[pl.ds(group * 16, 16)].reshape(4, 4, LANES)
        out = []
        for q in range(4):
            direction = place = jnp.zeros((1, LANES), F32)
            for j in range(4):
                row = rows[q, j : j + 1, :]
                direction = jnp.where(quarter_of == j, row, direction)
                place = jnp.where(quarter_of == (j + 2) % 4, row, place)
            place = jnp.concatenate([place[:, 64:], place[:, :64]], axis=1)
            block = jnp.floor(place * (1.0 / 128.0))
            out.append((direction, block, place - block * 128.0))
        return out

    def add_group(k, _):
        group = (cell + 8 - turn(k)) % 8
        arrived(got.at[pl.ds(group * 16, 16)], tile_recv.at[group])
        arrived(got_meta.at[pl.ds(group * 16, 16)], meta_recv.at[group])
        rows = load_meta(group)
        tiles = got[pl.ds(group * 16, 16)].reshape(512, LANES)
        for q, (direction, block, step) in enumerate(rows):
            places[group * 4 + q, 0:1, :] = block
            places[group * 4 + q, 1:2, :] = step
            hot = jnp.where(row_of == step, direction, 0.0).astype(BF16)
            for b in range(BLOCKS):
                hots[b * 128 : b * 128 + 128, q * 128 : q * 128 + 128] = hot * jnp.where(
                    block == b, 1.0, 0.0
                ).astype(BF16)
        acc[...] += mul(hots[...], tiles)
        return 0

    lax.fori_loop(0, 8, add_group, 0)
    for b in range(BLOCKS):
        flux[cell, :, b * 128 : b * 128 + 128] = acc[b * 128 : b * 128 + 128, :].astype(BF16)

    partner = z * 2 + 1 - core
    up, down, far = z_cell(1), z_cell(3), z_cell(2)
    left, right, full = pl.ds(0, 512), pl.ds(512, ROWS - 512), pl.ds(0, ROWS)
    z_copies = []

    def z_go(block, cols, to_cell, at):
        ref = flux.at[block, :, cols]
        copy = remote(ref, ref, z_send.at[at], z_recv.at[at], to_cell, tm)
        copy.start()
        z_copies.append(copy)

    def z_wait(block, cols, at):
        arrived(flux.at[block, :, cols], z_recv.at[at])

    z_go(cell, left, up, 0)
    z_go(cell, right, down, 2)
    z_go(cell, right, up, 1)
    z_go(cell, left, down, 3)
    z_go(cell, full, partner, 4)

    time_copy.wait()
    time_sends = []
    for k in (1, 2, 3):
        peer = y_at(k)
        copy = remote(
            time_ref.at[:, pl.ds(pl.multiple_of(peer * 512, 512), 512)],
            time_a.at[y],
            time_send.at[k - 1],
            time_recv.at[k - 1],
            cell,
            peer * 4 + x,
        )
        copy.start()
        time_sends.append(copy)
        peer = x_at(k)
        for other in range(4):
            copy = remote(
                time_ref.at[:, pl.ds(pl.multiple_of((other * 4 + peer) * 128, 128), 128)],
                time_b.at[x, :, pl.ds(other * 128, 128)],
                time_send.at[3 * k + other + (k - 1)],
                time_recv.at[3 * k + other + (k - 1)],
                cell,
                y * 4 + peer,
            )
            copy.start()
            time_sends.append(copy)
    time_a[y] = time_ref[:, pl.ds(pl.multiple_of(y * 512, 512), 512)]
    for other in range(4):
        time_b[x, :, other * 128 : other * 128 + 128] = time_ref[
            :, pl.ds(pl.multiple_of((other * 4 + x) * 128, 128), 128)
        ]

    arrived(cov, cov_sem)

    def other_core(c):
        return c // 2 * 2 + 1 - c % 2

    def mix(block, first=False):
        cols = pl.ds(pl.multiple_of(block * ROWS, 128), ROWS)
        product = mul(cov[:, cols], flux[block], NT)
        if first:
            mixed[...] = product
        else:
            mixed[...] += product

    mix(cell, True)
    z_wait(down, left, 0)
    z_go(down, left, up, 5)
    z_go(down, left, partner, 7)
    z_wait(up, right, 2)
    z_go(up, right, down, 6)
    z_go(up, right, partner, 8)
    z_wait(other_core(cell), full, 4)
    mix(other_core(cell))
    z_wait(down, right, 1)
    z_go(down, right, partner, 9)
    z_wait(up, left, 3)
    z_go(up, left, partner, 10)
    mix(down)
    mix(up)
    z_wait(other_core(down), left, 7)
    z_wait(other_core(down), right, 9)
    mix(other_core(down))
    z_wait(other_core(up), right, 8)
    z_wait(other_core(up), left, 10)
    mix(other_core(up))
    z_wait(far, left, 5)
    z_go(far, left, partner, 11)
    z_wait(far, right, 6)
    z_go(far, right, partner, 12)
    mix(far)
    z_wait(other_core(far), left, 11)
    z_wait(other_core(far), right, 12)
    mix(other_core(far))

    mix_a[:, pl.ds(pl.multiple_of(x * 128, 128), 128)] = mixed[:HALF, :].astype(BF16)
    mix_b[:, pl.ds(pl.multiple_of(y * 128, 128), 128)] = mixed[HALF:, :].astype(BF16)
    ag_copies = []

    def ag_go(buf, at_lane, rows, to_tm, at):
        ref = buf.at[rows, pl.ds(pl.multiple_of(at_lane * 128, 128), 128)]
        copy = remote(ref, ref, ag_send.at[at], ag_recv.at[at], cell, to_tm)
        copy.start()
        ag_copies.append(copy)

    def ag_wait(buf, at_lane, rows, at):
        arrived(buf.at[rows, pl.ds(pl.multiple_of(at_lane * 128, 128), 128)], ag_recv.at[at])

    first, second = pl.ds(0, QUARTER), pl.ds(QUARTER, QUARTER)
    x_up, x_down = y * 4 + x_at(1), y * 4 + x_at(3)
    y_up, y_down = y_at(1) * 4 + x, y_at(3) * 4 + x
    ag_go(mix_a, x, first, x_up, 0)
    ag_go(mix_a, x, second, x_down, 1)
    ag_go(mix_b, y, first, y_up, 2)
    ag_go(mix_b, y, second, y_down, 3)
    ag_go(mix_a, x, second, x_up, 4)
    ag_go(mix_a, x, first, x_down, 5)
    ag_go(mix_b, y, second, y_up, 6)
    ag_go(mix_b, y, first, y_down, 7)
    ag_wait(mix_a, x_at(3), first, 0)
    ag_go(mix_a, x_at(3), first, x_up, 8)
    ag_wait(mix_a, x_at(1), second, 1)
    ag_go(mix_a, x_at(1), second, x_down, 9)
    ag_wait(mix_b, y_at(3), first, 2)
    ag_go(mix_b, y_at(3), first, y_up, 10)
    ag_wait(mix_b, y_at(1), second, 3)
    ag_go(mix_b, y_at(1), second, y_down, 11)
    for k in (1, 2, 3):
        arrived(time_a.at[y_at(4 - k)], time_recv.at[k - 1])
        for other in range(4):
            arrived(
                time_b.at[x_at(4 - k), :, pl.ds(other * 128, 128)],
                time_recv.at[3 * k + other + (k - 1)],
            )
    ag_wait(mix_a, x_at(3), second, 4)
    ag_wait(mix_a, x_at(1), first, 5)
    ag_wait(mix_b, y_at(3), second, 6)
    ag_wait(mix_b, y_at(1), first, 7)
    ag_wait(mix_a, x_at(2), first, 8)
    ag_wait(mix_a, x_at(2), second, 9)
    rs_copies = []
    for k in (2, 1, 3):
        peer = y_at(k)
        part_a[k - 1] = mul(mix_a[...], time_a[peer], NT).astype(BF16)
        copy = remote(
            part_a.at[k - 1],
            in_a.at[k - 1],
            rs_send.at[k - 1],
            rs_recv.at[k - 1],
            cell,
            peer * 4 + x,
        )
        copy.start()
        rs_copies.append(copy)
        if k == 2:
            ag_wait(mix_b, y_at(2), first, 10)
            ag_wait(mix_b, y_at(2), second, 11)
        peer = x_at(k)
        part_b[k - 1] = mul(mix_b[...], time_b[peer], NT).astype(BF16)
        copy = remote(
            part_b.at[k - 1],
            in_b.at[k - 1],
            rs_send.at[k + 2],
            rs_recv.at[k + 2],
            cell,
            y * 4 + peer,
        )
        copy.start()
        rs_copies.append(copy)
    mixed[:HALF, :] = mul(mix_a[...], time_a[y], NT)
    mixed[HALF:, :] = mul(mix_b[...], time_b[x], NT)
    for k in (1, 3, 2):
        arrived(in_a.at[k - 1], rs_recv.at[k - 1])
        mixed[:HALF, :] += in_a[k - 1].astype(F32)
        arrived(in_b.at[k - 1], rs_recv.at[k + 2])
        mixed[HALF:, :] += in_b[k - 1].astype(F32)
    for b in range(BLOCKS):
        smooth[b * 128 : b * 128 + 128, :] = mixed[b * 128 : b * 128 + 128, :].T.astype(BF16)

    def dot_group(k):
        group = away(k)
        products[...] = mul(smooth[...], got[pl.ds(group * 16, 16)].reshape(512, LANES), NT)
        for q in range(4):
            block, step = places[group * 4 + q, 0:1, :], places[group * 4 + q, 1:2, :]
            cols = slice(q * 128, q * 128 + 128)
            picked = products[0:128, cols]
            for b in range(1, BLOCKS):
                picked = jnp.where(block == b, products[b * 128 : b * 128 + 128, cols], picked)
            picked = jnp.where(row_of == step, picked, 0.0)
            dots[group * 4 + q] = jnp.sum(picked, axis=0, keepdims=True)

    def send_dots(k, peers):
        group = away(k)
        for to_tm in peers:
            remote(
                dots.at[group * 4 + to_tm // 4], dots_back.at[me], back_send, back_recv, group, to_tm
            ).start()

    dot_group(0)

    def dots_and_send(k, _):
        send_dots(k - 1, planes)
        dot_group(k)
        return 0

    lax.fori_loop(1, 8, dots_and_send, 0)
    send_dots(7, planes[:15])
    dots_back[me] = dots[me // 4]
    owner_hot = hot_of(owner_ref[...], DEV).astype(BF16)
    obs_hot = hot_of(obs_ref[...], OBS).astype(BF16)
    in_slot = sub_iota(CAP, TILES).astype(F32) == rank_ref[...]
    arrived(dots_back.at[pl.ds(0, DEV - 1)], back_recv)
    by_rank[...] = dots_back[:, 0, :].T
    own = jnp.concatenate(split3(by_rank[pl.ds(pl.multiple_of(lane_base, CAP), CAP), :]), axis=0)
    parts = mul(own, owner_hot)
    tile_dots = jnp.sum(
        jnp.where(in_slot, parts[:CAP] + parts[CAP : 2 * CAP] + parts[2 * CAP :], 0.0),
        axis=0,
        keepdims=True,
    )
    high, middle, low = split3(tile_dots)
    three = jnp.concatenate(
        [high.astype(F32), middle.astype(F32), low.astype(F32), jnp.zeros((5, TILES), F32)], axis=0
    ).astype(BF16)
    direction, residual = dir_ref[...], res_ref[...]
    applied = jnp.sum(mul(three, obs_hot, NT), axis=0, keepdims=True)
    applied = applied + noise_ref[...] * direction

    lanes = lax.broadcasted_iota(jnp.int32, (1, LANES), 1)
    row = jnp.zeros((1, LANES), F32)
    for at, value in enumerate(
        (residual * residual, direction * applied, residual * applied, applied * applied)
    ):
        row = jnp.where(lanes == at, jnp.sum(value, axis=1, keepdims=True), row)
    sums[...] = row
    to_others(
        lambda to_cell, to_tm: remote(
            sums, sums_in.at[me], sum_send, sum_recv, to_cell, to_tm
        ).start()
    )
    sums_in[me] = row
    arrived(sums_in.at[pl.ds(0, DEV - 1)], sum_recv)
    total = jnp.sum(sums_in[...], axis=0)

    def total_of(at):
        return jnp.sum(jnp.where(lanes == at, total, 0.0), axis=1, keepdims=True)

    norm_now, curvature, cross_term, image_norm = (total_of(at) for at in range(4))
    step_size = norm_now / curvature
    norm_next = norm_now - 2.0 * step_size * cross_term + step_size * step_size * image_norm
    applied_ref[...] = applied
    size_ref[...] = jnp.broadcast_to(step_size, (1, OBS))
    ratio_ref[...] = jnp.broadcast_to(norm_next / norm_now, (1, OBS))

    arrived(values.at[pl.ds(0, DEV - 1)], tile_send)
    arrived(meta_ref.at[pl.ds(0, DEV - 1)], meta_send)
    for copy in time_sends + z_copies + ag_copies + rs_copies:
        copy.wait_send()
    arrived(dots_back.at[pl.ds(0, DEV - 1)], back_send)
    arrived(sums_in.at[pl.ds(0, DEV - 1)], sum_send)


def whole(*operands):
    vmem = pl.BlockSpec(memory_space=pltpu.VMEM)
    dma = pltpu.SemaphoreType.DMA
    row = jax.ShapeDtypeStruct((1, OBS), F32)
    return pl.pallas_call(
        main_kernel,
        out_shape=(row, row, row),
        in_specs=[vmem] * 8
        + [pl.BlockSpec(memory_space=pltpu.SMEM)]
        + [pl.BlockSpec(memory_space=pl.ANY)] * 3,
        out_specs=(vmem,) * 3,
        scratch_shapes=[
            pltpu.VMEM((TILES, LANES), BF16),
            pltpu.VMEM((LANES, 16 * LANES), BF16),
            pltpu.VMEM((DEV, 1, LANES), F32),
            pltpu.VMEM((TILES, LANES), F32),
            pltpu.VMEM((16, CAP, LANES), F32),
            pltpu.VMEM((DEV, CAP, LANES), BF16),
            pltpu.VMEM((ROWS, 8 * ROWS), BF16),
            pltpu.VMEM((DEV, CAP, LANES), BF16),
            pltpu.VMEM((DEV, 1, LANES), F32),
            pltpu.VMEM((DEV // 4, 2, LANES), F32),
            pltpu.VMEM((ROWS, 512), BF16),
            pltpu.VMEM((ROWS, LANES), F32),
            pltpu.VMEM((8, LANES, ROWS), BF16),
            pltpu.VMEM((ROWS, LANES), F32),
            pltpu.VMEM((HALF, 512), BF16),
            pltpu.VMEM((HALF, 512), BF16),
            pltpu.VMEM((4, LANES, 512), BF16),
            pltpu.VMEM((4, LANES, 512), BF16),
            pltpu.VMEM((3, HALF, LANES), BF16),
            pltpu.VMEM((3, HALF, LANES), BF16),
            pltpu.VMEM((3, HALF, LANES), BF16),
            pltpu.VMEM((3, HALF, LANES), BF16),
            pltpu.VMEM((ROWS, LANES), BF16),
            pltpu.VMEM((ROWS, 512), F32),
            pltpu.VMEM((DEV // 4, 1, LANES), F32),
            pltpu.VMEM((DEV, 1, LANES), F32),
            pltpu.VMEM((LANES, DEV), F32),
            pltpu.VMEM((1, LANES), F32),
            pltpu.VMEM((DEV, 1, LANES), F32),
            dma,
            dma,
            dma,
            dma,
            dma((8,)),
            dma,
            dma((8,)),
            dma((13,)),
            dma((13,)),
            dma((15,)),
            dma((15,)),
            dma((12,)),
            dma((12,)),
            dma((6,)),
            dma((6,)),
            dma,
            dma,
            dma,
            dma,
        ],
        compiler_params=pltpu.CompilerParams(
            collective_id=0, has_side_effects=True, vmem_limit_bytes=60 * 2**20
        ),
        name="whole",
    )(*operands)


def local(
    solution,
    residual,
    direction,
    noise_var,
    footprints,
    tile_owner,
    tile_block,
    tile_step,
    tile_obs,
    cell_cov,
    time_cov,
):
    row = functools.partial(jnp.reshape, shape=(1, OBS))
    tile_row = functools.partial(jnp.reshape, shape=(1, TILES))
    owner = tile_row(tile_owner)
    index, rank = prep(owner)
    outs = whole(
        row(residual),
        row(direction),
        row(noise_var),
        owner,
        tile_row(tile_block),
        tile_row(tile_step),
        tile_row(tile_obs),
        rank,
        index,
        footprints,
        cell_cov,
        time_cov,
    )
    applied, step_size, ratio = (out.reshape(OBS) for out in outs)
    new_residual = residual - step_size * applied
    return solution + step_size * direction, new_residual, new_residual + ratio * direction


def solution(mesh):
    both = P(CELL_TM)
    in_specs = (both,) * 4 + (P(CELL_TM, None),) * 2 + (both,) * 3
    in_specs += (P("cell", None), P("tm", None))
    return jax.shard_map(
        local, mesh=mesh, in_specs=in_specs, out_specs=(both,) * 3, check_vma=False
    )
```
